32 devices in a mesh: mp: 2 (over core), dev: 16 (over z, y, x).
Axes of the slice: x: 2, y: 2, z: 4, core: 2. Of those that a mesh axis runs over, the one named last changes fastest.
Arguments:
- spectrum: float32 [1024, 8192], P(None, ('mp', 'dev')), may hold values from 0.05 to 1
- water_mask: int32 [8192], P(('mp', 'dev')), may hold values 0 or 1
- courant: float32 [2, 1024], replicated, may hold values from 0.05 to 0.3
- stencil_sign: int32 [2, 1024], replicated, may hold values from 0 to 1
- quad_index: int32 [4, 1024, 2], replicated, may hold values from 0 to 1023
- quad_weight: float32 [4, 1024, 2], replicated, may hold values from 0.2 to 1
- nonlinear: float32 [1024], replicated, may hold values from 0.01 to 0.1
- stokes_table: bfloat16 [128, 1024], replicated, may hold values from -0.1875 to 0.1875
- point_index: int32 [4, 8192], P(None, ('mp', 'dev')), may hold values from 0 to 4095, as said below
- point_weight: float32 [4, 8192], P(None, ('mp', 'dev')), may hold values from 0.1 to 0.4
- ocean_index: int32 [4, 4096], P(None, ('mp', 'dev')), may hold values from 0 to 8191, as said below
- ocean_weight: float32 [4, 4096], P(None, ('mp', 'dev')), may hold values from 0.1 to 0.4
- currents: float32 [2, 64, 4096], P(None, None, ('mp', 'dev')), may hold values from -3 to 3
- coriolis: float32 [4096], P(('mp', 'dev')), may hold values from 0.2 to 0.6
- mixing: float32 [64], replicated, may hold values from 0.05 to 0.2
- surface_weights: float32 [64], replicated, may hold values from 0.005 to 0.05
Outputs:
- spectrum_out: float32 [1024, 8192], P(None, ('mp', 'dev'))
- currents_out: float32 [2, 64, 4096], P(None, None, ('mp', 'dev'))
The draws below stay inside these ranges and needn't reach their ends.
Inputs may be any that keep to these rules, and one draw needn't show every extreme that they name: `point_index`: entry j of point p names an ocean cell in row p // 256 plus -1, 0 or 1 and column (p % 256) // 2 plus -1, 0 or 1, both wrapping. `ocean_index`: entry j of cell c names a wave point in row c // 128 plus -1, 0 or 1 and column 2 (c % 128) plus -2 to 3, both wrapping.
All inputs are finite; a program needn't handle non-finite values. No bound on the sum of `water_mask` on one device may be relied on, other than what follows from the above.
Results may differ from the reference program's by a relative error of at most 0.0003.
The reference program's roundings to bfloat16 on the way count: a program that leaves them out, or rounds other values in their place, can miss the bound.
Values sent between devices are 32-bit elements; how exact they have to be, the bound alone decides.
A program may use at most 64 MiB of HBM per device.

```python
import math
import jax
import jax.numpy as jnp
from jax import lax

K = 1024
L = 64
MX = 256
STEPS = 2
OX = 128
MY = 32
P_SIZE = 8192
NOC = 4096


def draw_point_index(key, part):
    point_total = MX * MY
    position = jnp.arange(point_total, dtype=jnp.int32)
    row_key, column_key = jax.random.split(jax.random.fold_in(key, 11))
    row_pick = (position // MX)[None, :] + jax.random.randint(row_key, (4, point_total), -1, 2)
    column_pick = (position % MX // 2)[None, :] + jax.random.randint(column_key, (4, point_total), -1, 2)
    return (jnp.mod(row_pick, MY) * OX + jnp.mod(column_pick, OX)).astype(jnp.int32)


def draw_ocean_index(key, part):
    cell_total = OX * MY
    position = jnp.arange(cell_total, dtype=jnp.int32)
    row_key, column_key = jax.random.split(jax.random.fold_in(key, 23))
    row_pick = (position // OX)[None, :] + jax.random.randint(row_key, (4, cell_total), -1, 2)
    column_pick = (2 * (position % OX))[None, :] + jax.random.randint(column_key, (4, cell_total), -2, 4)
    return (jnp.mod(row_pick, MY) * MX + jnp.mod(column_pick, MX)).astype(jnp.int32)


def place_ends(drawn, stream_key, low, high):
    place = [jax.random.randint(jax.random.fold_in(stream_key, axis), (), 0, length) for axis, length in enumerate(drawn.shape)]
    longest = drawn.shape.index(max(drawn.shape))
    beside = place[:longest] + [(place[longest] + 1) % drawn.shape[longest]] + place[longest + 1:]
    return drawn.at[tuple(place)].set(low).at[tuple(beside)].set(high)


def block_levels(rng, extent, cuts, smallest, top_value):
    def one(dim, parts):
        steps = jax.random.uniform(jax.random.fold_in(jax.random.fold_in(rng, 6), dim), (parts,), jnp.float32, smallest / len(cuts), top_value / len(cuts))
        return jnp.repeat(jnp.exp(steps), extent[dim] // parts).reshape((-1,) + (1,) * (len(extent) - dim - 1))

    level = one(*cuts[0])
    for cut in cuts[1:]:
        level = level * one(*cut)
    return level


def noise(own_key, extent, deviation, bound, cuts=(), held_as=jnp.bfloat16):
    factor_of = block_levels(own_key, extent, cuts, -0.22, 0.18) if cuts else 1.0
    values = jax.random.normal(own_key, extent, jnp.float32) * deviation * factor_of
    return jnp.minimum(jnp.maximum(values, -bound), bound).astype(held_as)


def setup_inputs(seed: int = 0) -> dict:
    key_of = jax.random.split(jax.random.key(seed), 17)
    spectrum = jnp.clip(jnp.exp(math.log(1.0) - 2.9957323 * jax.random.uniform(key_of[0], (K, P_SIZE), jnp.float32) ** block_levels(key_of[0], (K, P_SIZE), ((1, 32),), -0.2, 0.2)), 0.05, 1.0)
    water_mask = place_ends((jax.random.randint(key_of[1], (P_SIZE,), 0, 8) < 7).astype(jnp.int32), jax.random.fold_in(key_of[1], 1), 0, 1)
    courant = jnp.clip(jnp.exp(jax.random.uniform(key_of[2], (2, K), jnp.float32, math.log(0.05), math.log(0.3))), 0.05, 0.3)
    stencil_sign = place_ends(jax.random.randint(key_of[3], (2, K), 0, 2), jax.random.fold_in(key_of[3], 1), 0, 1).astype(jnp.int32)
    quad_index = place_ends(jax.random.randint(key_of[4], (4, K, 2), 0, K), jax.random.fold_in(key_of[4], 1), 0, K - 1).astype(jnp.int32)
    quad_weight = jnp.clip(jax.random.uniform(key_of[5], (4, K, 2), jnp.float32, 0.2, 1.0), 0.2, 1.0)
    nonlinear = jnp.clip(jnp.exp(jax.random.uniform(key_of[6], (K,), jnp.float32, math.log(0.01), math.log(0.1))), 0.01, 0.1)
    stokes_table = noise(key_of[7], (2 * L, K), K ** -0.5, 0.1875)
    point_index = draw_point_index(jax.random.fold_in(key_of[16], 71), 0)
    point_weight = jnp.clip(0.1 + 0.3 * jax.random.uniform(key_of[9], (4, P_SIZE), jnp.float32) ** block_levels(key_of[9], (4, P_SIZE), ((1, 32),), -0.2, 0.2), 0.1, 0.4)
    ocean_index = draw_ocean_index(jax.random.fold_in(key_of[16], 71), 0)
    ocean_weight = jnp.clip(0.1 + 0.3 * jax.random.uniform(key_of[11], (4, NOC), jnp.float32) ** block_levels(key_of[11], (4, NOC), ((1, 32),), -0.2, 0.2), 0.1, 0.4)
    currents = noise(key_of[12], (2, L, NOC), 0.5, 3.0, ((2, 32),), jnp.float32)
    coriolis = jnp.clip(0.2 + 0.400000021 * jax.random.uniform(key_of[13], (NOC,), jnp.float32) ** block_levels(key_of[13], (NOC,), ((0, 32),), -0.2, 0.2), 0.2, 0.6)
    mixing = jnp.clip(jax.random.uniform(key_of[14], (L,), jnp.float32, 0.05, 0.2), 0.05, 0.2)
    surface_weights = jnp.clip(jnp.exp(jax.random.uniform(key_of[15], (L,), jnp.float32, math.log(0.005), math.log(0.05))), 0.005, 0.05)
    return dict(spectrum=spectrum, water_mask=water_mask, courant=courant, stencil_sign=stencil_sign, quad_index=quad_index, quad_weight=quad_weight, nonlinear=nonlinear, stokes_table=stokes_table, point_index=point_index, point_weight=point_weight, ocean_index=ocean_index, ocean_weight=ocean_weight, currents=currents, coriolis=coriolis, mixing=mixing, surface_weights=surface_weights)


ocean_step_size = 0.5


def advect(spectra, padded, point_flow, courant, stencil_sign):
    eastward = stencil_sign[0][:, None, None] == 1
    northward = stencil_sign[1][:, None, None] == 1
    sense_x = (2 * stencil_sign[0] - 1).astype(jnp.float32)[:, None, None]
    sense_y = (2 * stencil_sign[1] - 1).astype(jnp.float32)[:, None, None]
    behind_x = jnp.where(eastward, jnp.roll(spectra, 1, axis=2), jnp.roll(spectra, -1, axis=2))
    behind_y = jnp.where(northward, padded[:, :-2], padded[:, 2:])
    speed_x = courant[0][:, None, None] * (1.0 + 0.5 * jnp.tanh(sense_x * point_flow[0][None]))
    speed_y = courant[1][:, None, None] * (1.0 + 0.5 * jnp.tanh(sense_y * point_flow[1][None]))
    return spectra - speed_x * (spectra - behind_x) - speed_y * (spectra - behind_y)


def nonlinear_update(advected, interps, gain_rows, wet_row):
    total_sum = interps[0] + interps[1] + interps[2] + interps[3]
    pair_sum = interps[0] * interps[1] + interps[2] * interps[3]
    source = advected * advected * total_sum - advected * pair_sum
    return wet_row[None, :] * (advected + gain_rows[:, None] * source)


def vertical_mix(profile, mixing):
    above_level = jnp.concatenate([profile[:1], profile[:-1]], axis=0)
    below_level = jnp.concatenate([profile[1:], profile[-1:]], axis=0)
    return mixing[:, None, None] * (above_level - 2.0 * profile + below_level)


def ocean_tendency(zonal_flow, meridional, padded_zonal, mixing):
    vorticity = 0.5 * (jnp.roll(meridional, -1, axis=2) - jnp.roll(meridional, 1, axis=2)) - 0.5 * (padded_zonal[:, 2:] - padded_zonal[:, :-2])
    return vorticity, vertical_mix(zonal_flow, mixing), vertical_mix(meridional, mixing)


def ocean_advance(zonal_flow, meridional, tendency, stokes_drift, rotation):
    vorticity, mix_zonal, mix_meridional = tendency
    drift_x = stokes_drift[0]
    drift_y = stokes_drift[1]
    new_zonal = zonal_flow + ocean_step_size * (rotation[None] * (meridional + drift_y) + vorticity * drift_y + mix_zonal)
    new_meridional = meridional + ocean_step_size * (-rotation[None] * (zonal_flow + drift_x) - vorticity * drift_x + mix_meridional)
    return jnp.stack([new_zonal, new_meridional])


def reference(spectrum, water_mask, courant, stencil_sign, quad_index, quad_weight, nonlinear, stokes_table, point_index, point_weight, ocean_index, ocean_weight, currents, coriolis, mixing, surface_weights):
    repeated = quad_index[:, :, 0] == quad_index[:, :, 1]
    first_weight = jnp.where(repeated, quad_weight[:, :, 0] + quad_weight[:, :, 1], quad_weight[:, :, 0]).astype(jnp.bfloat16).astype(jnp.float32)
    second_weight = jnp.where(repeated, jnp.zeros_like(quad_weight[:, :, 1]), quad_weight[:, :, 1]).astype(jnp.bfloat16).astype(jnp.float32)
    first_index = quad_index[:, :, 0]
    second_index = quad_index[:, :, 1]
    wet_points = water_mask.astype(jnp.float32)
    stokes_rows = stokes_table.astype(jnp.float32)
    rotation = coriolis.reshape(MY, OX)
    ocean_state = currents
    spectra = spectrum
    for step_index in range(STEPS):
        surface = jnp.sum(surface_weights[None, :, None] * ocean_state, axis=1)
        point_flow = sum(point_weight[config][None, :] * surface[:, point_index[config]] for config in range(4))
        map_grid = spectra.reshape(K, MY, MX)
        padded = jnp.concatenate([map_grid[:, -1:], map_grid, map_grid[:, :1]], axis=1)
        advected = advect(map_grid, padded, point_flow.reshape(2, MY, MX), courant, stencil_sign)
        rounded = lax.optimization_barrier(advected.astype(jnp.bfloat16)).astype(jnp.float32)

        def one_block(pieces):
            block_rows, block_rounded, block_wet = pieces
            interps = first_weight[:, :, None] * block_rounded[first_index] + second_weight[:, :, None] * block_rounded[second_index]
            return nonlinear_update(block_rows, interps, nonlinear, block_wet)

        updated = lax.map(one_block, (advected.transpose(1, 0, 2), rounded.transpose(1, 0, 2), wet_points.reshape(MY, MX)))
        spectra = updated.transpose(1, 0, 2).reshape(K, MY * MX)
        spectra_rounded = lax.optimization_barrier(spectra.astype(jnp.bfloat16)).astype(jnp.float32)
        stokes = jnp.dot(stokes_rows, spectra_rounded, precision=lax.Precision.HIGHEST)
        stokes_drift = sum(ocean_weight[config][None, :] * stokes[:, ocean_index[config]] for config in range(4))
        stokes_drift = stokes_drift.reshape(2, L, MY, OX)
        zonal_flow = ocean_state[0].reshape(L, MY, OX)
        meridional = ocean_state[1].reshape(L, MY, OX)
        padded_zonal = jnp.concatenate([zonal_flow[:, -1:], zonal_flow, zonal_flow[:, :1]], axis=1)
        tendency = ocean_tendency(zonal_flow, meridional, padded_zonal, mixing)
        ocean_state = ocean_advance(zonal_flow, meridional, tendency, stokes_drift, rotation).reshape(2, L, MY * OX)
    return spectra, ocean_state
```

```python
import jax
import jax.numpy as jnp
from jax import lax
from jax.experimental import pallas as pl
from jax.experimental.pallas import tpu as pltpu
from jax.sharding import PartitionSpec as P

STEPS = 2
OCEAN_STEP = 0.5
TEAM = 4
COMM = 8
KPARTS = 4
MESH = pl.DeviceIdType.MESH
F32, BF16 = jnp.float32, jnp.bfloat16


def split(x):
    high = x.astype(BF16)
    return high, (x - high.astype(F32)).astype(BF16)


def dot(a, b):
    return jnp.dot(a, b, preferred_element_type=F32)


def dot_split(x, table_high, table_low):
    high, low = split(x)
    return dot(high, table_high) + (dot(low, table_high) + dot(high, table_low))


def wave_kernel(
    spec, wet, courant, sign, qidx, qwt, nonlinear, table, pidx, pwt, oidx, owt,
    currents, coriolis, mixing, sweight,
    spec_out, cur_out,
    araw, cols, lraw, quad, pk, pk2, rx, zpk, zin, ex, exin, edge, adv, advb, acc, mid, midb, state,
    mbuf, meta, bmeta, osm, orx, sbuf, srx, sall, zhalo, ptab, btab, otab, dm, drx, dbuf, dhalo, dself, tan,
    rxs, rxr, zs, zr, es, er, fs, fr, ms, mr, os_, or_, ss, sr, ds_, dr, us, ur, hs, hr,
):
    comps, points = spec.shape
    cells = coriolis.shape[1]
    levels = mixing.shape[1]
    dev_count = lax.axis_size("dev")
    total = lax.axis_size("mp") * dev_count
    pos = lax.axis_index("mp") * dev_count + lax.axis_index("dev")
    b = lax.rem(pos, TEAM)
    base = pos - b
    width = points // TEAM
    window = cells // TEAM
    size = comps // COMM
    half = size // 2
    lanes = 2 * width

    def wrap(p):
        return lax.rem(p + total, total)

    up, down = wrap(pos + 1), wrap(pos - 1)
    ahead, behind = wrap(pos + TEAM), wrap(pos - TEAM)
    mates = [lax.rem(b + i, TEAM) for i in range(1, TEAM)]

    def remote(src, dst, ssem, rsem, p):
        return pltpu.make_async_remote_copy(
            src_ref=src, dst_ref=dst, send_sem=ssem, recv_sem=rsem,
            device_id=(lax.div(p, dev_count), lax.rem(p, dev_count)), device_id_type=MESH,
        )

    def span(c, n):
        return pl.ds(pl.multiple_of(c * n, n), n)

    def rows(c):
        return span(c, size)

    def halves(c):
        return span(c, half)

    def each(low, high, body):
        def run(c, carry):
            body(c)
            return carry

        lax.fori_loop(low, high, run, 0)

    def start(copies):
        for copy in copies:
            copy.start()

    def received(copies):
        for copy in copies:
            copy.wait_recv()

    def sent(copies):
        for copy in copies:
            copy.wait_send()

    def piece_out(step, c):
        src = pk if step == 0 else pk2
        return [
            remote(src.at[d, halves(c)], rx.at[step, b, halves(c)], rxs.at[step, i, c], rxr.at[step, b, c], base + d)
            for i, d in enumerate(mates)
        ]

    def piece_in(step, c):
        src = pk if step == 0 else pk2
        return [
            remote(src.at[d, halves(c)], rx.at[step, d, halves(c)], rxs.at[step, i, c], rxr.at[step, d, c], base + d)
            for i, d in enumerate(mates)
        ]

    def halo(step, c):
        low = rx.at[0, TEAM - 1, halves(c)] if step == 0 else zpk.at[0, halves(c)]
        high = rx.at[0, 0, halves(c)] if step == 0 else zpk.at[1, halves(c)]
        return [
            remote(low, zin.at[step, 0, halves(c)], zs.at[step, 0, c], zr.at[step, 0, c], ahead),
            remote(high, zin.at[step, 1, halves(c)], zs.at[step, 1, c], zr.at[step, 1, c], behind),
        ]

    def edges_out():
        return [remote(ex.at[0], exin.at[b], es.at[i], er.at[b], base + d) for i, d in enumerate(mates)]

    def edges_in():
        return [remote(ex.at[0], exin.at[d], es.at[i], er.at[d], base + d) for i, d in enumerate(mates)]

    right, left = base + mates[0], base + mates[2]

    def sides():
        return [
            remote(ex.at[1], exin.at[TEAM], fs.at[0], fr.at[0], right),
            remote(ex.at[1], exin.at[TEAM + 1], fs.at[1], fr.at[1], left),
        ]

    def meta_out():
        return [remote(mbuf, meta.at[b], ms.at[i], mr.at[b], base + d) for i, d in enumerate(mates)]

    def meta_in():
        return [remote(mbuf, meta.at[d], ms.at[i], mr.at[d], base + d) for i, d in enumerate(mates)]

    def row_out(step):
        src, dst, ssem, rsem = (osm, orx, os_, or_) if step == 0 else (sbuf, srx, ss, sr)
        inner = [remote(src, dst.at[b + 1], ssem.at[i], rsem.at[b + 1], base + d) for i, d in enumerate(mates)]
        before = [
            remote(src, dst.at[TEAM + 1], ssem.at[3 + k], rsem.at[TEAM + 1], wrap(base - TEAM + k)) for k in range(TEAM)
        ]
        after = [remote(src, dst.at[0], ssem.at[3 + k], rsem.at[0], wrap(base + TEAM + k)) for k in range(TEAM)]
        return inner, before, after

    def row_start(step):
        inner, before, after = row_out(step)

        @pl.when(b == 0)
        def _():
            start(before)

        @pl.when(b == TEAM - 1)
        def _():
            start(after)

        start(inner)

    def row_sent(step):
        inner, before, after = row_out(step)
        sent(inner)

        @pl.when(b == 0)
        def _():
            sent(before)

        @pl.when(b == TEAM - 1)
        def _():
            sent(after)

    def row_in(step):
        src, dst, ssem, rsem = (osm, orx, os_, or_) if step == 0 else (sbuf, srx, ss, sr)
        copies = [remote(src, dst.at[d + 1], ssem.at[i], rsem.at[d + 1], base + d) for i, d in enumerate(mates)]
        copies.append(remote(src, dst.at[0], ssem.at[0], rsem.at[0], ahead))
        copies.append(remote(src, dst.at[TEAM + 1], ssem.at[0], rsem.at[TEAM + 1], behind))
        return copies

    def drift_out():
        copies = [
            remote(dm.at[0], drx.at[TEAM + b], ds_.at[3], dr.at[TEAM + b], wrap(base - 1)),
            remote(dm.at[TEAM + 1], drx.at[TEAM + b], ds_.at[4], dr.at[TEAM + b], wrap(base + TEAM)),
        ]
        return copies + [
            remote(dm.at[d + 1], drx.at[b], ds_.at[i], dr.at[b], base + d) for i, d in enumerate(mates)
        ]

    def drift_in():
        inner = [remote(dm.at[0], drx.at[d], ds_.at[i], dr.at[d], base + d) for i, d in enumerate(mates)]
        outer = [remote(dm.at[0], drx.at[TEAM + k], ds_.at[3], dr.at[TEAM + k], ahead) for k in range(TEAM)]
        return inner, outer

    def zonal_pair(step):
        src = currents.at[0] if step == 0 else state.at[0]
        return [
            remote(src, zhalo.at[step, 0], us.at[step, 0], ur.at[step, 0], up),
            remote(src, zhalo.at[step, 1], us.at[step, 1], ur.at[step, 1], down),
        ]

    def last_pair():
        return [
            remote(dbuf.at[0], dhalo.at[0], hs.at[0], hr.at[0], up),
            remote(dbuf.at[1], dhalo.at[1], hs.at[1], hr.at[1], down),
        ]

    drx[TEAM : 2 * TEAM] = jnp.zeros((TEAM, levels, lanes), F32)
    barrier = pltpu.get_barrier_semaphore()
    partners = [base + d for d in mates]
    partners += [wrap(base - TEAM + k) for k in range(TEAM)] + [wrap(base + TEAM + k) for k in range(TEAM)]
    for p in partners:
        pl.semaphore_signal(
            barrier, inc=1, device_id=(lax.div(p, dev_count), lax.rem(p, dev_count)), device_id_type=MESH
        )

    lane = lax.broadcasted_iota(jnp.int32, (half, lanes), 1)
    low = lane < width

    def even(a, c):
        return jnp.where(low, a, pltpu.roll(c, width, 1))

    def odd(a, c):
        return jnp.where(low, pltpu.roll(a, width, 1), c)

    lane_row = lax.broadcasted_iota(jnp.int32, (8, lanes), 1)
    wide_lane = lax.broadcasted_iota(jnp.int32, (size, lanes), 1)
    rim = lax.rem(wide_lane + 1, width) < 2

    def pack_rim(first, second):
        mixed = jnp.where(rim, first, pltpu.roll(second, 2, 1))
        out = jnp.zeros((8, lanes), F32)
        for g in range(size // 8):
            here = lax.rem(lane_row + 1 - 4 * g + lanes, width) < 4
            part = mixed[8 * g : 8 * g + 8]
            out = jnp.where(here, pltpu.roll(part, 4 * g, 1) if g else part, out)
        return out

    lraw[...] = jnp.zeros_like(lraw)
    lraw[0:1, 0:levels] = mixing[...]
    lraw[1:2, 0:levels] = sweight[...]
    lcols = jnp.transpose(lraw[...])
    level_mix = lcols[0:levels, 0:1]
    level_weight = lcols[0:levels, 1:2]

    def surface(source, dst, at):
        dst[at : at + 8, :] = jnp.zeros((8, cells), F32)
        for a in range(2):
            dst[at + a : at + a + 1, :] = jnp.sum(level_weight * source[a], axis=0, keepdims=True)

    osm[0:4, :] = oidx[...].astype(F32)
    osm[4:8, :] = owt[...]
    surface(currents, osm, 8)
    orx[b + 1] = osm[...]
    mbuf[...] = jnp.zeros_like(mbuf)
    mbuf[0:4, :] = pidx[...].astype(F32)
    mbuf[4:8, :] = pwt[...]
    mbuf[8:9, :] = wet[...].astype(F32)
    meta[b] = mbuf[...]

    def pack_in(c):
        for t in range(2):
            tile = spec[rows(c), t * lanes : (t + 1) * lanes]
            first, second = tile[0:half], tile[half:size]
            pk[2 * t, halves(c), :] = even(first, second)
            pk[2 * t + 1, halves(c), :] = odd(first, second)
        rx[0, b, halves(c), :] = pk[b, halves(c), :]
        ex[0, span(c, 8), :] = pack_rim(spec[rows(c), 0:lanes], spec[rows(c), lanes : 2 * lanes])

    each(0, COMM, pack_in)
    exin[b] = ex[0]
    pl.semaphore_wait(barrier, len(partners))

    row_start(0)
    start(meta_out())
    start(edges_out())
    each(0, COMM, lambda c: start(piece_out(0, c)))
    start(zonal_pair(0))

    araw[...] = jnp.zeros_like(araw)
    araw[0:2, :] = courant[...]
    araw[2:4, :] = (2 * sign[...] - 1).astype(F32)
    araw[4:5, :] = nonlinear[...]
    for j in range(4):
        araw[8 + 2 * j : 10 + 2 * j, :] = qidx[j].astype(F32)
        araw[16 + 2 * j : 18 + 2 * j, :] = qwt[j]
    cols[...] = jnp.transpose(araw[...])
    long_lane = lax.broadcasted_iota(jnp.int32, (32, comps), 1).astype(F32)

    def build_quad(c):
        for sub in range(size // 32):
            at = pl.ds(pl.multiple_of(c * size + sub * 32, 32), 32)
            col = cols[at, :]
            for j in range(4):
                one = jnp.where(col[:, 8 + 2 * j : 9 + 2 * j] == long_lane, col[:, 16 + 2 * j : 17 + 2 * j], 0.0)
                two = jnp.where(col[:, 9 + 2 * j : 10 + 2 * j] == long_lane, col[:, 17 + 2 * j : 18 + 2 * j], 0.0)
                quad[j, at, :] = (one + two).astype(BF16)

    def forward(c):
        received(piece_in(0, c))
        start(halo(0, c))

    def first(c):
        build_quad(2 * c)
        build_quad(2 * c + 1)
        forward(c)

    each(0, COMM // 2, first)

    received(meta_in())
    aside = lax.rem(b, 2)
    for t in range(2):
        pieces = []
        for r in (2 * t, 2 * t + 1):
            tile = meta[r, :, pl.ds(pl.multiple_of(lax.div(b, 2) * lanes, lanes), lanes)]
            pieces.append(jnp.where(aside == r % 2, tile, pltpu.roll(tile, width, 1)))
        bmeta[:, t * lanes : (t + 1) * lanes] = jnp.where(low[0:16], pieces[0], pieces[1])

    received(row_in(0))
    slots = lax.broadcasted_iota(jnp.int32, (cells, points), 0).astype(F32)
    for q in range(TEAM + 2):
        owner = (wrap(base - 1 + q) * cells).astype(F32)
        value = jnp.zeros((cells, points), F32)
        for j in range(4):
            value = value + jnp.where(bmeta[j : j + 1, :] - owner == slots, bmeta[4 + j : 5 + j, :], 0.0)
        ptab[0, q * cells : (q + 1) * cells, :], ptab[1, q * cells : (q + 1) * cells, :] = split(value)

    shift = lax.rem(cells + window // 2 - window * b, cells)
    pointer = lax.broadcasted_iota(jnp.int32, (width, cells), 0).astype(F32)
    for t in range((TEAM + 2) // 2):
        near = pltpu.roll(orx[2 * t, 0:8], shift, 1)
        far = pltpu.roll(orx[2 * t + 1, 0:8], shift, 1)
        both = jnp.where(low[0:8], near, pltpu.roll(far, width, 1))
        for r in range(TEAM):
            origin = ((base + r) * points + width * b).astype(F32)
            value = jnp.zeros((width, cells), F32)
            for j in range(4):
                value = value + jnp.where(both[j : j + 1, :] - origin == pointer, both[4 + j : 5 + j, :], 0.0)
            high_part, low_part = split(value)
            btab[0, r * width : (r + 1) * width, t * lanes : (t + 1) * lanes] = high_part
            btab[1, r * width : (r + 1) * width, t * lanes : (t + 1) * lanes] = low_part

    received(edges_in())
    lane_rim = lax.broadcasted_iota(jnp.int32, (size // 2, lanes), 1)
    turn4 = lax.rem(lane_rim, 4)
    upper = lane_rim >= width - 1

    def pick(values):
        return jnp.where(b == 0, values[0], jnp.where(b == 1, values[1], jnp.where(b == 2, values[2], values[3])))

    last = width - 1
    from_left = pick((1, last, lanes - 1, last + 2))
    from_right = pick((width, 2, width + 2, 0))
    to_left = (last, lanes - 1, last + 2, 1)
    to_right = (0, width, 2, width + 2)
    on_left = (
        (turn4 == 3) & upper & (lane_rim < lanes - 1),
        (turn4 == 3) & ((lane_rim < width - 1) | (lane_rim == lanes - 1)),
        (turn4 == 1) & upper,
        (turn4 == 1) & ~upper,
    )
    on_right = ((turn4 == 0) & ~upper, (turn4 == 0) & upper, (turn4 == 2) & ~upper, (turn4 == 2) & upper)
    merged = jnp.zeros((size // 2, lanes), F32)
    for r in range(TEAM):
        merged = jnp.where(on_left[r], pltpu.roll(exin[r], lax.rem(to_left[r] - from_left + lanes, lanes), 1), merged)
        merged = jnp.where(on_right[r], pltpu.roll(exin[r], lax.rem(to_right[r] - from_right + lanes, lanes), 1), merged)
    edge[0] = merged

    def flow(step):
        for q in range(TEAM + 2):
            sall[:, q * cells : (q + 1) * cells] = orx[q, 8:16] if step == 0 else srx[q]
        tan[...] = jnp.tanh(dot_split(sall[...], ptab[0], ptab[1]))

    flow(0)

    lane_half = lax.rem(lane, width)
    at_first, at_last = lane_half == 0, lane_half == width - 1

    def advect(step, c):
        received(halo(step, c))
        rim_row = edge[step, span(c, 8), :]
        out = []
        for sub in range(2):
            at = pl.ds(pl.multiple_of(c * size + sub * half, half), half)
            col = cols[at, :]
            if step == 0:
                join = odd if sub else even
                own = [join(rx[0, 2 * t, halves(c), :], rx[0, 2 * t + 1, halves(c), :]) for t in range(2)]
            else:
                own = [mid[at, t * lanes : (t + 1) * lanes] for t in range(2)]
            turned = [pltpu.roll(x, width, 1) for x in own]
            below, above = zin[step, 0, halves(c), :], zin[step, 1, halves(c), :]
            if sub:
                below = pltpu.roll(below, width, 1)
            else:
                above = pltpu.roll(above, width, 1)
            middle = jnp.where(low, turned[0], turned[1])
            north = (jnp.where(low, below, turned[0]), middle)
            south = (middle, jnp.where(low, turned[1], above))
            groups = range(sub * half // 8, (sub + 1) * half // 8)
            spin = [
                jnp.concatenate([pltpu.roll(rim_row, (k - 4 * g) % lanes, 1) for g in groups], axis=0)
                for k in (width + 1, width - 1, width - 3)
            ]
            sense_x, sense_y = col[:, 2:3], col[:, 3:4]
            values = []
            for t in range(2):
                x = own[t]
                west = jnp.where(at_first, spin[t], pltpu.roll(x, 1, 1))
                east = jnp.where(at_last, spin[t + 1], pltpu.roll(x, lanes - 1, 1))
                behind_x = jnp.where(sense_x > 0, west, east)
                behind_y = jnp.where(sense_y > 0, north[t], south[t])
                lane_at = slice(t * lanes, (t + 1) * lanes)
                speed_x = col[:, 0:1] * (1.0 + 0.5 * (sense_x * tan[0:1, lane_at]))
                speed_y = col[:, 1:2] * (1.0 + 0.5 * (sense_y * tan[1:2, lane_at]))
                values.append(x - speed_x * (x - behind_x) - speed_y * (x - behind_y))
            out.append(values)
        return out

    def keep(c, values):
        for sub in range(2):
            at = pl.ds(pl.multiple_of(c * size + sub * half, half), half)
            for t in range(2):
                adv[at, t * lanes : (t + 1) * lanes] = values[sub][t]
                advb[at, t * lanes : (t + 1) * lanes] = values[sub][t].astype(BF16)

    deep = comps // KPARTS

    def multiply(part):
        k_at = slice(part * deep, (part + 1) * deep)

        def body(i):
            j, at = lax.div(i, KPARTS), span(lax.rem(i, KPARTS), deep)
            value = dot(quad[j, at, k_at], advb[k_at, :])
            if part:
                value = value + acc[j, at, :]
            acc[j, at, :] = value

        each(0, 4 * KPARTS, body)

    def source(step, wet_row):
        target = mid if step == 0 else spec_out
        k_at = slice(comps - deep, comps)

        def body(c):
            at = rows(c)
            terms = [acc[j, at, :] + dot(quad[j, at, k_at], advb[k_at, :]) for j in range(4)]
            value = adv[at, :]
            total_sum = terms[0] + terms[1] + terms[2] + terms[3]
            pair_sum = terms[0] * terms[1] + terms[2] * terms[3]
            new = wet_row * (value + cols[at, 4:5] * (value * value * total_sum - value * pair_sum))
            target[at, :] = new
            midb[at, :] = new.astype(BF16)
            if step == 0:
                ex[1, span(c, 8), :] = pack_rim(new[:, 0:lanes], new[:, lanes : 2 * lanes])
                zpk[0, halves(c), :] = odd(new[0:half, lanes : 2 * lanes], new[half:size, lanes : 2 * lanes])
                zpk[1, halves(c), :] = even(new[0:half, 0:lanes], new[half:size, 0:lanes])

        each(0, COMM, body)

    level_row = lax.broadcasted_iota(jnp.int32, (levels, cells), 0)

    def mix(w):
        above = jnp.where(level_row == 0, w, pltpu.roll(w, 1, 0))
        below = jnp.where(level_row == levels - 1, w, pltpu.roll(w, levels - 1, 0))
        return level_mix * (above - 2.0 * w + below)

    def ocean(step, drift):
        before = currents if step == 0 else state
        target = state if step == 0 else cur_out
        received(zonal_pair(step))
        u, v = before[0], before[1]
        rot = coriolis[...]
        turn = 0.5 * (pltpu.roll(v, cells - 1, 1) - pltpu.roll(v, 1, 1)) - 0.5 * (zhalo[step, 1] - zhalo[step, 0])
        mix_u, mix_v = mix(u), mix(v)
        drift_x, drift_y = drift()
        target[0] = u + OCEAN_STEP * (rot * (v + drift_y) + turn * drift_y + mix_u)
        target[1] = v + OCEAN_STEP * (-rot * (u + drift_x) - turn * drift_x + mix_v)

    for c in range(COMM // 2):
        forward(COMM // 2 + c)
        if c < 2:
            for k in (2 * c, 2 * c + 1):
                keep(k, advect(0, k))
            multiply(c)
        else:
            keep(c + 2, advect(0, c + 2))
    multiply(2)

    oslots = lax.broadcasted_iota(jnp.int32, (points, cells), 0).astype(F32)
    origin = (pos * points).astype(F32)
    for q in range(3):
        value = jnp.zeros((points, cells), F32)
        for j in range(4):
            value = value + jnp.where(
                orx[b + q, j : j + 1, :] - origin == oslots, orx[b + q, 4 + j : 5 + j, :], 0.0
            )
        otab[q, 0], otab[q, 1] = split(value)

    for c in (COMM - 2, COMM - 1):
        keep(c, advect(0, c))
    source(0, bmeta[8:9, :])

    stokes = dot(table[...], midb[...])
    parts = dot_split(stokes, btab[0], btab[1])
    for t in range((TEAM + 2) // 2):
        zonal = parts[0:levels, t * lanes : (t + 1) * lanes]
        merid = parts[levels : 2 * levels, t * lanes : (t + 1) * lanes]
        dm[2 * t], dm[2 * t + 1] = even(zonal, merid), odd(zonal, merid)
    start(drift_out())
    drx[b] = dm[b + 1]
    start(sides())
    each(0, 3, lambda c: start(halo(1, c)))

    def team_drift():
        inner, outer = drift_in()
        received(inner)

        @pl.when((b == 0) | (b == TEAM - 1))
        def _():
            received(outer)

        drift_x = jnp.zeros((levels, cells), F32)
        drift_y = jnp.zeros((levels, cells), F32)
        for s in range(TEAM):
            part = drx[s] + drx[TEAM + s]
            to = (window * s - window // 2) % cells
            drift_x += pltpu.roll(jnp.where(low, part, 0.0), to, 1)
            drift_y += pltpu.roll(jnp.where(low, pltpu.roll(part, width, 1), 0.0), to, 1)
        return drift_x, drift_y

    ocean(0, team_drift)
    surface(state, sbuf, 0)
    row_start(1)
    srx[b + 1] = sbuf[...]
    each(3, COMM, lambda c: start(halo(1, c)))
    received(sides())
    edge[1] = jnp.where(lax.rem(lane_rim, 2) == 1, exin[TEAM], exin[TEAM + 1])
    received(row_in(1))
    flow(1)

    def give(c):
        values = advect(1, c)
        for t in range(2):
            pk2[2 * t, halves(c), :] = even(values[0][t], values[1][t])
            pk2[2 * t + 1, halves(c), :] = odd(values[0][t], values[1][t])
        start(piece_out(1, c))
        rx[1, b, halves(c), :] = pk2[b, halves(c), :]

    def take(c):
        received(piece_in(1, c))
        values = []
        for join in (even, odd):
            values.append([join(rx[1, 2 * t, halves(c), :], rx[1, 2 * t + 1, halves(c), :]) for t in range(2)])
        keep(c, values)

    each(0, 3, give)
    for c in range(3, COMM):
        give(c)
        take(c - 3)
        if c == COMM - 1:
            start(zonal_pair(1))
        if (c - 3) % 2:
            multiply((c - 3) // 2)
    take(COMM - 3)
    multiply(2)
    take(COMM - 2)
    take(COMM - 1)
    source(1, wet[...].astype(F32))

    stokes = dot(table[...], midb[...])
    copies = last_pair()
    dbuf[0] = dot_split(stokes, otab[2, 0], otab[2, 1])
    copies[0].start()
    dbuf[1] = dot_split(stokes, otab[0, 0], otab[0, 1])
    copies[1].start()
    dself[...] = dot_split(stokes, otab[1, 0], otab[1, 1])

    def last_drift():
        received(last_pair())
        drift = dself[...] + dhalo[0] + dhalo[1]
        return drift[0:levels], drift[levels : 2 * levels]

    ocean(1, last_drift)

    sent(meta_out())
    sent(edges_out())
    sent(sides())
    sent(drift_out())
    sent(last_pair())
    for step in range(STEPS):
        row_sent(step)
        sent(zonal_pair(step))
        each(0, COMM, lambda c: sent(piece_out(step, c)))
        each(0, COMM, lambda c: sent(halo(step, c)))


def local(
    spectrum, water_mask, courant, stencil_sign, quad_index, quad_weight, nonlinear, stokes_table,
    point_index, point_weight, ocean_index, ocean_weight, currents, coriolis, mixing, surface_weights,
):
    comps, points = spectrum.shape
    levels, cells = currents.shape[1:]
    lanes = points // 2
    packed = comps // 2
    rim = comps // 16
    vm = pl.BlockSpec(memory_space=pltpu.VMEM)
    dma = pltpu.SemaphoreType.DMA

    def f32(*shape):
        return pltpu.VMEM(shape, F32)

    def bf16(*shape):
        return pltpu.VMEM(shape, BF16)

    scratch = [
        f32(128, comps),
        f32(comps, 128),
        f32(128, 128),
        bf16(4, comps, comps),
        f32(TEAM, packed, lanes),
        f32(TEAM, packed, lanes),
        f32(STEPS, TEAM, packed, lanes),
        f32(2, packed, lanes),
        f32(STEPS, 2, packed, lanes),
        f32(STEPS, rim, lanes),
        f32(TEAM + 2, rim, lanes),
        f32(STEPS, rim, lanes),
        f32(comps, points),
        bf16(comps, points),
        f32(4, comps, points),
        f32(comps, points),
        bf16(comps, points),
        f32(2, levels, cells),
        f32(16, points),
        f32(TEAM, 16, points),
        f32(16, points),
        f32(16, cells),
        f32(TEAM + 2, 16, cells),
        f32(8, cells),
        f32(TEAM + 2, 8, cells),
        f32(8, (TEAM + 2) * cells),
        f32(STEPS, 2, levels, cells),
        bf16(2, (TEAM + 2) * cells, points),
        bf16(2, points, (TEAM + 2) // 2 * lanes),
        bf16(3, 2, points, cells),
        f32(TEAM + 2, levels, lanes),
        f32(2 * TEAM, levels, lanes),
        f32(2, 2 * levels, cells),
        f32(2, 2 * levels, cells),
        f32(2 * levels, cells),
        f32(8, points),
        dma((STEPS, 3, COMM)),
        dma((STEPS, TEAM, COMM)),
        dma((STEPS, 2, COMM)),
        dma((STEPS, 2, COMM)),
        dma((3,)),
        dma((TEAM,)),
        dma((2,)),
        dma((2,)),
        dma((3,)),
        dma((TEAM,)),
        dma((3 + TEAM,)),
        dma((TEAM + 2,)),
        dma((3 + TEAM,)),
        dma((TEAM + 2,)),
        dma((5,)),
        dma((2 * TEAM,)),
        dma((STEPS, 2)),
        dma((STEPS, 2)),
        dma((2,)),
        dma((2,)),
    ]
    return pl.pallas_call(
        wave_kernel,
        out_shape=(
            pltpu.VMEM((comps, points), F32),
            pltpu.VMEM(currents.shape, F32),
        ),
        in_specs=[vm] * 16,
        out_specs=(vm, vm),
        scratch_shapes=scratch,
        compiler_params=pltpu.CompilerParams(
            collective_id=0, has_side_effects=True, vmem_limit_bytes=56 * 1024 * 1024
        ),
    )(
        spectrum,
        water_mask.reshape(1, points),
        courant,
        stencil_sign,
        quad_index.transpose(0, 2, 1),
        quad_weight.transpose(0, 2, 1),
        nonlinear.reshape(1, comps),
        stokes_table,
        point_index,
        point_weight,
        ocean_index,
        ocean_weight,
        currents,
        coriolis.reshape(1, cells),
        mixing.reshape(1, levels),
        surface_weights.reshape(1, levels),
    )


def solution(mesh):
    ring = P(("mp", "dev"))
    split_last = P(None, ("mp", "dev"))
    deep = P(None, None, ("mp", "dev"))
    return jax.shard_map(
        local,
        mesh=mesh,
        in_specs=(
            split_last, ring, P(), P(), P(), P(), P(), P(), split_last, split_last, split_last, split_last, deep,
            ring, P(), P(),
        ),
        out_specs=(split_last, deep),
        check_vma=False,
    )
```

```python
import jax
import jax.numpy as jnp
from jax import lax
from jax.experimental import pallas as pl
from jax.experimental.pallas import tpu as pltpu
from jax.sharding import PartitionSpec as P

STEPS = 2
OCEAN_STEP = 0.5
TEAM = 4
COMM = 8
KPARTS = 4
MESH = pl.DeviceIdType.MESH
F32, BF16 = jnp.float32, jnp.bfloat16


def split(x):
    high = x.astype(BF16)
    return high, (x - high.astype(F32)).astype(BF16)


def dot(a, b):
    return jnp.dot(a, b, preferred_element_type=F32)


def dot_split(x, table_high, table_low):
    high, low = split(x)
    return dot(high, table_high) + (dot(low, table_high) + dot(high, table_low))


def wave_kernel(
    spec, wet, courant, sign, qidx, qwt, nonlinear, table, pidx, pwt, oidx, owt,
    currents, coriolis, mixing, sweight,
    spec_out, cur_out,
    araw, cols, lraw, quad, pk, pk2, rx, zpk, zin, ex, exin, edge, adv, advb, acc, mid, midb, state,
    mbuf, meta, bmeta, osm, orx, sbuf, srx, sall, zhalo, ptab, btab, otab, dm, drx, dbuf, dhalo, dself, tan,
    rxs, rxr, zs, zr, es, er, fs, fr, ms, mr, os_, or_, ss, sr, ds_, dr, us, ur, hs, hr,
):
    comps, points = spec.shape
    cells = coriolis.shape[1]
    levels = mixing.shape[1]
    dev_count = lax.axis_size("dev")
    total = lax.axis_size("mp") * dev_count
    pos = lax.axis_index("mp") * dev_count + lax.axis_index("dev")
    b = lax.rem(pos, TEAM)
    base = pos - b
    width = points // TEAM
    window = cells // TEAM
    size = comps // COMM
    half = size // 2
    lanes = 2 * width

    none = lax.div(pos, total)

    def wrap(p):
        return lax.rem(p + total, total)

    up, down = wrap(pos + 1), wrap(pos - 1)
    ahead, behind = wrap(pos + TEAM), wrap(pos - TEAM)
    mates = [lax.rem(b + i, TEAM) for i in range(1, TEAM)]

    def remote(src, dst, ssem, rsem, p):
        return pltpu.make_async_remote_copy(
            src_ref=src, dst_ref=dst, send_sem=ssem, recv_sem=rsem,
            device_id=(lax.div(p, dev_count), lax.rem(p, dev_count)), device_id_type=MESH,
        )

    def span(c, n):
        return pl.ds(pl.multiple_of(c * n, n), n)

    def rows(c):
        return span(c, size)

    def halves(c):
        return span(c, half)

    def each(low, high, body):
        def run(c, carry):
            body(c)
            return carry

        lax.fori_loop(low, high, run, 0)

    def start(copies):
        for copy in copies:
            copy.start()

    def received(copies):
        for copy in copies:
            copy.wait_recv()

    def sent(copies):
        for copy in copies:
            copy.wait_send()

    def piece_out(step, c):
        src = pk if step == 0 else pk2
        return [
            remote(src.at[d, halves(c)], rx.at[step, b, halves(c)], rxs.at[step, i], rxr.at[step, b, c], base + d)
            for i, d in enumerate(mates)
        ]

    def piece_in(step, c):
        src = pk if step == 0 else pk2
        return [
            remote(src.at[d, halves(c)], rx.at[step, d, halves(c)], rxs.at[step, i], rxr.at[step, d, c], base + d)
            for i, d in enumerate(mates)
        ]

    def halo(step, c):
        low = rx.at[0, TEAM - 1, halves(c)] if step == 0 else zpk.at[0, halves(c)]
        high = rx.at[0, 0, halves(c)] if step == 0 else zpk.at[1, halves(c)]
        return [
            remote(low, zin.at[step, 0, halves(c)], zs.at[step, 0], zr.at[step, 0, c], ahead),
            remote(high, zin.at[step, 1, halves(c)], zs.at[step, 1], zr.at[step, 1, c], behind),
        ]

    def all_out(step):
        src = pk if step == 0 else pk2
        copies = [
            remote(src.at[d], rx.at[step, b], rxs.at[step, i], rxr.at[step, b, 0], base + d)
            for i, d in enumerate(mates)
        ]
        low_from = rx.at[0, TEAM - 1] if step == 0 else zpk.at[0]
        high_from = rx.at[0, 0] if step == 0 else zpk.at[1]
        copies.append(remote(low_from, zin.at[step, 0], zs.at[step, 0], zr.at[step, 0, 0], ahead))
        copies.append(remote(high_from, zin.at[step, 1], zs.at[step, 1], zr.at[step, 1, 0], behind))
        return copies

    def edges_out():
        return [remote(ex.at[0], exin.at[b], es.at[i], er.at[b], base + d) for i, d in enumerate(mates)]

    def edges_in():
        return [remote(ex.at[0], exin.at[d], es.at[i], er.at[d], base + d) for i, d in enumerate(mates)]

    right, left = base + mates[0], base + mates[2]

    def sides():
        return [
            remote(ex.at[1], exin.at[TEAM], fs.at[0], fr.at[0], right),
            remote(ex.at[1], exin.at[TEAM + 1], fs.at[1], fr.at[1], left),
        ]

    def meta_out():
        return [remote(mbuf, meta.at[b], ms.at[i], mr.at[b], base + d) for i, d in enumerate(mates)]

    def meta_in():
        return [remote(mbuf, meta.at[d], ms.at[i], mr.at[d], base + d) for i, d in enumerate(mates)]

    def row_out(step):
        src, dst, ssem, rsem = (osm, orx, os_, or_) if step == 0 else (sbuf, srx, ss, sr)
        inner = [remote(src, dst.at[b + 1], ssem.at[i], rsem.at[b + 1], base + d) for i, d in enumerate(mates)]
        before = [
            remote(src, dst.at[TEAM + 1], ssem.at[3 + k], rsem.at[TEAM + 1], wrap(base - TEAM + k)) for k in range(TEAM)
        ]
        after = [remote(src, dst.at[0], ssem.at[3 + k], rsem.at[0], wrap(base + TEAM + k)) for k in range(TEAM)]
        return inner, before, after

    def row_start(step):
        inner, before, after = row_out(step)

        @pl.when(b == 0)
        def _():
            start(before)

        @pl.when(b == TEAM - 1)
        def _():
            start(after)

        start(inner)

    def row_sent(step):
        inner, before, after = row_out(step)
        sent(inner)

        @pl.when(b == 0)
        def _():
            sent(before)

        @pl.when(b == TEAM - 1)
        def _():
            sent(after)

    def row_in(step):
        src, dst, ssem, rsem = (osm, orx, os_, or_) if step == 0 else (sbuf, srx, ss, sr)
        copies = [remote(src, dst.at[d + 1], ssem.at[i], rsem.at[d + 1], base + d) for i, d in enumerate(mates)]
        copies.append(remote(src, dst.at[0], ssem.at[0], rsem.at[0], ahead))
        copies.append(remote(src, dst.at[TEAM + 1], ssem.at[0], rsem.at[TEAM + 1], behind))
        return copies

    def drift_out():
        copies = [
            remote(dm.at[0], drx.at[TEAM + b], ds_.at[3], dr.at[TEAM + b], wrap(base - 1)),
            remote(dm.at[TEAM + 1], drx.at[TEAM + b], ds_.at[4], dr.at[TEAM + b], wrap(base + TEAM)),
        ]
        return copies + [
            remote(dm.at[d + 1], drx.at[b], ds_.at[i], dr.at[b], base + d) for i, d in enumerate(mates)
        ]

    def drift_in():
        inner = [remote(dm.at[0], drx.at[d], ds_.at[i], dr.at[d], base + d) for i, d in enumerate(mates)]
        outer = [remote(dm.at[0], drx.at[TEAM + k], ds_.at[3], dr.at[TEAM + k], ahead) for k in range(TEAM)]
        return inner, outer

    def zonal_pair(step):
        src = currents.at[0] if step == 0 else state.at[0]
        return [
            remote(src, zhalo.at[step, 0], us.at[step, 0], ur.at[step, 0], up),
            remote(src, zhalo.at[step, 1], us.at[step, 1], ur.at[step, 1], down),
        ]

    def last_pair():
        return [
            remote(dbuf.at[0], dhalo.at[0], hs.at[0], hr.at[0], up),
            remote(dbuf.at[1], dhalo.at[1], hs.at[1], hr.at[1], down),
        ]

    drx[TEAM : 2 * TEAM] = jnp.zeros((TEAM, levels, lanes), F32)
    barrier = pltpu.get_barrier_semaphore()
    partners = [base + d for d in mates]
    partners += [wrap(base - TEAM + k) for k in range(TEAM)] + [wrap(base + TEAM + k) for k in range(TEAM)]
    for p in partners:
        pl.semaphore_signal(
            barrier, inc=1, device_id=(lax.div(p, dev_count), lax.rem(p, dev_count)), device_id_type=MESH
        )

    lane = lax.broadcasted_iota(jnp.int32, (half, lanes), 1)
    low = lane < width

    def even(a, c):
        return jnp.where(low, a, pltpu.roll(c, width, 1))

    def odd(a, c):
        return jnp.where(low, pltpu.roll(a, width, 1), c)

    lane_row = lax.broadcasted_iota(jnp.int32, (8, lanes), 1)
    wide_lane = lax.broadcasted_iota(jnp.int32, (size, lanes), 1)
    rim = lax.rem(wide_lane + 1, width) < 2

    def pack_rim(first, second):
        mixed = jnp.where(rim, first, pltpu.roll(second, 2, 1))
        out = jnp.zeros((8, lanes), F32)
        for g in range(size // 8):
            here = lax.rem(lane_row + 1 - 4 * g + lanes, width) < 4
            part = mixed[8 * g : 8 * g + 8]
            out = jnp.where(here, pltpu.roll(part, 4 * g, 1) if g else part, out)
        return out

    lraw[...] = jnp.zeros_like(lraw)
    lraw[0:1, 0:levels] = mixing[...]
    lraw[1:2, 0:levels] = sweight[...]
    lcols = jnp.transpose(lraw[...])
    level_mix = lcols[0:levels, 0:1]
    level_weight = lcols[0:levels, 1:2]

    def surface(source, dst, at):
        dst[at : at + 8, :] = jnp.zeros((8, cells), F32)
        for a in range(2):
            dst[at + a : at + a + 1, :] = jnp.sum(level_weight * source[a], axis=0, keepdims=True)

    osm[0:4, :] = oidx[...].astype(F32)
    osm[4:8, :] = owt[...]
    surface(currents, osm, 8)
    orx[b + 1] = osm[...]
    mbuf[...] = jnp.zeros_like(mbuf)
    mbuf[0:4, :] = pidx[...].astype(F32)
    mbuf[4:8, :] = pwt[...]
    mbuf[8:9, :] = wet[...].astype(F32)
    meta[b] = mbuf[...]

    def pack_in(c):
        for t in range(2):
            tile = spec[rows(c), t * lanes : (t + 1) * lanes]
            first, second = tile[0:half], tile[half:size]
            pk[2 * t, halves(c), :] = even(first, second)
            pk[2 * t + 1, halves(c), :] = odd(first, second)
        rx[0, b, halves(c), :] = pk[b, halves(c), :]
        start(piece_out(0, c))

    def rim_in(c):
        ex[0, span(c, 8), :] = pack_rim(spec[rows(c), 0:lanes], spec[rows(c), lanes : 2 * lanes])

    each(0, COMM, rim_in)
    exin[b] = ex[0]
    pl.semaphore_wait(barrier, len(partners))

    each(0, 1, pack_in)
    row_start(0)
    start(meta_out())
    each(1, 2, pack_in)
    start(edges_out())
    each(2, COMM, pack_in)
    start(zonal_pair(0))
    araw[...] = jnp.zeros_like(araw)
    araw[0:2, :] = courant[...]
    araw[2:4, :] = (2 * sign[...] - 1).astype(F32)
    araw[4:5, :] = nonlinear[...]
    for j in range(4):
        index, weight = qidx[j], qwt[j]
        twice = index[0:1] == index[1:2]
        araw[8 + 2 * j : 10 + 2 * j, :] = index.astype(F32)
        araw[16 + 2 * j : 17 + 2 * j, :] = jnp.where(twice, weight[0:1] + weight[1:2], weight[0:1])
        araw[17 + 2 * j : 18 + 2 * j, :] = weight[1:2]
    cols[...] = jnp.transpose(araw[...])
    long_lane = lax.broadcasted_iota(jnp.int32, (32, comps), 1).astype(F32)

    def build_quad(c):
        for sub in range(size // 32):
            begin = pl.multiple_of(c * size + sub * 32, 32)
            col = cols[pl.ds(begin, 32), :]
            for j in range(4):
                two = jnp.where(col[:, 9 + 2 * j : 10 + 2 * j] == long_lane, col[:, 17 + 2 * j : 18 + 2 * j], 0.0)
                one = jnp.where(col[:, 8 + 2 * j : 9 + 2 * j] == long_lane, col[:, 16 + 2 * j : 17 + 2 * j], two)
                quad[pl.ds(begin + j * comps, 32), :] = one.astype(BF16)

    def forward(c):
        received(piece_in(0, c))
        start(halo(0, c))

    each(0, COMM // 2, build_quad)
    forward(0)
    each(COMM // 2, COMM - 1, build_quad)
    forward(1)
    each(COMM - 1, COMM, build_quad)
    received(meta_in())
    aside = lax.rem(b, 2)
    for t in range(2):
        pieces = []
        for r in (2 * t, 2 * t + 1):
            tile = meta[r, :, pl.ds(pl.multiple_of(lax.div(b, 2) * lanes, lanes), lanes)]
            pieces.append(jnp.where(aside == r % 2, tile, pltpu.roll(tile, width, 1)))
        bmeta[:, t * lanes : (t + 1) * lanes] = jnp.where(low[0:16], pieces[0], pieces[1])

    received(row_in(0))
    slots = lax.broadcasted_iota(jnp.int32, (cells, points), 0).astype(F32)
    for q in range(TEAM + 2):
        owner = (wrap(base - 1 + q) * cells).astype(F32)
        value = jnp.zeros((cells, points), F32)
        for j in range(4):
            value = value + jnp.where(bmeta[j : j + 1, :] - owner == slots, bmeta[4 + j : 5 + j, :], 0.0)
        ptab[0, q * cells : (q + 1) * cells, :], ptab[1, q * cells : (q + 1) * cells, :] = split(value)

    shift = lax.rem(cells + window // 2 - window * b, cells)
    pointer = lax.broadcasted_iota(jnp.int32, (width, cells), 0).astype(F32)
    for t in range((TEAM + 2) // 2):
        near = pltpu.roll(orx[2 * t, 0:8], shift, 1)
        far = pltpu.roll(orx[2 * t + 1, 0:8], shift, 1)
        both = jnp.where(low[0:8], near, pltpu.roll(far, width, 1))
        for r in range(TEAM):
            origin = ((base + r) * points + width * b).astype(F32)
            value = jnp.zeros((width, cells), F32)
            for j in range(4):
                value = value + jnp.where(both[j : j + 1, :] - origin == pointer, both[4 + j : 5 + j, :], 0.0)
            high_part, low_part = split(value)
            btab[0, r * width : (r + 1) * width, t * lanes : (t + 1) * lanes] = high_part
            btab[1, r * width : (r + 1) * width, t * lanes : (t + 1) * lanes] = low_part

    forward(2)
    received(edges_in())
    lane_rim = lax.broadcasted_iota(jnp.int32, (size // 2, lanes), 1)
    turn4 = lax.rem(lane_rim, 4)
    upper = lane_rim >= width - 1

    def pick(values):
        return jnp.where(b == 0, values[0], jnp.where(b == 1, values[1], jnp.where(b == 2, values[2], values[3])))

    last = width - 1
    from_left = pick((1, last, lanes - 1, last + 2))
    from_right = pick((width, 2, width + 2, 0))
    to_left = (last, lanes - 1, last + 2, 1)
    to_right = (0, width, 2, width + 2)
    on_left = (
        (turn4 == 3) & upper & (lane_rim < lanes - 1),
        (turn4 == 3) & ((lane_rim < width - 1) | (lane_rim == lanes - 1)),
        (turn4 == 1) & upper,
        (turn4 == 1) & ~upper,
    )
    on_right = ((turn4 == 0) & ~upper, (turn4 == 0) & upper, (turn4 == 2) & ~upper, (turn4 == 2) & upper)
    merged = jnp.zeros((size // 2, lanes), F32)
    for r in range(TEAM):
        merged = jnp.where(on_left[r], pltpu.roll(exin[r], lax.rem(to_left[r] - from_left + lanes, lanes), 1), merged)
        merged = jnp.where(on_right[r], pltpu.roll(exin[r], lax.rem(to_right[r] - from_right + lanes, lanes), 1), merged)
    edge[0] = merged

    def flow(step):
        for q in range(TEAM + 2):
            sall[:, q * cells : (q + 1) * cells] = orx[q, 8:16] if step == 0 else srx[q]
        tan[...] = jnp.tanh(dot_split(sall[...], ptab[0], ptab[1]))

    flow(0)

    lane_half = lax.rem(lane, width)
    at_first, at_last = lane_half == 0, lane_half == width - 1

    unit = half // 2
    low_unit = low[0:unit]
    at_first, at_last = at_first[0:unit], at_last[0:unit]

    def advect(step, c, emit):
        received(halo(step, c))

        def body(r):
            packed = pl.ds(pl.multiple_of(c * half + r * unit, unit), unit)
            turn = lax.rem(lanes - 4 * (unit // 8) * r, lanes)
            rim_row = pltpu.roll(edge[step, span(c, 8), :], turn, 1)
            out = []
            for sub in range(2):
                at = pl.ds(pl.multiple_of(c * size + sub * half + r * unit, unit), unit)
                col = cols[at, :]
                if step == 0:
                    own = []
                    for t in range(2):
                        a, d = rx[0, 2 * t, packed, :], rx[0, 2 * t + 1, packed, :]
                        if sub:
                            own.append(jnp.where(low_unit, pltpu.roll(a, width, 1), d))
                        else:
                            own.append(jnp.where(low_unit, a, pltpu.roll(d, width, 1)))
                else:
                    own = [mid[at, t * lanes : (t + 1) * lanes] for t in range(2)]
                turned = [pltpu.roll(x, width, 1) for x in own]
                below, above = zin[step, 0, packed, :], zin[step, 1, packed, :]
                if sub:
                    below = pltpu.roll(below, width, 1)
                else:
                    above = pltpu.roll(above, width, 1)
                middle = jnp.where(low_unit, turned[0], turned[1])
                north = (jnp.where(low_unit, below, turned[0]), middle)
                south = (middle, jnp.where(low_unit, turned[1], above))
                groups = range(sub * half // 8, sub * half // 8 + unit // 8)
                spin = [
                    jnp.concatenate([pltpu.roll(rim_row, (k - 4 * g) % lanes, 1) for g in groups], axis=0)
                    for k in (width + 1, width - 1, width - 3)
                ]
                sense_x, sense_y = col[:, 2:3], col[:, 3:4]
                values = []
                for t in range(2):
                    x = own[t]
                    west = jnp.where(at_first, spin[t], pltpu.roll(x, 1, 1))
                    east = jnp.where(at_last, spin[t + 1], pltpu.roll(x, lanes - 1, 1))
                    behind_x = jnp.where(sense_x > 0, west, east)
                    behind_y = jnp.where(sense_y > 0, north[t], south[t])
                    lane_at = slice(t * lanes, (t + 1) * lanes)
                    speed_x = col[:, 0:1] * (1.0 + 0.5 * (sense_x * tan[0:1, lane_at]))
                    speed_y = col[:, 1:2] * (1.0 + 0.5 * (sense_y * tan[1:2, lane_at]))
                    values.append(x - speed_x * (x - behind_x) - speed_y * (x - behind_y))
                out.append(values)
            emit(c, r, out)

        each(0, half // unit, body)

    def keep(c, r, values):
        for sub in range(2):
            at = pl.ds(pl.multiple_of(c * size + sub * half + r * unit, unit), unit)
            for t in range(2):
                adv[at, t * lanes : (t + 1) * lanes] = values[sub][t]
                advb[at, t * lanes : (t + 1) * lanes] = values[sub][t].astype(BF16)

    deep = comps // KPARTS

    def multiply(part):
        k_at = slice(part * deep, (part + 1) * deep)

        def body(i):
            if part:
                acc[...] = acc[...] + dot(quad[:, k_at], advb[k_at, :])
            else:
                acc[...] = dot(quad[:, k_at], advb[k_at, :])

        each(none, none + 1, body)

    def source(step, wet_row):
        target = mid if step == 0 else spec_out

        def body(c):
            at = rows(c)
            terms = [acc[pl.ds(pl.multiple_of(j * comps + c * size, size), size), :] for j in range(4)]
            value = adv[at, :]
            total_sum = terms[0] + terms[1] + terms[2] + terms[3]
            pair_sum = terms[0] * terms[1] + terms[2] * terms[3]
            new = wet_row * (value + cols[at, 4:5] * (value * value * total_sum - value * pair_sum))
            target[at, :] = new
            midb[at, :] = new.astype(BF16)
            if step == 0:
                ex[1, span(c, 8), :] = pack_rim(new[:, 0:lanes], new[:, lanes : 2 * lanes])
                zpk[0, halves(c), :] = odd(new[0:half, lanes : 2 * lanes], new[half:size, lanes : 2 * lanes])
                zpk[1, halves(c), :] = even(new[0:half, 0:lanes], new[half:size, 0:lanes])

        each(0, COMM, body)

    level_row = lax.broadcasted_iota(jnp.int32, (levels, cells), 0)

    def mix(w):
        above = jnp.where(level_row == 0, w, pltpu.roll(w, 1, 0))
        below = jnp.where(level_row == levels - 1, w, pltpu.roll(w, levels - 1, 0))
        return level_mix * (above - 2.0 * w + below)

    def ocean(step, drift):
        before = currents if step == 0 else state
        target = state if step == 0 else cur_out
        received(zonal_pair(step))
        u, v = before[0], before[1]
        rot = coriolis[...]
        turn = 0.5 * (pltpu.roll(v, cells - 1, 1) - pltpu.roll(v, 1, 1)) - 0.5 * (zhalo[step, 1] - zhalo[step, 0])
        mix_u, mix_v = mix(u), mix(v)
        drift_x, drift_y = drift()
        target[0] = u + OCEAN_STEP * (rot * (v + drift_y) + turn * drift_y + mix_u)
        target[1] = v + OCEAN_STEP * (-rot * (u + drift_x) - turn * drift_x + mix_v)

    oslots = lax.broadcasted_iota(jnp.int32, (points, cells), 0).astype(F32)
    origin = (pos * points).astype(F32)

    def last_table(q):
        value = jnp.zeros((points, cells), F32)
        for j in range(4):
            value = value + jnp.where(
                orx[b + q, j : j + 1, :] - origin == oslots, orx[b + q, 4 + j : 5 + j, :], 0.0
            )
        otab[q, 0], otab[q, 1] = split(value)

    for c in range(3, COMM):
        forward(c)
        advect(0, c - 3, keep)
        if (c - 3) % 2:
            multiply((c - 3) // 2)
    advect(0, COMM - 3, keep)
    multiply(2)
    advect(0, COMM - 2, keep)
    advect(0, COMM - 1, keep)
    multiply(KPARTS - 1)
    source(0, bmeta[8:9, :])

    stokes = dot(table[...], midb[...])
    parts = dot_split(stokes, btab[0], btab[1])
    for t in range((TEAM + 2) // 2):
        zonal = parts[0:levels, t * lanes : (t + 1) * lanes]
        merid = parts[levels : 2 * levels, t * lanes : (t + 1) * lanes]
        dm[2 * t], dm[2 * t + 1] = even(zonal, merid), odd(zonal, merid)
    start(drift_out())
    drx[b] = dm[b + 1]
    start(sides())
    each(0, 2, lambda c: start(halo(1, c)))
    for q in range(3):
        last_table(q)

    def team_drift():
        inner, outer = drift_in()
        received(inner)

        @pl.when((b == 0) | (b == TEAM - 1))
        def _():
            received(outer)

        drift_x = jnp.zeros((levels, cells), F32)
        drift_y = jnp.zeros((levels, cells), F32)
        for s in range(TEAM):
            part = drx[s] + drx[TEAM + s]
            to = (window * s - window // 2) % cells
            drift_x += pltpu.roll(jnp.where(low, part, 0.0), to, 1)
            drift_y += pltpu.roll(jnp.where(low, pltpu.roll(part, width, 1), 0.0), to, 1)
        return drift_x, drift_y

    ocean(0, team_drift)
    surface(state, sbuf, 0)
    row_start(1)
    srx[b + 1] = sbuf[...]
    each(2, COMM, lambda c: start(halo(1, c)))
    received(sides())
    edge[1] = jnp.where(lax.rem(lane_rim, 2) == 1, exin[TEAM], exin[TEAM + 1])
    received(row_in(1))
    flow(1)

    def stack(c, r, values):
        packed = pl.ds(pl.multiple_of(c * half + r * unit, unit), unit)
        for t in range(2):
            first, second = values[0][t], values[1][t]
            pk2[2 * t, packed, :] = jnp.where(low_unit, first, pltpu.roll(second, width, 1))
            pk2[2 * t + 1, packed, :] = jnp.where(low_unit, pltpu.roll(first, width, 1), second)

    def give(c):
        advect(1, c, stack)
        start(piece_out(1, c))
        rx[1, b, halves(c), :] = pk2[b, halves(c), :]

    def take(c):
        received(piece_in(1, c))
        for sub, join in enumerate((even, odd)):
            at = pl.ds(pl.multiple_of(c * size + sub * half, half), half)
            for t in range(2):
                value = join(rx[1, 2 * t, halves(c), :], rx[1, 2 * t + 1, halves(c), :])
                adv[at, t * lanes : (t + 1) * lanes] = value
                advb[at, t * lanes : (t + 1) * lanes] = value.astype(BF16)

    each(0, 3, give)
    for c in range(3, COMM):
        give(c)
        take(c - 3)
        if c == COMM - 1:
            start(zonal_pair(1))
        if (c - 3) % 2:
            multiply((c - 3) // 2)
    take(COMM - 3)
    multiply(2)
    take(COMM - 2)
    take(COMM - 1)
    multiply(KPARTS - 1)
    source(1, wet[...].astype(F32))

    stokes = dot(table[...], midb[...])
    copies = last_pair()
    dbuf[0] = dot_split(stokes, otab[2, 0], otab[2, 1])
    copies[0].start()
    dbuf[1] = dot_split(stokes, otab[0, 0], otab[0, 1])
    copies[1].start()
    dself[...] = dot_split(stokes, otab[1, 0], otab[1, 1])

    def last_drift():
        received(last_pair())
        drift = dself[...] + dhalo[0] + dhalo[1]
        return drift[0:levels], drift[levels : 2 * levels]

    ocean(1, last_drift)

    sent(meta_out())
    sent(edges_out())
    sent(sides())
    sent(drift_out())
    sent(last_pair())
    for step in range(STEPS):
        row_sent(step)
        sent(zonal_pair(step))
        sent(all_out(step))


def local(
    spectrum, water_mask, courant, stencil_sign, quad_index, quad_weight, nonlinear, stokes_table,
    point_index, point_weight, ocean_index, ocean_weight, currents, coriolis, mixing, surface_weights,
):
    comps, points = spectrum.shape
    levels, cells = currents.shape[1:]
    lanes = points // 2
    packed = comps // 2
    rim = comps // 16
    vm = pl.BlockSpec(memory_space=pltpu.VMEM)
    dma = pltpu.SemaphoreType.DMA

    def f32(*shape):
        return pltpu.VMEM(shape, F32)

    def bf16(*shape):
        return pltpu.VMEM(shape, BF16)

    scratch = [
        f32(128, comps),
        f32(comps, 128),
        f32(128, 128),
        bf16(4 * comps, comps),
        f32(TEAM, packed, lanes),
        f32(TEAM, packed, lanes),
        f32(STEPS, TEAM, packed, lanes),
        f32(2, packed, lanes),
        f32(STEPS, 2, packed, lanes),
        f32(STEPS, rim, lanes),
        f32(TEAM + 2, rim, lanes),
        f32(STEPS, rim, lanes),
        f32(comps, points),
        bf16(comps, points),
        f32(4 * comps, points),
        f32(comps, points),
        bf16(comps, points),
        f32(2, levels, cells),
        f32(16, points),
        f32(TEAM, 16, points),
        f32(16, points),
        f32(16, cells),
        f32(TEAM + 2, 16, cells),
        f32(8, cells),
        f32(TEAM + 2, 8, cells),
        f32(8, (TEAM + 2) * cells),
        f32(STEPS, 2, levels, cells),
        bf16(2, (TEAM + 2) * cells, points),
        bf16(2, points, (TEAM + 2) // 2 * lanes),
        bf16(3, 2, points, cells),
        f32(TEAM + 2, levels, lanes),
        f32(2 * TEAM, levels, lanes),
        f32(2, 2 * levels, cells),
        f32(2, 2 * levels, cells),
        f32(2 * levels, cells),
        f32(8, points),
        dma((STEPS, 3)),
        dma((STEPS, TEAM, COMM)),
        dma((STEPS, 2)),
        dma((STEPS, 2, COMM)),
        dma((3,)),
        dma((TEAM,)),
        dma((2,)),
        dma((2,)),
        dma((3,)),
        dma((TEAM,)),
        dma((3 + TEAM,)),
        dma((TEAM + 2,)),
        dma((3 + TEAM,)),
        dma((TEAM + 2,)),
        dma((5,)),
        dma((2 * TEAM,)),
        dma((STEPS, 2)),
        dma((STEPS, 2)),
        dma((2,)),
        dma((2,)),
    ]
    return pl.pallas_call(
        wave_kernel,
        out_shape=(
            pltpu.VMEM((comps, points), F32),
            pltpu.VMEM(currents.shape, F32),
        ),
        in_specs=[vm] * 16,
        out_specs=(vm, vm),
        scratch_shapes=scratch,
        compiler_params=pltpu.CompilerParams(
            collective_id=0, has_side_effects=True, vmem_limit_bytes=56 * 1024 * 1024
        ),
    )(
        spectrum,
        water_mask.reshape(1, points),
        courant,
        stencil_sign,
        quad_index.transpose(0, 2, 1),
        quad_weight.transpose(0, 2, 1),
        nonlinear.reshape(1, comps),
        stokes_table,
        point_index,
        point_weight,
        ocean_index,
        ocean_weight,
        currents,
        coriolis.reshape(1, cells),
        mixing.reshape(1, levels),
        surface_weights.reshape(1, levels),
    )


def solution(mesh):
    ring = P(("mp", "dev"))
    split_last = P(None, ("mp", "dev"))
    deep = P(None, None, ("mp", "dev"))
    return jax.shard_map(
        local,
        mesh=mesh,
        in_specs=(
            split_last, ring, P(), P(), P(), P(), P(), P(), split_last, split_last, split_last, split_last, deep,
            ring, P(), P(),
        ),
        out_specs=(split_last, deep),
        check_vma=False,
    )
```

```python
import jax
import jax.numpy as jnp
from jax import lax
from jax.experimental import pallas as pl
from jax.experimental.pallas import tpu as pltpu
from jax.sharding import PartitionSpec as P

STEPS = 2
OCEAN_STEP = 0.5
TEAM = 4
COMM = 8
EARLY = 4
INPUTS = 16
KPARTS = 4
MESH = pl.DeviceIdType.MESH
F32, BF16 = jnp.float32, jnp.bfloat16


def split(x):
    high = x.astype(BF16)
    return high, (x - high.astype(F32)).astype(BF16)


def dot(a, b):
    return jnp.dot(a, b, preferred_element_type=F32)


def dot_split(x, table_high, table_low):
    high, low = split(x)
    return dot(high, table_high) + (dot(low, table_high) + dot(high, table_low))


def wave_kernel(*refs):
    given, (spec_out, cur_out), scratch = refs[:INPUTS], refs[INPUTS : INPUTS + 2], refs[INPUTS + 2 :]
    copied, load_sems, rest = scratch[:INPUTS], scratch[INPUTS], scratch[INPUTS + 1 :]
    loads = [pltpu.make_async_copy(a, c, load_sems.at[i]) for i, (a, c) in enumerate(zip(given, copied))]
    wave_body(loads, *copied, spec_out, cur_out, *rest)


def wave_body(
    loads,
    spec, wet, courant, sign, qidx, qwt, nonlinear, table, pidx, pwt, oidx, owt,
    currents, coriolis, mixing, sweight,
    spec_out, cur_out,
    araw, cols, lraw, quad, pk, pk2, pkb, rx, rxb, zpk, zin, ex, exin, ce, cein, edge, adv, advb, acc, mid, midb, state,
    mbuf, meta, bmeta, osm, orx, sbuf, srx, sall, zhalo, ptab, rtab, btab, otab, dm, drx, dbuf, dhalo, dself, tan, tanr,
    rxs, rxr, bs, br, zs, zr, es, er, fs, fr, ms, mr, os_, or_, ss, sr, ds_, dr, us, ur, hs, hr,
):
    comps, points = spec.shape
    cells = coriolis.shape[1]
    levels = mixing.shape[1]
    dev_count = lax.axis_size("dev")
    total = lax.axis_size("mp") * dev_count
    pos = lax.axis_index("mp") * dev_count + lax.axis_index("dev")
    b = lax.rem(pos, TEAM)
    base = pos - b
    width = points // TEAM
    window = cells // TEAM
    size = comps // COMM
    half = size // 2
    lanes = 2 * width

    none = lax.div(pos, total)

    def wrap(p):
        return lax.rem(p + total, total)

    up, down = wrap(pos + 1), wrap(pos - 1)
    ahead, behind = wrap(pos + TEAM), wrap(pos - TEAM)
    mates = [lax.rem(b + i, TEAM) for i in range(1, TEAM)]

    def remote(src, dst, ssem, rsem, p):
        return pltpu.make_async_remote_copy(
            src_ref=src, dst_ref=dst, send_sem=ssem, recv_sem=rsem,
            device_id=(lax.div(p, dev_count), lax.rem(p, dev_count)), device_id_type=MESH,
        )

    def span(c, n):
        return pl.ds(pl.multiple_of(c * n, n), n)

    def rows(c):
        return span(c, size)

    def halves(c):
        return span(c, half)

    def each(low, high, body):
        def run(c, carry):
            body(c)
            return carry

        lax.fori_loop(low, high, run, 0)

    def start(copies):
        for copy in copies:
            copy.start()

    def received(copies):
        for copy in copies:
            copy.wait_recv()

    def sent(copies):
        for copy in copies:
            copy.wait_send()

    def piece_out(step, c):
        src = pk if step == 0 else pk2
        return [
            remote(src.at[d, halves(c)], rx.at[step, b, halves(c)], rxs.at[step, i], rxr.at[step, b, c], base + d)
            for i, d in enumerate(mates)
        ]

    def piece_in(step, c):
        src = pk if step == 0 else pk2
        return [
            remote(src.at[d, halves(c)], rx.at[step, d, halves(c)], rxs.at[step, i], rxr.at[step, d, c], base + d)
            for i, d in enumerate(mates)
        ]

    def halo(step, c):
        low = rx.at[0, TEAM - 1, halves(c)] if step == 0 else zpk.at[0, halves(c)]
        high = rx.at[0, 0, halves(c)] if step == 0 else zpk.at[1, halves(c)]
        return [
            remote(low, zin.at[step, 0, halves(c)], zs.at[step, 0], zr.at[step, 0, c], ahead),
            remote(high, zin.at[step, 1, halves(c)], zs.at[step, 1], zr.at[step, 1, c], behind),
        ]

    def beside_out(c):
        return [
            remote(pkb.at[d, halves(c)], rxb.at[b, halves(c)], bs.at[i], br.at[b, c], base + d)
            for i, d in enumerate(mates)
        ]

    def beside_in(c):
        return [
            remote(pkb.at[d, halves(c)], rxb.at[d, halves(c)], bs.at[i], br.at[d, c], base + d)
            for i, d in enumerate(mates)
        ]

    def beside_all():
        return [remote(pkb.at[d], rxb.at[b], bs.at[i], br.at[b, 0], base + d) for i, d in enumerate(mates)]

    def all_out(step):
        src = pk if step == 0 else pk2
        copies = [
            remote(src.at[d], rx.at[step, b], rxs.at[step, i], rxr.at[step, b, 0], base + d)
            for i, d in enumerate(mates)
        ]
        low_from = rx.at[0, TEAM - 1] if step == 0 else zpk.at[0]
        high_from = rx.at[0, 0] if step == 0 else zpk.at[1]
        copies.append(remote(low_from, zin.at[step, 0], zs.at[step, 0], zr.at[step, 0, 0], ahead))
        copies.append(remote(high_from, zin.at[step, 1], zs.at[step, 1], zr.at[step, 1, 0], behind))
        return copies

    def edges_out():
        return [remote(ce.at[d], cein.at[b], es.at[i], er.at[b], base + d) for i, d in enumerate(mates)]

    def edges_in():
        return [remote(ce.at[d], cein.at[d], es.at[i], er.at[d], base + d) for i, d in enumerate(mates)]

    right, left = base + mates[0], base + mates[2]

    def sides():
        return [
            remote(ex.at[1], exin.at[0], fs.at[0], fr.at[0], right),
            remote(ex.at[1], exin.at[1], fs.at[1], fr.at[1], left),
        ]

    def meta_out():
        return [remote(mbuf, meta.at[b], ms.at[i], mr.at[b], base + d) for i, d in enumerate(mates)]

    def meta_in():
        return [remote(mbuf, meta.at[d], ms.at[i], mr.at[d], base + d) for i, d in enumerate(mates)]

    def row_out(step):
        src, dst, ssem, rsem = (osm, orx, os_, or_) if step == 0 else (sbuf, srx, ss, sr)
        inner = [remote(src, dst.at[b + 1], ssem.at[i], rsem.at[b + 1], base + d) for i, d in enumerate(mates)]
        before = [
            remote(src, dst.at[TEAM + 1], ssem.at[3 + k], rsem.at[TEAM + 1], wrap(base - TEAM + k)) for k in range(TEAM)
        ]
        after = [remote(src, dst.at[0], ssem.at[3 + k], rsem.at[0], wrap(base + TEAM + k)) for k in range(TEAM)]
        return inner, before, after

    def row_start(step):
        inner, before, after = row_out(step)

        @pl.when(b == 0)
        def _():
            start(before)

        @pl.when(b == TEAM - 1)
        def _():
            start(after)

        start(inner)

    def row_sent(step):
        inner, before, after = row_out(step)
        sent(inner)

        @pl.when(b == 0)
        def _():
            sent(before)

        @pl.when(b == TEAM - 1)
        def _():
            sent(after)

    def row_in(step):
        src, dst, ssem, rsem = (osm, orx, os_, or_) if step == 0 else (sbuf, srx, ss, sr)
        copies = [remote(src, dst.at[d + 1], ssem.at[i], rsem.at[d + 1], base + d) for i, d in enumerate(mates)]
        copies.append(remote(src, dst.at[0], ssem.at[0], rsem.at[0], ahead))
        copies.append(remote(src, dst.at[TEAM + 1], ssem.at[0], rsem.at[TEAM + 1], behind))
        return copies

    def drift_out():
        copies = [
            remote(dm.at[0], drx.at[TEAM + b], ds_.at[3], dr.at[TEAM + b], wrap(base - 1)),
            remote(dm.at[TEAM + 1], drx.at[TEAM + b], ds_.at[4], dr.at[TEAM + b], wrap(base + TEAM)),
        ]
        return copies + [
            remote(dm.at[d + 1], drx.at[b], ds_.at[i], dr.at[b], base + d) for i, d in enumerate(mates)
        ]

    def drift_in():
        inner = [remote(dm.at[0], drx.at[d], ds_.at[i], dr.at[d], base + d) for i, d in enumerate(mates)]
        outer = [remote(dm.at[0], drx.at[TEAM + k], ds_.at[3], dr.at[TEAM + k], ahead) for k in range(TEAM)]
        return inner, outer

    def zonal_pair(step):
        src = currents.at[0] if step == 0 else state.at[0]
        return [
            remote(src, zhalo.at[step, 0], us.at[step, 0], ur.at[step, 0], up),
            remote(src, zhalo.at[step, 1], us.at[step, 1], ur.at[step, 1], down),
        ]

    def last_pair():
        return [
            remote(dbuf.at[0], dhalo.at[0], hs.at[0], hr.at[0], up),
            remote(dbuf.at[1], dhalo.at[1], hs.at[1], hr.at[1], down),
        ]

    start(loads)
    drx[TEAM : 2 * TEAM] = jnp.zeros((TEAM, levels, lanes), F32)
    barrier = pltpu.get_barrier_semaphore()
    partners = [base + d for d in mates]
    partners += [wrap(base - TEAM + k) for k in range(TEAM)] + [wrap(base + TEAM + k) for k in range(TEAM)]
    for p in partners:
        pl.semaphore_signal(
            barrier, inc=1, device_id=(lax.div(p, dev_count), lax.rem(p, dev_count)), device_id_type=MESH
        )

    lane = lax.broadcasted_iota(jnp.int32, (half, lanes), 1)
    low = lane < width

    def even(a, c):
        return jnp.where(low, a, pltpu.roll(c, width, 1))

    def odd(a, c):
        return jnp.where(low, pltpu.roll(a, width, 1), c)

    lane_row = lax.broadcasted_iota(jnp.int32, (8, lanes), 1)
    wide_lane = lax.broadcasted_iota(jnp.int32, (size, lanes), 1)
    rim = lax.rem(wide_lane + 1, width) < 2

    def pack_rim(first, second):
        mixed = jnp.where(rim, first, pltpu.roll(second, 2, 1))
        out = jnp.zeros((8, lanes), F32)
        for g in range(size // 8):
            here = lax.rem(lane_row + 1 - 4 * g + lanes, width) < 4
            part = mixed[8 * g : 8 * g + 8]
            out = jnp.where(here, pltpu.roll(part, 4 * g, 1) if g else part, out)
        return out

    for load in loads:
        load.wait()
    pl.semaphore_wait(barrier, len(partners))

    def pack_in(c):
        for t in range(2):
            tile = spec[rows(c), t * lanes : (t + 1) * lanes]
            first, second = tile[0:half], tile[half:size]
            pk[2 * t, halves(c), :] = even(first, second)
            pk[2 * t + 1, halves(c), :] = odd(first, second)
        rx[0, b, halves(c), :] = pk[b, halves(c), :]
        start(piece_out(0, c))

    each(0, 1, pack_in)
    lraw[...] = jnp.zeros_like(lraw)
    lraw[0:1, 0:levels] = mixing[...]
    lraw[1:2, 0:levels] = sweight[...]
    lcols = jnp.transpose(lraw[...])
    level_mix = lcols[0:levels, 0:1]
    level_weight = lcols[0:levels, 1:2]

    def surface(source, dst, at):
        dst[at : at + 8, :] = jnp.zeros((8, cells), F32)
        for a in range(2):
            dst[at + a : at + a + 1, :] = jnp.sum(level_weight * source[a], axis=0, keepdims=True)

    osm[0:4, :] = oidx[...].astype(F32)
    osm[4:8, :] = owt[...]
    surface(currents, osm, 8)
    orx[b + 1] = osm[...]
    row_start(0)
    mbuf[0:4, :] = pidx[...].astype(F32)
    mbuf[0:1, :] = (2 * pidx[0:1, :] + wet[...]).astype(F32)
    mbuf[4:8, :] = pwt[...]
    meta[b] = mbuf[...]
    start(meta_out())
    each(1, 2, pack_in)

    def rim_in(c):
        ex[0, span(c, 8), :] = pack_rim(spec[rows(c), 0:lanes], spec[rows(c), lanes : 2 * lanes])

    each(0, COMM, rim_in)
    last = width - 1
    from_left = (1, last, lanes - 1, last + 2)
    from_right = (width, 2, width + 2, 0)
    quarter = lax.rem(lane_row, 4)
    ahead_half = lane_row < width
    for d in range(TEAM):
        for v in range(COMM // 4):
            out = jnp.zeros((8, lanes), F32)
            for k in range(4):
                part = ex[0, 8 * (4 * v + k) : 8 * (4 * v + k) + 8, :]
                west = pltpu.roll(part, (k - from_left[d]) % lanes, 1)
                east = pltpu.roll(part, (width + k - from_right[d]) % lanes, 1)
                out = jnp.where(quarter == k, jnp.where(ahead_half, west, east), out)
            ce[d, 8 * v : 8 * v + 8, :] = out
    cein[b] = ce[b]
    start(edges_out())
    each(2, COMM, pack_in)
    start(zonal_pair(0))
    araw[...] = jnp.zeros_like(araw)
    araw[0:2, :] = courant[...]
    araw[2:4, :] = (2 * sign[...] - 1).astype(F32)
    araw[4:5, :] = nonlinear[...]
    for j in range(4):
        index, weight = qidx[j], qwt[j]
        twice = index[0:1] == index[1:2]
        araw[8 + 2 * j : 10 + 2 * j, :] = index.astype(F32)
        araw[16 + 2 * j : 17 + 2 * j, :] = jnp.where(twice, weight[0:1] + weight[1:2], weight[0:1])
        araw[17 + 2 * j : 18 + 2 * j, :] = weight[1:2]
    cols[...] = jnp.transpose(araw[...])
    long_lane = lax.broadcasted_iota(jnp.int32, (32, comps), 1).astype(F32)

    def build_quad(c):
        for sub in range(size // 32):
            begin = pl.multiple_of(c * size + sub * 32, 32)
            col = cols[pl.ds(begin, 32), :]
            for j in range(4):
                two = jnp.where(col[:, 9 + 2 * j : 10 + 2 * j] == long_lane, col[:, 17 + 2 * j : 18 + 2 * j], 0.0)
                one = jnp.where(col[:, 8 + 2 * j : 9 + 2 * j] == long_lane, col[:, 16 + 2 * j : 17 + 2 * j], two)
                quad[pl.ds(begin + j * comps, 32), :] = one.astype(BF16)

    def forward(c):
        received(piece_in(0, c))
        start(halo(0, c))

    each(0, COMM // 2, build_quad)
    forward(0)
    each(COMM // 2, COMM - 1, build_quad)
    forward(1)
    each(COMM - 1, COMM, build_quad)
    received(meta_in())
    aside = lax.rem(b, 2)
    for t in range(2):
        pieces = []
        for r in (2 * t, 2 * t + 1):
            tile = meta[r, :, pl.ds(pl.multiple_of(lax.div(b, 2) * lanes, lanes), lanes)]
            pieces.append(jnp.where(aside == r % 2, tile, pltpu.roll(tile, width, 1)))
        bmeta[0:8, t * lanes : (t + 1) * lanes] = jnp.where(low[0:8], pieces[0], pieces[1])

    joined = bmeta[0:1, :]
    halved = jnp.floor(0.5 * joined)
    bmeta[8:9, :] = joined - 2.0 * halved
    bmeta[0:1, :] = halved
    received(row_in(0))
    slots = lax.broadcasted_iota(jnp.int32, (cells, points), 0).astype(F32)
    for q in range(TEAM + 2):
        owner = (wrap(base - 1 + q) * cells).astype(F32)
        value = jnp.zeros((cells, points), F32)
        for j in range(4):
            value = value + jnp.where(bmeta[j : j + 1, :] - owner == slots, bmeta[4 + j : 5 + j, :], 0.0)
        ptab[0, q * cells : (q + 1) * cells, :], ptab[1, q * cells : (q + 1) * cells, :] = split(value)

    shift = lax.rem(cells + window // 2 - window * b, cells)
    pointer = lax.broadcasted_iota(jnp.int32, (width, cells), 0).astype(F32)
    for t in range((TEAM + 2) // 2):
        near = pltpu.roll(orx[2 * t, 0:8], shift, 1)
        far = pltpu.roll(orx[2 * t + 1, 0:8], shift, 1)
        both = jnp.where(low[0:8], near, pltpu.roll(far, width, 1))
        for r in range(TEAM):
            origin = ((base + r) * points + width * b).astype(F32)
            value = jnp.zeros((width, cells), F32)
            for j in range(4):
                value = value + jnp.where(both[j : j + 1, :] - origin == pointer, both[4 + j : 5 + j, :], 0.0)
            high_part, low_part = split(value)
            btab[0, r * width : (r + 1) * width, t * lanes : (t + 1) * lanes] = high_part
            btab[1, r * width : (r + 1) * width, t * lanes : (t + 1) * lanes] = low_part

    forward(2)
    received(edges_in())
    lane_rim = lax.broadcasted_iota(jnp.int32, (8 * COMM, lanes), 1)
    upper = lane_row >= last
    to_left = (last, lanes - 1, last + 2, 1)
    to_right = (0, width, 2, width + 2)
    on_left = (
        (quarter == 3) & upper & (lane_row < lanes - 1),
        (quarter == 3) & ((lane_row < last) | (lane_row == lanes - 1)),
        (quarter == 1) & upper,
        (quarter == 1) & ~upper,
    )
    on_right = ((quarter == 0) & ~upper, (quarter == 0) & upper, (quarter == 2) & ~upper, (quarter == 2) & upper)
    for c in range(COMM):
        v, k = c // 4, c % 4
        out = jnp.zeros((8, lanes), F32)
        for r in range(TEAM):
            part = cein[r, 8 * v : 8 * v + 8, :]
            out = jnp.where(on_left[r], pltpu.roll(part, (to_left[r] - k) % lanes, 1), out)
            out = jnp.where(on_right[r], pltpu.roll(part, (to_right[r] - width - k) % lanes, 1), out)
        edge[0, 8 * c : 8 * c + 8, :] = out

    def flow(step):
        for q in range(TEAM + 2):
            sall[:, q * cells : (q + 1) * cells] = orx[q, 8:16] if step == 0 else srx[q]
        tan[...] = jnp.tanh(dot_split(sall[...], ptab[0], ptab[1]))

    flow(0)

    lane_half = lax.rem(lane, width)
    at_first, at_last = lane_half == 0, lane_half == width - 1

    unit = half
    low_unit = low[0:unit]
    at_first, at_last = at_first[0:unit], at_last[0:unit]

    def advect(step, c, emit):
        received(halo(step, c))

        def body(r):
            packed = pl.ds(pl.multiple_of(c * half + r * unit, unit), unit)
            turn = lax.rem(lanes - 4 * (unit // 8) * r, lanes)
            rim_row = pltpu.roll(edge[step, span(c, 8), :], turn, 1)
            out = []
            for sub in range(2):
                at = pl.ds(pl.multiple_of(c * size + sub * half + r * unit, unit), unit)
                col = cols[at, :]
                if step == 0:
                    own = []
                    for t in range(2):
                        a, d = rx[0, 2 * t, packed, :], rx[0, 2 * t + 1, packed, :]
                        if sub:
                            own.append(jnp.where(low_unit, pltpu.roll(a, width, 1), d))
                        else:
                            own.append(jnp.where(low_unit, a, pltpu.roll(d, width, 1)))
                else:
                    own = [mid[at, t * lanes : (t + 1) * lanes] for t in range(2)]
                turned = [pltpu.roll(x, width, 1) for x in own]
                below, above = zin[step, 0, packed, :], zin[step, 1, packed, :]
                if sub:
                    below = pltpu.roll(below, width, 1)
                else:
                    above = pltpu.roll(above, width, 1)
                middle = jnp.where(low_unit, turned[0], turned[1])
                north = (jnp.where(low_unit, below, turned[0]), middle)
                south = (middle, jnp.where(low_unit, turned[1], above))
                groups = range(sub * half // 8, sub * half // 8 + unit // 8)
                spin = [
                    jnp.concatenate([pltpu.roll(rim_row, (k - 4 * g) % lanes, 1) for g in groups], axis=0)
                    for k in (width + 1, width - 1, width - 3)
                ]
                sense_x, sense_y = col[:, 2:3], col[:, 3:4]
                values = []
                for t in range(2):
                    x = own[t]
                    west = jnp.where(at_first, spin[t], pltpu.roll(x, 1, 1))
                    east = jnp.where(at_last, spin[t + 1], pltpu.roll(x, lanes - 1, 1))
                    behind_x = jnp.where(sense_x > 0, west, east)
                    behind_y = jnp.where(sense_y > 0, north[t], south[t])
                    lane_at = slice(t * lanes, (t + 1) * lanes)
                    speed_x = col[:, 0:1] * (1.0 + 0.5 * (sense_x * tan[0:1, lane_at]))
                    speed_y = col[:, 1:2] * (1.0 + 0.5 * (sense_y * tan[1:2, lane_at]))
                    values.append(x - speed_x * (x - behind_x) - speed_y * (x - behind_y))
                out.append(values)
            emit(c, r, out)

        each(0, half // unit, body)

    def keep(c, r, values):
        for sub in range(2):
            at = pl.ds(pl.multiple_of(c * size + sub * half + r * unit, unit), unit)
            for t in range(2):
                adv[at, t * lanes : (t + 1) * lanes] = values[sub][t]
                advb[at, t * lanes : (t + 1) * lanes] = values[sub][t].astype(BF16)

    deep = comps // KPARTS

    def multiply(part):
        k_at = slice(part * deep, (part + 1) * deep)

        def body(i):
            if part:
                acc[...] = acc[...] + dot(quad[:, k_at], advb[k_at, :])
            else:
                acc[...] = dot(quad[:, k_at], advb[k_at, :])

        each(none, none + 1, body)

    def halo_out(c):
        tiles = [mid[rows(c), t * lanes : (t + 1) * lanes] for t in range(2)]
        zpk[0, halves(c), :] = odd(tiles[1][0:half], tiles[1][half:size])
        zpk[1, halves(c), :] = even(tiles[0][0:half], tiles[0][half:size])
        start(halo(1, c))

    def rim_out(c):
        ex[1, span(c, 8), :] = pack_rim(mid[rows(c), 0:lanes], mid[rows(c), lanes : 2 * lanes])

    def source(step, wet_row):
        target = mid if step == 0 else spec_out

        def body(c):
            at = rows(c)
            terms = [acc[pl.ds(pl.multiple_of(j * comps + c * size, size), size), :] for j in range(4)]
            value = adv[at, :]
            total_sum = terms[0] + terms[1] + terms[2] + terms[3]
            pair_sum = terms[0] * terms[1] + terms[2] * terms[3]
            new = wet_row * (value + cols[at, 4:5] * (value * value * total_sum - value * pair_sum))
            target[at, :] = new
            midb[at, :] = new.astype(BF16)

        if step == 0:
            each(0, 1, body)
            each(0, 1, halo_out)
            each(1, COMM, body)
        else:
            each(0, COMM, body)

    level_row = lax.broadcasted_iota(jnp.int32, (levels, cells), 0)

    def mix(w):
        above = jnp.where(level_row == 0, w, pltpu.roll(w, 1, 0))
        below = jnp.where(level_row == levels - 1, w, pltpu.roll(w, levels - 1, 0))
        return level_mix * (above - 2.0 * w + below)

    def ocean(step, drift):
        before = currents if step == 0 else state
        target = state if step == 0 else cur_out
        received(zonal_pair(step))
        u, v = before[0], before[1]
        rot = coriolis[...]
        turn = 0.5 * (pltpu.roll(v, cells - 1, 1) - pltpu.roll(v, 1, 1)) - 0.5 * (zhalo[step, 1] - zhalo[step, 0])
        mix_u, mix_v = mix(u), mix(v)
        drift_x, drift_y = drift()
        target[0] = u + OCEAN_STEP * (rot * (v + drift_y) + turn * drift_y + mix_u)
        target[1] = v + OCEAN_STEP * (-rot * (u + drift_x) - turn * drift_x + mix_v)

    oslots = lax.broadcasted_iota(jnp.int32, (points, cells), 0).astype(F32)
    origin = (pos * points).astype(F32)

    def last_table(q):
        value = jnp.zeros((points, cells), F32)
        for j in range(4):
            value = value + jnp.where(
                orx[b + q, j : j + 1, :] - origin == oslots, orx[b + q, 4 + j : 5 + j, :], 0.0
            )
        otab[q, 0], otab[q, 1] = split(value)
        owner = (wrap(pos - 1 + q) * cells).astype(F32)
        value = jnp.zeros((cells, points), F32)
        for j in range(4):
            value = value + jnp.where(pidx[j : j + 1, :].astype(F32) - owner == slots, pwt[j : j + 1, :], 0.0)
        rtab[0, q * cells : (q + 1) * cells, :], rtab[1, q * cells : (q + 1) * cells, :] = split(value)

    for c in range(3, COMM):
        forward(c)
        advect(0, c - 3, keep)
        if (c - 3) % 2:
            multiply((c - 3) // 2)
    advect(0, COMM - 3, keep)
    multiply(2)
    advect(0, COMM - 2, keep)
    advect(0, COMM - 1, keep)
    multiply(KPARTS - 1)
    source(0, bmeta[8:9, :])

    stokes = dot(table[...], midb[...])
    parts = dot_split(stokes, btab[0], btab[1])
    for t in range((TEAM + 2) // 2):
        zonal = parts[0:levels, t * lanes : (t + 1) * lanes]
        merid = parts[levels : 2 * levels, t * lanes : (t + 1) * lanes]
        dm[2 * t], dm[2 * t + 1] = even(zonal, merid), odd(zonal, merid)
    start(drift_out())
    drx[b] = dm[b + 1]
    def own_out(c):
        for t in range(2):
            tile = mid[rows(c), t * lanes : (t + 1) * lanes]
            first, second = tile[0:half], tile[half:size]
            pk2[2 * t, halves(c), :] = even(first, second)
            pk2[2 * t + 1, halves(c), :] = odd(first, second)
        start(piece_out(1, c))
        rx[1, b, halves(c), :] = pk2[b, halves(c), :]

    each(1, 3, halo_out)
    each(0, EARLY, own_out)
    each(0, COMM, rim_out)
    start(sides())
    for q in range(3):
        last_table(q)

    def team_drift():
        inner, outer = drift_in()
        received(inner)

        @pl.when((b == 0) | (b == TEAM - 1))
        def _():
            received(outer)

        drift_x = jnp.zeros((levels, cells), F32)
        drift_y = jnp.zeros((levels, cells), F32)
        for s in range(TEAM):
            part = drx[s] + drx[TEAM + s]
            to = (window * s - window // 2) % cells
            drift_x += pltpu.roll(jnp.where(low, part, 0.0), to, 1)
            drift_y += pltpu.roll(jnp.where(low, pltpu.roll(part, width, 1), 0.0), to, 1)
        return drift_x, drift_y

    ocean(0, team_drift)
    surface(state, sbuf, 0)
    row_start(1)
    srx[b + 1] = sbuf[...]
    each(3, COMM, halo_out)

    def beside(c):
        received(halo(1, c))
        sides_y = []
        for sub in range(2):
            at = pl.ds(pl.multiple_of(c * size + sub * half, half), half)
            turned = [pltpu.roll(mid[at, t * lanes : (t + 1) * lanes], width, 1) for t in range(2)]
            below, above = zin[1, 0, halves(c), :], zin[1, 1, halves(c), :]
            if sub:
                below = pltpu.roll(below, width, 1)
            else:
                above = pltpu.roll(above, width, 1)
            middle = jnp.where(low, turned[0], turned[1])
            north = (jnp.where(low, below, turned[0]), middle)
            south = (middle, jnp.where(low, turned[1], above))
            sense_y = cols[at, 3:4]
            sides_y.append([jnp.where(sense_y > 0, north[t], south[t]) for t in range(2)])
        for t in range(2):
            pkb[2 * t, halves(c), :] = even(sides_y[0][t], sides_y[1][t])
            pkb[2 * t + 1, halves(c), :] = odd(sides_y[0][t], sides_y[1][t])
        start(beside_out(c))
        rxb[b, halves(c), :] = pkb[b, halves(c), :]

    each(0, EARLY, beside)
    received(sides())
    edge[1] = jnp.where(lax.rem(lane_rim, 2) == 1, exin[0], exin[1])
    received(row_in(1))
    flow(1)

    def stack(c, r, values):
        packed = pl.ds(pl.multiple_of(c * half + r * unit, unit), unit)
        for t in range(2):
            first, second = values[0][t], values[1][t]
            pk2[2 * t, packed, :] = jnp.where(low_unit, first, pltpu.roll(second, width, 1))
            pk2[2 * t + 1, packed, :] = jnp.where(low_unit, pltpu.roll(first, width, 1), second)

    def give(c):
        advect(1, c, stack)
        start(piece_out(1, c))
        rx[1, b, halves(c), :] = pk2[b, halves(c), :]

    def take(c):
        received(piece_in(1, c))
        for sub, join in enumerate((even, odd)):
            at = pl.ds(pl.multiple_of(c * size + sub * half, half), half)
            for t in range(2):
                value = join(rx[1, 2 * t, halves(c), :], rx[1, 2 * t + 1, halves(c), :])
                adv[at, t * lanes : (t + 1) * lanes] = value
                advb[at, t * lanes : (t + 1) * lanes] = value.astype(BF16)

    def flow_row():
        own_part = sall[:, pl.ds(pl.multiple_of(b * cells, cells), 3 * cells)]
        tanr[...] = jnp.tanh(dot_split(own_part, rtab[0], rtab[1]))

    def advance(c):
        received(piece_in(1, c))
        received(beside_in(c))
        for sub, join in enumerate((even, odd)):
            at = pl.ds(pl.multiple_of(c * size + sub * half, half), half)
            col = cols[at, :]
            sense_x, sense_y = col[:, 2:3], col[:, 3:4]
            own = [join(rx[1, 2 * t, halves(c), :], rx[1, 2 * t + 1, halves(c), :]) for t in range(2)]
            behind_y = [join(rxb[2 * t, halves(c), :], rxb[2 * t + 1, halves(c), :]) for t in range(2)]
            forth = [pltpu.roll(x, 1, 1) for x in own]
            back = [pltpu.roll(x, lanes - 1, 1) for x in own]
            for t in range(2):
                x = own[t]
                west = jnp.where(lane == 0, forth[1 - t], forth[t])
                east = jnp.where(lane == lanes - 1, back[1 - t], back[t])
                behind_x = jnp.where(sense_x > 0, west, east)
                lane_at = slice(t * lanes, (t + 1) * lanes)
                speed_x = col[:, 0:1] * (1.0 + 0.5 * (sense_x * tanr[0:1, lane_at]))
                speed_y = col[:, 1:2] * (1.0 + 0.5 * (sense_y * tanr[1:2, lane_at]))
                value = x - speed_x * (x - behind_x) - speed_y * (x - behind_y[t])
                adv[at, lane_at] = value
                advb[at, lane_at] = value.astype(BF16)

    each(EARLY, COMM, give)
    start(zonal_pair(1))
    flow_row()
    for part in range(KPARTS):
        turn = advance if part < EARLY // 2 else take
        each(2 * part, 2 * part + 2, turn)
        multiply(part)
    source(1, wet[...].astype(F32))

    stokes = dot(table[...], midb[...])
    copies = last_pair()
    dbuf[0] = dot_split(stokes, otab[2, 0], otab[2, 1])
    copies[0].start()
    dbuf[1] = dot_split(stokes, otab[0, 0], otab[0, 1])
    copies[1].start()
    dself[...] = dot_split(stokes, otab[1, 0], otab[1, 1])

    def last_drift():
        received(last_pair())
        drift = dself[...] + dhalo[0] + dhalo[1]
        return drift[0:levels], drift[levels : 2 * levels]

    ocean(1, last_drift)

    sent(beside_all())
    sent(meta_out())
    sent(edges_out())
    sent(sides())
    sent(drift_out())
    sent(last_pair())
    for step in range(STEPS):
        row_sent(step)
        sent(zonal_pair(step))
        sent(all_out(step))


def local(
    spectrum, water_mask, courant, stencil_sign, quad_index, quad_weight, nonlinear, stokes_table,
    point_index, point_weight, ocean_index, ocean_weight, currents, coriolis, mixing, surface_weights,
):
    comps, points = spectrum.shape
    levels, cells = currents.shape[1:]
    lanes = points // 2
    packed = comps // 2
    rim = comps // 16
    vm = pl.BlockSpec(memory_space=pltpu.VMEM)
    dma = pltpu.SemaphoreType.DMA

    def f32(*shape):
        return pltpu.VMEM(shape, F32)

    def bf16(*shape):
        return pltpu.VMEM(shape, BF16)

    scratch = [
        f32(128, comps),
        f32(comps, 128),
        f32(128, 128),
        bf16(4 * comps, comps),
        f32(TEAM, packed, lanes),
        f32(TEAM, packed, lanes),
        f32(TEAM, packed * EARLY // COMM, lanes),
        f32(STEPS, TEAM, packed, lanes),
        f32(TEAM, packed * EARLY // COMM, lanes),
        f32(2, packed, lanes),
        f32(STEPS, 2, packed, lanes),
        f32(STEPS, rim, lanes),
        f32(2, rim, lanes),
        f32(TEAM, rim // 4, lanes),
        f32(TEAM, rim // 4, lanes),
        f32(STEPS, rim, lanes),
        f32(comps, points),
        bf16(comps, points),
        f32(4 * comps, points),
        f32(comps, points),
        bf16(comps, points),
        f32(2, levels, cells),
        f32(8, points),
        f32(TEAM, 8, points),
        f32(16, points),
        f32(16, cells),
        f32(TEAM + 2, 16, cells),
        f32(8, cells),
        f32(TEAM + 2, 8, cells),
        f32(8, (TEAM + 2) * cells),
        f32(STEPS, 2, levels, cells),
        bf16(2, (TEAM + 2) * cells, points),
        bf16(2, 3 * cells, points),
        bf16(2, points, (TEAM + 2) // 2 * lanes),
        bf16(3, 2, points, cells),
        f32(TEAM + 2, levels, lanes),
        f32(2 * TEAM, levels, lanes),
        f32(2, 2 * levels, cells),
        f32(2, 2 * levels, cells),
        f32(2 * levels, cells),
        f32(8, points),
        f32(8, points),
        dma((STEPS, 3)),
        dma((STEPS, TEAM, COMM)),
        dma((3,)),
        dma((TEAM, EARLY)),
        dma((STEPS, 2)),
        dma((STEPS, 2, COMM)),
        dma((3,)),
        dma((TEAM,)),
        dma((2,)),
        dma((2,)),
        dma((3,)),
        dma((TEAM,)),
        dma((3 + TEAM,)),
        dma((TEAM + 2,)),
        dma((3 + TEAM,)),
        dma((TEAM + 2,)),
        dma((5,)),
        dma((2 * TEAM,)),
        dma((STEPS, 2)),
        dma((STEPS, 2)),
        dma((2,)),
        dma((2,)),
    ]
    operands = (
        spectrum,
        water_mask.reshape(1, points),
        courant,
        stencil_sign,
        quad_index.transpose(0, 2, 1),
        quad_weight.transpose(0, 2, 1),
        nonlinear.reshape(1, comps),
        stokes_table,
        point_index,
        point_weight,
        ocean_index,
        ocean_weight,
        currents,
        coriolis.reshape(1, cells),
        mixing.reshape(1, levels),
        surface_weights.reshape(1, levels),
    )
    scratch = [pltpu.VMEM(x.shape, x.dtype) for x in operands] + [dma((INPUTS,))] + scratch
    return pl.pallas_call(
        wave_kernel,
        out_shape=(
            pltpu.VMEM((comps, points), F32),
            pltpu.VMEM(currents.shape, F32),
        ),
        in_specs=[pl.BlockSpec(memory_space=pltpu.HBM)] * INPUTS,
        out_specs=(vm, vm),
        scratch_shapes=scratch,
        compiler_params=pltpu.CompilerParams(
            collective_id=0, has_side_effects=True, vmem_limit_bytes=56 * 1024 * 1024
        ),
    )(*operands)


def solution(mesh):
    ring = P(("mp", "dev"))
    split_last = P(None, ("mp", "dev"))
    deep = P(None, None, ("mp", "dev"))
    return jax.shard_map(
        local,
        mesh=mesh,
        in_specs=(
            split_last, ring, P(), P(), P(), P(), P(), P(), split_last, split_last, split_last, split_last, deep,
            ring, P(), P(),
        ),
        out_specs=(split_last, deep),
        check_vma=False,
    )
```

```python
import jax
import jax.numpy as jnp
from jax import lax
from jax.experimental import pallas as pl
from jax.experimental.pallas import tpu as pltpu
from jax.sharding import PartitionSpec as P

STEPS = 2
OCEAN_STEP = 0.5
TEAM = 4
COMM = 8
EARLY = 3
INPUTS = 16
KPARTS = 4
MESH = pl.DeviceIdType.MESH
F32, BF16 = jnp.float32, jnp.bfloat16


def split(x):
    high = x.astype(BF16)
    return high, (x - high.astype(F32)).astype(BF16)


def dot(a, b):
    return jnp.dot(a, b, preferred_element_type=F32)


def dot_split(x, table_high, table_low):
    high, low = split(x)
    return dot(high, table_high) + (dot(low, table_high) + dot(high, table_low))


def wave_kernel(*refs):
    given, (spec_out, cur_out), scratch = refs[:INPUTS], refs[INPUTS : INPUTS + 2], refs[INPUTS + 2 :]
    copied, load_sems, rest = scratch[:INPUTS], scratch[INPUTS], scratch[INPUTS + 1 :]
    loads = [pltpu.make_async_copy(a, c, load_sems.at[i]) for i, (a, c) in enumerate(zip(given, copied))]
    wave_body(loads, *copied, spec_out, cur_out, *rest)


def wave_body(
    loads,
    spec, wet, courant, sign, qidx, qwt, nonlinear, table, pidx, pwt, oidx, owt,
    currents, coriolis, mixing, sweight,
    spec_out, cur_out,
    araw, cols, lraw, quad, pk, pk2, pkb, rx, rxb, zpk, zin, ex, exin, ce, cein, edge, adv, advb, acc, mid, midb, state,
    mbuf, meta, bmeta, osm, orx, sbuf, srx, sall, zhalo, ptab, rtab, btab, otab, dm, drx, dbuf, dhalo, dself, tan, tanr,
    rxs, rxr, bs, br, zs, zr, es, er, fs, fr, ms, mr, os_, or_, ss, sr, ds_, dr, us, ur, hs, hr,
):
    comps, points = spec.shape
    cells = coriolis.shape[1]
    levels = mixing.shape[1]
    dev_count = lax.axis_size("dev")
    total = lax.axis_size("mp") * dev_count
    pos = lax.axis_index("mp") * dev_count + lax.axis_index("dev")
    b = lax.rem(pos, TEAM)
    base = pos - b
    width = points // TEAM
    window = cells // TEAM
    size = comps // COMM
    half = size // 2
    lanes = 2 * width

    none = lax.div(pos, total)

    def wrap(p):
        return lax.rem(p + total, total)

    up, down = wrap(pos + 1), wrap(pos - 1)
    ahead, behind = wrap(pos + TEAM), wrap(pos - TEAM)
    mates = [lax.rem(b + i, TEAM) for i in range(1, TEAM)]

    def remote(src, dst, ssem, rsem, p):
        return pltpu.make_async_remote_copy(
            src_ref=src, dst_ref=dst, send_sem=ssem, recv_sem=rsem,
            device_id=(lax.div(p, dev_count), lax.rem(p, dev_count)), device_id_type=MESH,
        )

    def span(c, n):
        return pl.ds(pl.multiple_of(c * n, n), n)

    def rows(c):
        return span(c, size)

    def halves(c):
        return span(c, half)

    def each(low, high, body):
        def run(c, carry):
            body(c)
            return carry

        lax.fori_loop(low, high, run, 0)

    def start(copies):
        for copy in copies:
            copy.start()

    def received(copies):
        for copy in copies:
            copy.wait_recv()

    def sent(copies):
        for copy in copies:
            copy.wait_send()

    def spread(src, dst, ssem, rsem):
        return [remote(src.at[d], dst, ssem, rsem, base + d) for d in mates]

    def gather(src, dst, ssem, rsem, count):
        return [remote(src.at[0:count], dst.at[0:count], ssem, rsem, base + mates[0])]

    def piece(step, c):
        return (pk if step == 0 else pk2).at[:, halves(c)], rx.at[step, :, halves(c)]

    def piece_out(step, c):
        src, dst = piece(step, c)
        return spread(src, dst.at[b], rxs.at[step], rxr.at[step, c])

    def piece_in(step, c):
        src, dst = piece(step, c)
        return gather(src, dst, rxs.at[step], rxr.at[step, c], TEAM - 1)

    def piece_all(step):
        return gather(pk if step == 0 else pk2, rx.at[step], rxs.at[step], rxr.at[step, 0], TEAM - 1)

    def halo(step, c):
        from_low = rx.at[0, TEAM - 1, halves(c)] if step == 0 else zpk.at[0, halves(c)]
        from_high = rx.at[0, 0, halves(c)] if step == 0 else zpk.at[1, halves(c)]
        return [
            remote(from_low, zin.at[step, 0, halves(c)], zs.at[step], zr.at[step, c], ahead),
            remote(from_high, zin.at[step, 1, halves(c)], zs.at[step], zr.at[step, c], behind),
        ]

    def halo_in(step, c):
        return [remote(zpk.at[:, halves(c)], zin.at[step, :, halves(c)], zs.at[step], zr.at[step, c], ahead)]

    def halo_all(step):
        return [remote(zpk, zin.at[step], zs.at[step], zr.at[step, 0], ahead)]

    def beside_out(c):
        return spread(pkb.at[:, halves(c)], rxb.at[b, halves(c)], bs.at[0], br.at[c])

    def beside_in(c):
        return gather(pkb.at[:, halves(c)], rxb.at[:, halves(c)], bs.at[0], br.at[c], TEAM - 1)

    def beside_all():
        return gather(pkb, rxb, bs.at[0], br.at[0], TEAM - 1)

    def edges_out():
        return spread(ce, cein.at[b], es.at[0], er.at[0])

    def edges_in():
        return gather(ce, cein, es.at[0], er.at[0], TEAM - 1)

    right, left = base + mates[0], base + mates[2]

    later = pl.ds(8 * EARLY, 8 * (COMM - EARLY))

    def sides_out():
        return [
            remote(ex.at[1, later], exin.at[0, later], fs.at[0], fr.at[0], right),
            remote(ex.at[1, later], exin.at[1, later], fs.at[0], fr.at[0], left),
        ]

    def sides():
        return [remote(ex.at[:, later], exin.at[:, later], fs.at[0], fr.at[0], right)]

    def meta_out():
        return [remote(mbuf, meta.at[b], ms.at[0], mr.at[0], base + d) for d in mates]

    def meta_in():
        return gather(meta, meta, ms.at[0], mr.at[0], TEAM - 1)

    def row_refs(step):
        return (osm, orx, os_, or_) if step == 0 else (sbuf, srx, ss, sr)

    def row_out(step):
        src, dst, ssem, rsem = row_refs(step)
        inner = [remote(src, dst.at[b + 1], ssem.at[0], rsem.at[0], base + d) for d in mates]
        before = [
            remote(src, dst.at[TEAM + 1], ssem.at[1], rsem.at[0], wrap(base - TEAM + k)) for k in range(TEAM)
        ]
        after = [remote(src, dst.at[0], ssem.at[1], rsem.at[0], wrap(base + TEAM + k)) for k in range(TEAM)]
        return inner, before, after

    def row_start(step):
        inner, before, after = row_out(step)

        @pl.when(b == 0)
        def _():
            start(before)

        @pl.when(b == TEAM - 1)
        def _():
            start(after)

        start(inner)

    def row_sent(step):
        src, dst, ssem, rsem = row_refs(step)
        sent(gather(dst, dst, ssem.at[0], rsem.at[0], TEAM - 1))

        @pl.when((b == 0) | (b == TEAM - 1))
        def _():
            sent(gather(dst, dst, ssem.at[1], rsem.at[0], TEAM))

    def row_in(step):
        src, dst, ssem, rsem = row_refs(step)
        return gather(dst, dst, ssem.at[0], rsem.at[0], TEAM + 1)

    def drift_out():
        copies = [
            remote(dm.at[0], drx.at[TEAM + b], ds_.at[0], dr.at[1], wrap(base - 1)),
            remote(dm.at[TEAM + 1], drx.at[TEAM + b], ds_.at[0], dr.at[1], wrap(base + TEAM)),
        ]
        return copies + [remote(dm.at[d + 1], drx.at[b], ds_.at[0], dr.at[0], base + d) for d in mates]

    def drift_all():
        return gather(dm, drx, ds_.at[0], dr.at[0], TEAM + 1)

    def drift_in():
        return gather(dm, drx, ds_.at[0], dr.at[0], TEAM - 1), gather(dm, drx, ds_.at[0], dr.at[1], TEAM)

    def zonal_out(step):
        src = currents.at[0] if step == 0 else state.at[0]
        return [
            remote(src, zhalo.at[step, 0], us.at[step], ur.at[step], up),
            remote(src, zhalo.at[step, 1], us.at[step], ur.at[step], down),
        ]

    def zonal_pair(step):
        return [remote(currents, zhalo.at[step], us.at[step], ur.at[step], up)]

    def last_out():
        return [
            remote(dbuf.at[0], dhalo.at[0], hs.at[0], hr.at[0], up),
            remote(dbuf.at[1], dhalo.at[1], hs.at[0], hr.at[0], down),
        ]

    def last_pair():
        return [remote(dbuf, dhalo, hs.at[0], hr.at[0], up)]

    start(loads)
    drx[TEAM : 2 * TEAM] = jnp.zeros((TEAM, levels, lanes), F32)
    barrier = pltpu.get_barrier_semaphore()
    partners = [base + d for d in mates]
    partners += [wrap(base - TEAM + k) for k in range(TEAM)] + [wrap(base + TEAM + k) for k in range(TEAM)]
    for p in partners:
        pl.semaphore_signal(
            barrier, inc=1, device_id=(lax.div(p, dev_count), lax.rem(p, dev_count)), device_id_type=MESH
        )

    lane = lax.broadcasted_iota(jnp.int32, (half, lanes), 1)
    low = lane < width

    def even(a, c):
        return jnp.where(low, a, pltpu.roll(c, width, 1))

    def odd(a, c):
        return jnp.where(low, pltpu.roll(a, width, 1), c)

    lane_row = lax.broadcasted_iota(jnp.int32, (8, lanes), 1)
    wide_lane = lax.broadcasted_iota(jnp.int32, (size, lanes), 1)
    rim = lax.rem(wide_lane + 1, width) < 2

    def pack_rim(first, second):
        mixed = jnp.where(rim, first, pltpu.roll(second, 2, 1))
        out = jnp.zeros((8, lanes), F32)
        for g in range(size // 8):
            here = lax.rem(lane_row + 1 - 4 * g + lanes, width) < 4
            part = mixed[8 * g : 8 * g + 8]
            out = jnp.where(here, pltpu.roll(part, 4 * g, 1) if g else part, out)
        return out

    for load in loads:
        load.wait()
    pl.semaphore_wait(barrier, len(partners))

    def pack_in(c):
        for t in range(2):
            tile = spec[rows(c), t * lanes : (t + 1) * lanes]
            first, second = tile[0:half], tile[half:size]
            pk[2 * t, halves(c), :] = even(first, second)
            pk[2 * t + 1, halves(c), :] = odd(first, second)
        rx[0, b, halves(c), :] = pk[b, halves(c), :]
        start(piece_out(0, c))

    each(0, 1, pack_in)
    lraw[...] = jnp.zeros_like(lraw)
    lraw[0:1, 0:levels] = mixing[...]
    lraw[1:2, 0:levels] = sweight[...]
    lcols = jnp.transpose(lraw[...])
    level_mix = lcols[0:levels, 0:1]
    level_weight = lcols[0:levels, 1:2]

    def surface(source, dst, at):
        dst[at : at + 8, :] = jnp.zeros((8, cells), F32)
        for a in range(2):
            dst[at + a : at + a + 1, :] = jnp.sum(level_weight * source[a], axis=0, keepdims=True)

    osm[0:4, :] = oidx[...].astype(F32)
    osm[4:8, :] = owt[...]
    surface(currents, osm, 8)
    orx[b + 1] = osm[...]
    row_start(0)
    mbuf[0:4, :] = pidx[...].astype(F32)
    mbuf[0:1, :] = (2 * pidx[0:1, :] + wet[...]).astype(F32)
    mbuf[4:8, :] = pwt[...]
    meta[b] = mbuf[...]
    start(meta_out())
    each(1, 2, pack_in)

    def rim_in(c):
        ex[0, span(c, 8), :] = pack_rim(spec[rows(c), 0:lanes], spec[rows(c), lanes : 2 * lanes])

    each(0, COMM, rim_in)
    last = width - 1
    from_left = (1, last, lanes - 1, last + 2)
    from_right = (width, 2, width + 2, 0)
    quarter = lax.rem(lane_row, 4)
    ahead_half = lane_row < width
    for d in range(TEAM):
        for v in range(COMM // 4):
            out = jnp.zeros((8, lanes), F32)
            for k in range(4):
                part = ex[0, 8 * (4 * v + k) : 8 * (4 * v + k) + 8, :]
                west = pltpu.roll(part, (k - from_left[d]) % lanes, 1)
                east = pltpu.roll(part, (width + k - from_right[d]) % lanes, 1)
                out = jnp.where(quarter == k, jnp.where(ahead_half, west, east), out)
            ce[d, 8 * v : 8 * v + 8, :] = out
    cein[b] = ce[b]
    start(edges_out())
    each(2, COMM, pack_in)
    start(zonal_out(0))
    araw[...] = jnp.zeros_like(araw)
    araw[0:2, :] = courant[...]
    araw[2:4, :] = (2 * sign[...] - 1).astype(F32)
    araw[4:5, :] = nonlinear[...]
    for j in range(4):
        index, weight = qidx[j], qwt[j]
        twice = index[0:1] == index[1:2]
        araw[8 + 2 * j : 10 + 2 * j, :] = index.astype(F32)
        araw[16 + 2 * j : 17 + 2 * j, :] = jnp.where(twice, weight[0:1] + weight[1:2], weight[0:1])
        araw[17 + 2 * j : 18 + 2 * j, :] = weight[1:2]
    cols[...] = jnp.transpose(araw[...])
    long_lane = lax.broadcasted_iota(jnp.int32, (32, comps), 1).astype(F32)

    def build_quad(c):
        for sub in range(size // 32):
            begin = pl.multiple_of(c * size + sub * 32, 32)
            col = cols[pl.ds(begin, 32), :]
            for j in range(4):
                two = jnp.where(col[:, 9 + 2 * j : 10 + 2 * j] == long_lane, col[:, 17 + 2 * j : 18 + 2 * j], 0.0)
                one = jnp.where(col[:, 8 + 2 * j : 9 + 2 * j] == long_lane, col[:, 16 + 2 * j : 17 + 2 * j], two)
                quad[pl.ds(begin + j * comps, 32), :] = one.astype(BF16)

    def forward(c):
        received(piece_in(0, c))
        start(halo(0, c))

    each(0, COMM // 2, build_quad)
    forward(0)
    each(COMM // 2, COMM - 1, build_quad)
    forward(1)
    each(COMM - 1, COMM, build_quad)
    received(meta_in())
    aside = lax.rem(b, 2)
    for t in range(2):
        pieces = []
        for r in (2 * t, 2 * t + 1):
            tile = meta[r, :, pl.ds(pl.multiple_of(lax.div(b, 2) * lanes, lanes), lanes)]
            pieces.append(jnp.where(aside == r % 2, tile, pltpu.roll(tile, width, 1)))
        bmeta[0:8, t * lanes : (t + 1) * lanes] = jnp.where(low[0:8], pieces[0], pieces[1])

    joined = bmeta[0:1, :]
    halved = jnp.floor(0.5 * joined)
    bmeta[8:9, :] = joined - 2.0 * halved
    bmeta[0:1, :] = halved
    received(row_in(0))
    slots = lax.broadcasted_iota(jnp.int32, (cells, points), 0).astype(F32)
    for q in range(TEAM + 2):
        owner = (wrap(base - 1 + q) * cells).astype(F32)
        value = jnp.zeros((cells, points), F32)
        for j in range(4):
            value = value + jnp.where(bmeta[j : j + 1, :] - owner == slots, bmeta[4 + j : 5 + j, :], 0.0)
        ptab[0, q * cells : (q + 1) * cells, :], ptab[1, q * cells : (q + 1) * cells, :] = split(value)

    shift = lax.rem(cells + window // 2 - window * b, cells)
    pointer = lax.broadcasted_iota(jnp.int32, (width, cells), 0).astype(F32)
    for t in range((TEAM + 2) // 2):
        near = pltpu.roll(orx[2 * t, 0:8], shift, 1)
        far = pltpu.roll(orx[2 * t + 1, 0:8], shift, 1)
        both = jnp.where(low[0:8], near, pltpu.roll(far, width, 1))
        for r in range(TEAM):
            origin = ((base + r) * points + width * b).astype(F32)
            value = jnp.zeros((width, cells), F32)
            for j in range(4):
                value = value + jnp.where(both[j : j + 1, :] - origin == pointer, both[4 + j : 5 + j, :], 0.0)
            high_part, low_part = split(value)
            btab[0, r * width : (r + 1) * width, t * lanes : (t + 1) * lanes] = high_part
            btab[1, r * width : (r + 1) * width, t * lanes : (t + 1) * lanes] = low_part

    forward(2)
    received(edges_in())
    lane_rim = lax.broadcasted_iota(jnp.int32, (8 * COMM, lanes), 1)
    upper = lane_row >= last
    to_left = (last, lanes - 1, last + 2, 1)
    to_right = (0, width, 2, width + 2)
    on_left = (
        (quarter == 3) & upper & (lane_row < lanes - 1),
        (quarter == 3) & ((lane_row < last) | (lane_row == lanes - 1)),
        (quarter == 1) & upper,
        (quarter == 1) & ~upper,
    )
    on_right = ((quarter == 0) & ~upper, (quarter == 0) & upper, (quarter == 2) & ~upper, (quarter == 2) & upper)
    for c in range(COMM):
        v, k = c // 4, c % 4
        out = jnp.zeros((8, lanes), F32)
        for r in range(TEAM):
            part = cein[r, 8 * v : 8 * v + 8, :]
            out = jnp.where(on_left[r], pltpu.roll(part, (to_left[r] - k) % lanes, 1), out)
            out = jnp.where(on_right[r], pltpu.roll(part, (to_right[r] - width - k) % lanes, 1), out)
        edge[0, 8 * c : 8 * c + 8, :] = out

    def flow(step):
        for q in range(TEAM + 2):
            sall[:, q * cells : (q + 1) * cells] = orx[q, 8:16] if step == 0 else srx[q]
        tan[...] = jnp.tanh(dot_split(sall[...], ptab[0], ptab[1]))

    flow(0)

    lane_half = lax.rem(lane, width)
    at_first, at_last = lane_half == 0, lane_half == width - 1

    unit = half
    low_unit = low[0:unit]
    at_first, at_last = at_first[0:unit], at_last[0:unit]

    def advect(step, c, emit):
        received(halo_in(step, c))

        def body(r):
            packed = pl.ds(pl.multiple_of(c * half + r * unit, unit), unit)
            turn = lax.rem(lanes - 4 * (unit // 8) * r, lanes)
            rim_row = pltpu.roll(edge[step, span(c, 8), :], turn, 1)
            out = []
            for sub in range(2):
                at = pl.ds(pl.multiple_of(c * size + sub * half + r * unit, unit), unit)
                col = cols[at, :]
                if step == 0:
                    own = []
                    for t in range(2):
                        a, d = rx[0, 2 * t, packed, :], rx[0, 2 * t + 1, packed, :]
                        if sub:
                            own.append(jnp.where(low_unit, pltpu.roll(a, width, 1), d))
                        else:
                            own.append(jnp.where(low_unit, a, pltpu.roll(d, width, 1)))
                else:
                    own = [mid[at, t * lanes : (t + 1) * lanes] for t in range(2)]
                turned = [pltpu.roll(x, width, 1) for x in own]
                below, above = zin[step, 0, packed, :], zin[step, 1, packed, :]
                if sub:
                    below = pltpu.roll(below, width, 1)
                else:
                    above = pltpu.roll(above, width, 1)
                middle = jnp.where(low_unit, turned[0], turned[1])
                north = (jnp.where(low_unit, below, turned[0]), middle)
                south = (middle, jnp.where(low_unit, turned[1], above))
                groups = range(sub * half // 8, sub * half // 8 + unit // 8)
                spin = [
                    jnp.concatenate([pltpu.roll(rim_row, (k - 4 * g) % lanes, 1) for g in groups], axis=0)
                    for k in (width + 1, width - 1, width - 3)
                ]
                sense_x, sense_y = col[:, 2:3], col[:, 3:4]
                values = []
                for t in range(2):
                    x = own[t]
                    west = jnp.where(at_first, spin[t], pltpu.roll(x, 1, 1))
                    east = jnp.where(at_last, spin[t + 1], pltpu.roll(x, lanes - 1, 1))
                    behind_x = jnp.where(sense_x > 0, west, east)
                    behind_y = jnp.where(sense_y > 0, north[t], south[t])
                    lane_at = slice(t * lanes, (t + 1) * lanes)
                    speed_x = col[:, 0:1] * (1.0 + 0.5 * (sense_x * tan[0:1, lane_at]))
                    speed_y = col[:, 1:2] * (1.0 + 0.5 * (sense_y * tan[1:2, lane_at]))
                    values.append(x - speed_x * (x - behind_x) - speed_y * (x - behind_y))
                out.append(values)
            emit(c, r, out)

        each(0, half // unit, body)

    def keep(c, r, values):
        for sub in range(2):
            at = pl.ds(pl.multiple_of(c * size + sub * half + r * unit, unit), unit)
            for t in range(2):
                adv[at, t * lanes : (t + 1) * lanes] = values[sub][t]
                advb[at, t * lanes : (t + 1) * lanes] = values[sub][t].astype(BF16)

    deep = comps // KPARTS

    def multiply(part):
        k_at = slice(part * deep, (part + 1) * deep)

        def body(i):
            if part:
                acc[...] = acc[...] + dot(quad[:, k_at], advb[k_at, :])
            else:
                acc[...] = dot(quad[:, k_at], advb[k_at, :])

        each(none, none + 1, body)

    def halo_out(c):
        tiles = [mid[rows(c), t * lanes : (t + 1) * lanes] for t in range(2)]
        zpk[0, halves(c), :] = odd(tiles[1][0:half], tiles[1][half:size])
        zpk[1, halves(c), :] = even(tiles[0][0:half], tiles[0][half:size])
        start(halo(1, c))

    def rim_out(c):
        ex[1, span(c, 8), :] = pack_rim(mid[rows(c), 0:lanes], mid[rows(c), lanes : 2 * lanes])

    def source(step, wet_row):
        target = mid if step == 0 else spec_out

        def body(c):
            at = rows(c)
            terms = [acc[pl.ds(pl.multiple_of(j * comps + c * size, size), size), :] for j in range(4)]
            value = adv[at, :]
            total_sum = terms[0] + terms[1] + terms[2] + terms[3]
            pair_sum = terms[0] * terms[1] + terms[2] * terms[3]
            new = wet_row * (value + cols[at, 4:5] * (value * value * total_sum - value * pair_sum))
            target[at, :] = new
            midb[at, :] = new.astype(BF16)

        if step == 0:
            each(0, 1, body)
            each(0, 1, halo_out)
            each(1, COMM, body)
        else:
            each(0, COMM, body)

    level_row = lax.broadcasted_iota(jnp.int32, (levels, cells), 0)

    def mix(w):
        above = jnp.where(level_row == 0, w, pltpu.roll(w, 1, 0))
        below = jnp.where(level_row == levels - 1, w, pltpu.roll(w, levels - 1, 0))
        return level_mix * (above - 2.0 * w + below)

    def ocean(step, drift):
        before = currents if step == 0 else state
        target = state if step == 0 else cur_out
        received(zonal_pair(step))
        u, v = before[0], before[1]
        rot = coriolis[...]
        turn = 0.5 * (pltpu.roll(v, cells - 1, 1) - pltpu.roll(v, 1, 1)) - 0.5 * (zhalo[step, 1] - zhalo[step, 0])
        mix_u, mix_v = mix(u), mix(v)
        drift_x, drift_y = drift()
        target[0] = u + OCEAN_STEP * (rot * (v + drift_y) + turn * drift_y + mix_u)
        target[1] = v + OCEAN_STEP * (-rot * (u + drift_x) - turn * drift_x + mix_v)

    oslots = lax.broadcasted_iota(jnp.int32, (points, cells), 0).astype(F32)
    origin = (pos * points).astype(F32)

    def last_table(q):
        value = jnp.zeros((points, cells), F32)
        for j in range(4):
            value = value + jnp.where(
                orx[b + q, j : j + 1, :] - origin == oslots, orx[b + q, 4 + j : 5 + j, :], 0.0
            )
        otab[q, 0], otab[q, 1] = split(value)
        owner = (wrap(pos - 1 + q) * cells).astype(F32)
        value = jnp.zeros((cells, points), F32)
        for j in range(4):
            value = value + jnp.where(pidx[j : j + 1, :].astype(F32) - owner == slots, pwt[j : j + 1, :], 0.0)
        rtab[0, q * cells : (q + 1) * cells, :], rtab[1, q * cells : (q + 1) * cells, :] = split(value)

    for c in range(3, COMM):
        forward(c)
        advect(0, c - 3, keep)
        if (c - 3) % 2:
            multiply((c - 3) // 2)
    advect(0, COMM - 3, keep)
    multiply(2)
    advect(0, COMM - 2, keep)
    advect(0, COMM - 1, keep)
    multiply(KPARTS - 1)
    source(0, bmeta[8:9, :])

    stokes = dot(table[...], midb[...])
    parts = dot_split(stokes, btab[0], btab[1])
    for t in range((TEAM + 2) // 2):
        zonal = parts[0:levels, t * lanes : (t + 1) * lanes]
        merid = parts[levels : 2 * levels, t * lanes : (t + 1) * lanes]
        dm[2 * t], dm[2 * t + 1] = even(zonal, merid), odd(zonal, merid)
    start(drift_out())
    drx[b] = dm[b + 1]
    def own_out(c):
        for t in range(2):
            tile = mid[rows(c), t * lanes : (t + 1) * lanes]
            first, second = tile[0:half], tile[half:size]
            pk2[2 * t, halves(c), :] = even(first, second)
            pk2[2 * t + 1, halves(c), :] = odd(first, second)
        start(piece_out(1, c))
        rx[1, b, halves(c), :] = pk2[b, halves(c), :]

    each(1, 2, halo_out)
    each(0, EARLY - 1, own_out)
    each(EARLY, COMM, rim_out)
    start(sides_out())
    for q in range(3):
        last_table(q)

    def team_drift():
        inner, outer = drift_in()
        received(inner)

        @pl.when((b == 0) | (b == TEAM - 1))
        def _():
            received(outer)

        drift_x = jnp.zeros((levels, cells), F32)
        drift_y = jnp.zeros((levels, cells), F32)
        for s in range(TEAM):
            part = drx[s] + drx[TEAM + s]
            to = (window * s - window // 2) % cells
            drift_x += pltpu.roll(jnp.where(low, part, 0.0), to, 1)
            drift_y += pltpu.roll(jnp.where(low, pltpu.roll(part, width, 1), 0.0), to, 1)
        return drift_x, drift_y

    ocean(0, team_drift)
    surface(state, sbuf, 0)
    row_start(1)
    each(2, 5, halo_out)
    each(EARLY - 1, EARLY, own_out)
    each(5, COMM, halo_out)
    srx[b + 1] = sbuf[...]

    def beside(c):
        received(halo_in(1, c))
        sides_y = []
        for sub in range(2):
            at = pl.ds(pl.multiple_of(c * size + sub * half, half), half)
            turned = [pltpu.roll(mid[at, t * lanes : (t + 1) * lanes], width, 1) for t in range(2)]
            below, above = zin[1, 0, halves(c), :], zin[1, 1, halves(c), :]
            if sub:
                below = pltpu.roll(below, width, 1)
            else:
                above = pltpu.roll(above, width, 1)
            middle = jnp.where(low, turned[0], turned[1])
            north = (jnp.where(low, below, turned[0]), middle)
            south = (middle, jnp.where(low, turned[1], above))
            sense_y = cols[at, 3:4]
            sides_y.append([jnp.where(sense_y > 0, north[t], south[t]) for t in range(2)])
        for t in range(2):
            pkb[2 * t, halves(c), :] = even(sides_y[0][t], sides_y[1][t])
            pkb[2 * t + 1, halves(c), :] = odd(sides_y[0][t], sides_y[1][t])
        start(beside_out(c))
        rxb[b, halves(c), :] = pkb[b, halves(c), :]

    each(0, EARLY, beside)
    received(sides())
    edge[1, later, :] = jnp.where(lax.rem(lane_rim[8 * EARLY :], 2) == 1, exin[0, later, :], exin[1, later, :])
    received(row_in(1))
    flow(1)

    def stack(c, r, values):
        packed = pl.ds(pl.multiple_of(c * half + r * unit, unit), unit)
        for t in range(2):
            first, second = values[0][t], values[1][t]
            pk2[2 * t, packed, :] = jnp.where(low_unit, first, pltpu.roll(second, width, 1))
            pk2[2 * t + 1, packed, :] = jnp.where(low_unit, pltpu.roll(first, width, 1), second)

    def give(c):
        advect(1, c, stack)
        start(piece_out(1, c))
        rx[1, b, halves(c), :] = pk2[b, halves(c), :]

    def take(c):
        received(piece_in(1, c))
        for sub, join in enumerate((even, odd)):
            at = pl.ds(pl.multiple_of(c * size + sub * half, half), half)
            for t in range(2):
                value = join(rx[1, 2 * t, halves(c), :], rx[1, 2 * t + 1, halves(c), :])
                adv[at, t * lanes : (t + 1) * lanes] = value
                advb[at, t * lanes : (t + 1) * lanes] = value.astype(BF16)

    def flow_row():
        own_part = sall[:, pl.ds(pl.multiple_of(b * cells, cells), 3 * cells)]
        tanr[...] = jnp.tanh(dot_split(own_part, rtab[0], rtab[1]))

    def advance(c):
        received(piece_in(1, c))
        received(beside_in(c))
        for sub, join in enumerate((even, odd)):
            at = pl.ds(pl.multiple_of(c * size + sub * half, half), half)
            col = cols[at, :]
            sense_x, sense_y = col[:, 2:3], col[:, 3:4]
            own = [join(rx[1, 2 * t, halves(c), :], rx[1, 2 * t + 1, halves(c), :]) for t in range(2)]
            behind_y = [join(rxb[2 * t, halves(c), :], rxb[2 * t + 1, halves(c), :]) for t in range(2)]
            forth = [pltpu.roll(x, 1, 1) for x in own]
            back = [pltpu.roll(x, lanes - 1, 1) for x in own]
            for t in range(2):
                x = own[t]
                west = jnp.where(lane == 0, forth[1 - t], forth[t])
                east = jnp.where(lane == lanes - 1, back[1 - t], back[t])
                behind_x = jnp.where(sense_x > 0, west, east)
                lane_at = slice(t * lanes, (t + 1) * lanes)
                speed_x = col[:, 0:1] * (1.0 + 0.5 * (sense_x * tanr[0:1, lane_at]))
                speed_y = col[:, 1:2] * (1.0 + 0.5 * (sense_y * tanr[1:2, lane_at]))
                value = x - speed_x * (x - behind_x) - speed_y * (x - behind_y[t])
                adv[at, lane_at] = value
                advb[at, lane_at] = value.astype(BF16)

    each(EARLY, COMM, give)
    start(zonal_out(1))
    flow_row()
    for c in range(COMM):
        advance(c) if c < EARLY else take(c)
        if c % 2:
            multiply(c // 2)
    source(1, wet[...].astype(F32))

    stokes = dot(table[...], midb[...])
    copies = last_out()
    dbuf[0] = dot_split(stokes, otab[2, 0], otab[2, 1])
    copies[0].start()
    dbuf[1] = dot_split(stokes, otab[0, 0], otab[0, 1])
    copies[1].start()
    dself[...] = dot_split(stokes, otab[1, 0], otab[1, 1])

    def last_drift():
        received(last_pair())
        drift = dself[...] + dhalo[0] + dhalo[1]
        return drift[0:levels], drift[levels : 2 * levels]

    ocean(1, last_drift)

    sent(beside_all())
    sent(meta_in())
    sent(edges_in())
    sent(sides())
    sent(drift_all())
    sent(last_pair())
    for step in range(STEPS):
        row_sent(step)
        sent(zonal_pair(step))
        sent(piece_all(step))
        sent(halo_all(step))


def local(
    spectrum, water_mask, courant, stencil_sign, quad_index, quad_weight, nonlinear, stokes_table,
    point_index, point_weight, ocean_index, ocean_weight, currents, coriolis, mixing, surface_weights,
):
    comps, points = spectrum.shape
    levels, cells = currents.shape[1:]
    lanes = points // 2
    packed = comps // 2
    rim = comps // 16
    vm = pl.BlockSpec(memory_space=pltpu.VMEM)
    dma = pltpu.SemaphoreType.DMA

    def f32(*shape):
        return pltpu.VMEM(shape, F32)

    def bf16(*shape):
        return pltpu.VMEM(shape, BF16)

    scratch = [
        f32(128, comps),
        f32(comps, 128),
        f32(128, 128),
        bf16(4 * comps, comps),
        f32(TEAM, packed, lanes),
        f32(TEAM, packed, lanes),
        f32(TEAM, packed * EARLY // COMM, lanes),
        f32(STEPS, TEAM, packed, lanes),
        f32(TEAM, packed * EARLY // COMM, lanes),
        f32(2, packed, lanes),
        f32(STEPS, 2, packed, lanes),
        f32(STEPS, rim, lanes),
        f32(2, rim, lanes),
        f32(TEAM, rim // 4, lanes),
        f32(TEAM, rim // 4, lanes),
        f32(STEPS, rim, lanes),
        f32(comps, points),
        bf16(comps, points),
        f32(4 * comps, points),
        f32(comps, points),
        bf16(comps, points),
        f32(2, levels, cells),
        f32(8, points),
        f32(TEAM, 8, points),
        f32(16, points),
        f32(16, cells),
        f32(TEAM + 2, 16, cells),
        f32(8, cells),
        f32(TEAM + 2, 8, cells),
        f32(8, (TEAM + 2) * cells),
        f32(STEPS, 2, levels, cells),
        bf16(2, (TEAM + 2) * cells, points),
        bf16(2, 3 * cells, points),
        bf16(2, points, (TEAM + 2) // 2 * lanes),
        bf16(3, 2, points, cells),
        f32(TEAM + 2, levels, lanes),
        f32(2 * TEAM, levels, lanes),
        f32(2, 2 * levels, cells),
        f32(2, 2 * levels, cells),
        f32(2 * levels, cells),
        f32(8, points),
        f32(8, points),
        dma((STEPS,)),
        dma((STEPS, COMM)),
        dma((1,)),
        dma((EARLY,)),
        dma((STEPS,)),
        dma((STEPS, COMM)),
        dma((1,)),
        dma((1,)),
        dma((1,)),
        dma((1,)),
        dma((1,)),
        dma((1,)),
        dma((2,)),
        dma((1,)),
        dma((2,)),
        dma((1,)),
        dma((1,)),
        dma((2,)),
        dma((STEPS,)),
        dma((STEPS,)),
        dma((1,)),
        dma((1,)),
    ]
    operands = (
        spectrum,
        water_mask.reshape(1, points),
        courant,
        stencil_sign,
        quad_index.transpose(0, 2, 1),
        quad_weight.transpose(0, 2, 1),
        nonlinear.reshape(1, comps),
        stokes_table,
        point_index,
        point_weight,
        ocean_index,
        ocean_weight,
        currents,
        coriolis.reshape(1, cells),
        mixing.reshape(1, levels),
        surface_weights.reshape(1, levels),
    )
    scratch = [pltpu.VMEM(x.shape, x.dtype) for x in operands] + [dma((INPUTS,))] + scratch
    return pl.pallas_call(
        wave_kernel,
        out_shape=(
            pltpu.VMEM((comps, points), F32),
            pltpu.VMEM(currents.shape, F32),
        ),
        in_specs=[pl.BlockSpec(memory_space=pltpu.HBM)] * INPUTS,
        out_specs=(vm, vm),
        scratch_shapes=scratch,
        compiler_params=pltpu.CompilerParams(
            collective_id=0, has_side_effects=True, vmem_limit_bytes=56 * 1024 * 1024
        ),
    )(*operands)


def solution(mesh):
    ring = P(("mp", "dev"))
    split_last = P(None, ("mp", "dev"))
    deep = P(None, None, ("mp", "dev"))
    return jax.shard_map(
        local,
        mesh=mesh,
        in_specs=(
            split_last, ring, P(), P(), P(), P(), P(), P(), split_last, split_last, split_last, split_last, deep,
            ring, P(), P(),
        ),
        out_specs=(split_last, deep),
        check_vma=False,
    )
```

```python
import jax
import jax.numpy as jnp
from jax import lax
from jax.experimental import pallas as pl
from jax.experimental.pallas import tpu as pltpu
from jax.sharding import PartitionSpec as P

STEPS = 2
OCEAN_STEP = 0.5
TEAM = 4
COMM = 8
EARLY = 3
INPUTS = 16
KPARTS = 4
MESH = pl.DeviceIdType.MESH
F32, BF16 = jnp.float32, jnp.bfloat16


def split(x):
    high = x.astype(BF16)
    return high, (x - high.astype(F32)).astype(BF16)


def dot(a, b):
    return jnp.dot(a, b, preferred_element_type=F32)


def dot_split(x, table_high, table_low):
    high, low = split(x)
    return dot(high, table_high) + (dot(low, table_high) + dot(high, table_low))


def wave_kernel(*refs):
    given, (spec_out, cur_out), scratch = refs[:INPUTS], refs[INPUTS : INPUTS + 2], refs[INPUTS + 2 :]
    copied, load_sems, rest = scratch[:INPUTS], scratch[INPUTS], scratch[INPUTS + 1 :]
    loads = [pltpu.make_async_copy(a, c, load_sems.at[i]) for i, (a, c) in enumerate(zip(given, copied))]
    wave_body(loads, *copied, spec_out, cur_out, *rest)


def wave_body(
    loads,
    spec, wet, courant, sign, qidx, qwt, nonlinear, table, pidx, pwt, oidx, owt,
    currents, coriolis, mixing, sweight,
    spec_out, cur_out,
    araw, cols, lraw, quad, pk, pk2, pkb, rx, rxb, zpk, zin, ex, exin, ce, cein, edge, adv, advb, acc, mid, midb, state,
    mbuf, meta, bmeta, osm, orx, sbuf, srx, sall, zhalo, ptab, rtab, btab, otab, dm, drx, dbuf, dhalo, dself, tan, tanr,
    rxs, rxr, bs, br, zs, zr, es, er, fs, fr, ms, mr, os_, or_, ss, sr, ds_, dr, us, ur, hs, hr, hello,
):
    comps, points = spec.shape
    cells = coriolis.shape[1]
    levels = mixing.shape[1]
    dev_count = lax.axis_size("dev")
    total = lax.axis_size("mp") * dev_count
    pos = lax.axis_index("mp") * dev_count + lax.axis_index("dev")
    b = lax.rem(pos, TEAM)
    base = pos - b
    width = points // TEAM
    window = cells // TEAM
    size = comps // COMM
    half = size // 2
    lanes = 2 * width

    none = lax.div(pos, total)

    def wrap(p):
        return lax.rem(p + total, total)

    up, down = wrap(pos + 1), wrap(pos - 1)
    ahead, behind = wrap(pos + TEAM), wrap(pos - TEAM)
    mates = [lax.rem(b + i, TEAM) for i in range(1, TEAM)]

    def remote(src, dst, ssem, rsem, p):
        return pltpu.make_async_remote_copy(
            src_ref=src, dst_ref=dst, send_sem=ssem, recv_sem=rsem,
            device_id=(lax.div(p, dev_count), lax.rem(p, dev_count)), device_id_type=MESH,
        )

    def span(c, n):
        return pl.ds(pl.multiple_of(c * n, n), n)

    def rows(c):
        return span(c, size)

    def halves(c):
        return span(c, half)

    def each(low, high, body):
        def run(c, carry):
            body(c)
            return carry

        lax.fori_loop(low, high, run, 0)

    def start(copies):
        for copy in copies:
            copy.start()

    def received(copies):
        for copy in copies:
            copy.wait_recv()

    def sent(copies):
        for copy in copies:
            copy.wait_send()

    def spread(src, dst, ssem, rsem):
        return [remote(src.at[d], dst, ssem, rsem, base + d) for d in mates]

    def gather(src, dst, ssem, rsem, count):
        return [remote(src.at[0:count], dst.at[0:count], ssem, rsem, base + mates[0])]

    def piece(step, c):
        return (pk if step == 0 else pk2).at[:, halves(c)], rx.at[step, :, halves(c)]

    def piece_out(step, c):
        src, dst = piece(step, c)
        return spread(src, dst.at[b], rxs.at[step], rxr.at[step, c])

    def piece_in(step, c):
        src, dst = piece(step, c)
        return gather(src, dst, rxs.at[step], rxr.at[step, c], TEAM - 1)

    def piece_all(step):
        return gather(pk if step == 0 else pk2, rx.at[step], rxs.at[step], rxr.at[step, 0], TEAM - 1)

    def halo(step, c):
        from_low = rx.at[0, TEAM - 1, halves(c)] if step == 0 else zpk.at[0, halves(c)]
        from_high = rx.at[0, 0, halves(c)] if step == 0 else zpk.at[1, halves(c)]
        return [
            remote(from_low, zin.at[step, 0, halves(c)], zs.at[step], zr.at[step, c], ahead),
            remote(from_high, zin.at[step, 1, halves(c)], zs.at[step], zr.at[step, c], behind),
        ]

    def halo_in(step, c):
        return [remote(zpk.at[:, halves(c)], zin.at[step, :, halves(c)], zs.at[step], zr.at[step, c], ahead)]

    def halo_all(step):
        return [remote(zpk, zin.at[step], zs.at[step], zr.at[step, 0], ahead)]

    def beside_out(c):
        return spread(pkb.at[:, halves(c)], rxb.at[b, halves(c)], bs.at[0], br.at[c])

    def beside_in(c):
        return gather(pkb.at[:, halves(c)], rxb.at[:, halves(c)], bs.at[0], br.at[c], TEAM - 1)

    def beside_all():
        return gather(pkb, rxb, bs.at[0], br.at[0], TEAM - 1)

    def edges_out():
        return spread(ce, cein.at[b], es.at[0], er.at[0])

    def edges_in():
        return gather(ce, cein, es.at[0], er.at[0], TEAM - 1)

    right, left = base + mates[0], base + mates[2]

    later = pl.ds(8 * EARLY, 8 * (COMM - EARLY))

    def sides_out():
        return [
            remote(ex.at[1, later], exin.at[0, later], fs.at[0], fr.at[0], right),
            remote(ex.at[1, later], exin.at[1, later], fs.at[0], fr.at[0], left),
        ]

    def sides():
        return [remote(ex.at[:, later], exin.at[:, later], fs.at[0], fr.at[0], right)]

    def meta_out():
        return [remote(mbuf, meta.at[b], ms.at[0], mr.at[0], base + d) for d in mates]

    def meta_in():
        return gather(meta, meta, ms.at[0], mr.at[0], TEAM - 1)

    def row_refs(step):
        return (osm, orx, os_, or_) if step == 0 else (sbuf, srx, ss, sr)

    def row_out(step):
        src, dst, ssem, rsem = row_refs(step)
        inner = [remote(src, dst.at[b + 1], ssem.at[0], rsem.at[0], base + d) for d in mates]
        before = [
            remote(src, dst.at[TEAM + 1], ssem.at[1], rsem.at[0], wrap(base - TEAM + k)) for k in range(TEAM)
        ]
        after = [remote(src, dst.at[0], ssem.at[1], rsem.at[0], wrap(base + TEAM + k)) for k in range(TEAM)]
        return inner, before, after

    def row_start(step):
        start(row_out(step)[0])

    def row_start_outer(step):
        inner, before, after = row_out(step)

        @pl.when(b == 0)
        def _():
            start(before)

        @pl.when(b == TEAM - 1)
        def _():
            start(after)

    def row_sent(step):
        src, dst, ssem, rsem = row_refs(step)
        sent(gather(dst, dst, ssem.at[0], rsem.at[0], TEAM - 1))

        @pl.when((b == 0) | (b == TEAM - 1))
        def _():
            sent(gather(dst, dst, ssem.at[1], rsem.at[0], TEAM))

    def row_in(step):
        src, dst, ssem, rsem = row_refs(step)
        return gather(dst, dst, ssem.at[0], rsem.at[0], TEAM + 1)

    def drift_out():
        copies = [
            remote(dm.at[0], drx.at[TEAM + b], ds_.at[0], dr.at[1], wrap(base - 1)),
            remote(dm.at[TEAM + 1], drx.at[TEAM + b], ds_.at[0], dr.at[1], wrap(base + TEAM)),
        ]
        return copies + [remote(dm.at[d + 1], drx.at[b], ds_.at[0], dr.at[0], base + d) for d in mates]

    def drift_all():
        return gather(dm, drx, ds_.at[0], dr.at[0], TEAM + 1)

    def drift_in():
        return gather(dm, drx, ds_.at[0], dr.at[0], TEAM - 1), gather(dm, drx, ds_.at[0], dr.at[1], TEAM)

    def zonal_out(step):
        src = currents.at[0] if step == 0 else state.at[0]
        return [
            remote(src, zhalo.at[step, 0], us.at[step], ur.at[step], up),
            remote(src, zhalo.at[step, 1], us.at[step], ur.at[step], down),
        ]

    def zonal_pair(step):
        return [remote(currents, zhalo.at[step], us.at[step], ur.at[step], up)]

    def last_out():
        return [
            remote(dbuf.at[0], dhalo.at[0], hs.at[0], hr.at[0], up),
            remote(dbuf.at[1], dhalo.at[1], hs.at[0], hr.at[0], down),
        ]

    def last_pair():
        return [remote(dbuf, dhalo, hs.at[0], hr.at[0], up)]

    start(loads)
    drx[TEAM : 2 * TEAM] = jnp.zeros((TEAM, levels, lanes), F32)
    barrier = pltpu.get_barrier_semaphore()

    def greet(sem, p):
        pl.semaphore_signal(
            sem, inc=1, device_id=(lax.div(p, dev_count), lax.rem(p, dev_count)), device_id_type=MESH
        )

    partners = [base + d for d in mates] + [ahead, behind]
    for p in partners:
        greet(barrier, p)

    lane = lax.broadcasted_iota(jnp.int32, (half, lanes), 1)
    low = lane < width

    def even(a, c):
        return jnp.where(low, a, pltpu.roll(c, width, 1))

    def odd(a, c):
        return jnp.where(low, pltpu.roll(a, width, 1), c)

    lane_row = lax.broadcasted_iota(jnp.int32, (8, lanes), 1)
    wide_lane = lax.broadcasted_iota(jnp.int32, (size, lanes), 1)
    rim = lax.rem(wide_lane + 1, width) < 2

    def pack_rim(first, second):
        mixed = jnp.where(rim, first, pltpu.roll(second, 2, 1))
        out = jnp.zeros((8, lanes), F32)
        for g in range(size // 8):
            here = lax.rem(lane_row + 1 - 4 * g + lanes, width) < 4
            part = mixed[8 * g : 8 * g + 8]
            out = jnp.where(here, pltpu.roll(part, 4 * g, 1) if g else part, out)
        return out

    for load in loads:
        load.wait()
    pl.semaphore_wait(barrier, len(partners))
    greet(hello, ahead)
    greet(hello, behind)

    def pack_in(c):
        for t in range(2):
            tile = spec[rows(c), t * lanes : (t + 1) * lanes]
            first, second = tile[0:half], tile[half:size]
            pk[2 * t, halves(c), :] = even(first, second)
            pk[2 * t + 1, halves(c), :] = odd(first, second)
        rx[0, b, halves(c), :] = pk[b, halves(c), :]
        start(piece_out(0, c))

    each(0, 1, pack_in)
    lraw[...] = jnp.zeros_like(lraw)
    lraw[0:1, 0:levels] = mixing[...]
    lraw[1:2, 0:levels] = sweight[...]
    lcols = jnp.transpose(lraw[...])
    level_mix = lcols[0:levels, 0:1]
    level_weight = lcols[0:levels, 1:2]

    def surface(source, dst, at):
        dst[at : at + 8, :] = jnp.zeros((8, cells), F32)
        for a in range(2):
            dst[at + a : at + a + 1, :] = jnp.sum(level_weight * source[a], axis=0, keepdims=True)

    osm[0:4, :] = oidx[...].astype(F32)
    osm[4:8, :] = owt[...]
    surface(currents, osm, 8)
    orx[b + 1] = osm[...]
    row_start(0)
    mbuf[0:4, :] = pidx[...].astype(F32)
    mbuf[0:1, :] = (2 * pidx[0:1, :] + wet[...]).astype(F32)
    mbuf[4:8, :] = pwt[...]
    meta[b] = mbuf[...]
    start(meta_out())
    each(1, 2, pack_in)

    def rim_in(c):
        ex[0, span(c, 8), :] = pack_rim(spec[rows(c), 0:lanes], spec[rows(c), lanes : 2 * lanes])

    each(0, COMM, rim_in)
    last = width - 1
    from_left = (1, last, lanes - 1, last + 2)
    from_right = (width, 2, width + 2, 0)
    quarter = lax.rem(lane_row, 4)
    ahead_half = lane_row < width
    for d in range(TEAM):
        for v in range(COMM // 4):
            out = jnp.zeros((8, lanes), F32)
            for k in range(4):
                part = ex[0, 8 * (4 * v + k) : 8 * (4 * v + k) + 8, :]
                west = pltpu.roll(part, (k - from_left[d]) % lanes, 1)
                east = pltpu.roll(part, (width + k - from_right[d]) % lanes, 1)
                out = jnp.where(quarter == k, jnp.where(ahead_half, west, east), out)
            ce[d, 8 * v : 8 * v + 8, :] = out
    cein[b] = ce[b]
    start(edges_out())
    each(2, COMM, pack_in)
    pl.semaphore_wait(hello, 2)
    row_start_outer(0)
    start(zonal_out(0))
    araw[...] = jnp.zeros_like(araw)
    araw[0:2, :] = courant[...]
    araw[2:4, :] = (2 * sign[...] - 1).astype(F32)
    araw[4:5, :] = nonlinear[...]
    for j in range(4):
        index, weight = qidx[j], qwt[j]
        twice = index[0:1] == index[1:2]
        araw[8 + 2 * j : 10 + 2 * j, :] = index.astype(F32)
        araw[16 + 2 * j : 17 + 2 * j, :] = jnp.where(twice, weight[0:1] + weight[1:2], weight[0:1])
        araw[17 + 2 * j : 18 + 2 * j, :] = weight[1:2]
    cols[...] = jnp.transpose(araw[...])
    long_lane = lax.broadcasted_iota(jnp.int32, (32, comps), 1).astype(F32)

    def build_quad(c):
        for sub in range(size // 32):
            begin = pl.multiple_of(c * size + sub * 32, 32)
            col = cols[pl.ds(begin, 32), :]
            for j in range(4):
                two = jnp.where(col[:, 9 + 2 * j : 10 + 2 * j] == long_lane, col[:, 17 + 2 * j : 18 + 2 * j], 0.0)
                one = jnp.where(col[:, 8 + 2 * j : 9 + 2 * j] == long_lane, col[:, 16 + 2 * j : 17 + 2 * j], two)
                quad[pl.ds(begin + j * comps, 32), :] = one.astype(BF16)

    def forward(c):
        received(piece_in(0, c))
        start(halo(0, c))

    each(0, COMM // 2, build_quad)
    forward(0)
    each(COMM // 2, COMM - 1, build_quad)
    forward(1)
    each(COMM - 1, COMM, build_quad)
    received(meta_in())
    aside = lax.rem(b, 2)
    for t in range(2):
        pieces = []
        for r in (2 * t, 2 * t + 1):
            tile = meta[r, :, pl.ds(pl.multiple_of(lax.div(b, 2) * lanes, lanes), lanes)]
            pieces.append(jnp.where(aside == r % 2, tile, pltpu.roll(tile, width, 1)))
        bmeta[0:8, t * lanes : (t + 1) * lanes] = jnp.where(low[0:8], pieces[0], pieces[1])

    joined = bmeta[0:1, :]
    halved = jnp.floor(0.5 * joined)
    bmeta[8:9, :] = joined - 2.0 * halved
    bmeta[0:1, :] = halved
    received(row_in(0))
    slots = lax.broadcasted_iota(jnp.int32, (cells, points), 0).astype(F32)
    for q in range(TEAM + 2):
        owner = (wrap(base - 1 + q) * cells).astype(F32)
        value = jnp.zeros((cells, points), F32)
        for j in range(4):
            value = value + jnp.where(bmeta[j : j + 1, :] - owner == slots, bmeta[4 + j : 5 + j, :], 0.0)
        ptab[0, q * cells : (q + 1) * cells, :], ptab[1, q * cells : (q + 1) * cells, :] = split(value)

    shift = lax.rem(cells + window // 2 - window * b, cells)
    pointer = lax.broadcasted_iota(jnp.int32, (width, cells), 0).astype(F32)
    for t in range((TEAM + 2) // 2):
        near = pltpu.roll(orx[2 * t, 0:8], shift, 1)
        far = pltpu.roll(orx[2 * t + 1, 0:8], shift, 1)
        both = jnp.where(low[0:8], near, pltpu.roll(far, width, 1))
        for r in range(TEAM):
            origin = ((base + r) * points + width * b).astype(F32)
            value = jnp.zeros((width, cells), F32)
            for j in range(4):
                value = value + jnp.where(both[j : j + 1, :] - origin == pointer, both[4 + j : 5 + j, :], 0.0)
            high_part, low_part = split(value)
            btab[0, r * width : (r + 1) * width, t * lanes : (t + 1) * lanes] = high_part
            btab[1, r * width : (r + 1) * width, t * lanes : (t + 1) * lanes] = low_part

    forward(2)
    received(edges_in())
    lane_rim = lax.broadcasted_iota(jnp.int32, (8 * COMM, lanes), 1)
    upper = lane_row >= last
    to_left = (last, lanes - 1, last + 2, 1)
    to_right = (0, width, 2, width + 2)
    on_left = (
        (quarter == 3) & upper & (lane_row < lanes - 1),
        (quarter == 3) & ((lane_row < last) | (lane_row == lanes - 1)),
        (quarter == 1) & upper,
        (quarter == 1) & ~upper,
    )
    on_right = ((quarter == 0) & ~upper, (quarter == 0) & upper, (quarter == 2) & ~upper, (quarter == 2) & upper)
    for c in range(COMM):
        v, k = c // 4, c % 4
        out = jnp.zeros((8, lanes), F32)
        for r in range(TEAM):
            part = cein[r, 8 * v : 8 * v + 8, :]
            out = jnp.where(on_left[r], pltpu.roll(part, (to_left[r] - k) % lanes, 1), out)
            out = jnp.where(on_right[r], pltpu.roll(part, (to_right[r] - width - k) % lanes, 1), out)
        edge[0, 8 * c : 8 * c + 8, :] = out

    def flow(step):
        for q in range(TEAM + 2):
            sall[:, q * cells : (q + 1) * cells] = orx[q, 8:16] if step == 0 else srx[q]
        tan[...] = jnp.tanh(dot_split(sall[...], ptab[0], ptab[1]))

    flow(0)

    lane_half = lax.rem(lane, width)
    at_first, at_last = lane_half == 0, lane_half == width - 1

    unit = half
    low_unit = low[0:unit]
    at_first, at_last = at_first[0:unit], at_last[0:unit]

    def advect(step, c, emit):
        received(halo_in(step, c))

        def body(r):
            packed = pl.ds(pl.multiple_of(c * half + r * unit, unit), unit)
            turn = lax.rem(lanes - 4 * (unit // 8) * r, lanes)
            rim_row = pltpu.roll(edge[step, span(c, 8), :], turn, 1)
            out = []
            for sub in range(2):
                at = pl.ds(pl.multiple_of(c * size + sub * half + r * unit, unit), unit)
                col = cols[at, :]
                if step == 0:
                    own = []
                    for t in range(2):
                        a, d = rx[0, 2 * t, packed, :], rx[0, 2 * t + 1, packed, :]
                        if sub:
                            own.append(jnp.where(low_unit, pltpu.roll(a, width, 1), d))
                        else:
                            own.append(jnp.where(low_unit, a, pltpu.roll(d, width, 1)))
                else:
                    own = [mid[at, t * lanes : (t + 1) * lanes] for t in range(2)]
                turned = [pltpu.roll(x, width, 1) for x in own]
                below, above = zin[step, 0, packed, :], zin[step, 1, packed, :]
                if sub:
                    below = pltpu.roll(below, width, 1)
                else:
                    above = pltpu.roll(above, width, 1)
                middle = jnp.where(low_unit, turned[0], turned[1])
                north = (jnp.where(low_unit, below, turned[0]), middle)
                south = (middle, jnp.where(low_unit, turned[1], above))
                groups = range(sub * half // 8, sub * half // 8 + unit // 8)
                spin = [
                    jnp.concatenate([pltpu.roll(rim_row, (k - 4 * g) % lanes, 1) for g in groups], axis=0)
                    for k in (width + 1, width - 1, width - 3)
                ]
                sense_x, sense_y = col[:, 2:3], col[:, 3:4]
                values = []
                for t in range(2):
                    x = own[t]
                    west = jnp.where(at_first, spin[t], pltpu.roll(x, 1, 1))
                    east = jnp.where(at_last, spin[t + 1], pltpu.roll(x, lanes - 1, 1))
                    behind_x = jnp.where(sense_x > 0, west, east)
                    behind_y = jnp.where(sense_y > 0, north[t], south[t])
                    lane_at = slice(t * lanes, (t + 1) * lanes)
                    speed_x = col[:, 0:1] * (1.0 + 0.5 * (sense_x * tan[0:1, lane_at]))
                    speed_y = col[:, 1:2] * (1.0 + 0.5 * (sense_y * tan[1:2, lane_at]))
                    values.append(x - speed_x * (x - behind_x) - speed_y * (x - behind_y))
                out.append(values)
            emit(c, r, out)

        each(0, half // unit, body)

    def keep(c, r, values):
        for sub in range(2):
            at = pl.ds(pl.multiple_of(c * size + sub * half + r * unit, unit), unit)
            for t in range(2):
                adv[at, t * lanes : (t + 1) * lanes] = values[sub][t]
                advb[at, t * lanes : (t + 1) * lanes] = values[sub][t].astype(BF16)

    deep = comps // KPARTS

    def multiply(part):
        k_at = slice(part * deep, (part + 1) * deep)

        def body(i):
            if part:
                acc[...] = acc[...] + dot(quad[:, k_at], advb[k_at, :])
            else:
                acc[...] = dot(quad[:, k_at], advb[k_at, :])

        each(none, none + 1, body)

    def halo_out(c):
        tiles = [mid[rows(c), t * lanes : (t + 1) * lanes] for t in range(2)]
        zpk[0, halves(c), :] = odd(tiles[1][0:half], tiles[1][half:size])
        zpk[1, halves(c), :] = even(tiles[0][0:half], tiles[0][half:size])
        start(halo(1, c))

    def rim_out(c):
        ex[1, span(c, 8), :] = pack_rim(mid[rows(c), 0:lanes], mid[rows(c), lanes : 2 * lanes])

    def source(step, wet_row):
        target = mid if step == 0 else spec_out

        def body(c):
            at = rows(c)
            terms = [acc[pl.ds(pl.multiple_of(j * comps + c * size, size), size), :] for j in range(4)]
            value = adv[at, :]
            total_sum = terms[0] + terms[1] + terms[2] + terms[3]
            pair_sum = terms[0] * terms[1] + terms[2] * terms[3]
            new = wet_row * (value + cols[at, 4:5] * (value * value * total_sum - value * pair_sum))
            target[at, :] = new
            midb[at, :] = new.astype(BF16)

        if step == 0:
            each(0, 1, body)
            each(0, 1, halo_out)
            each(1, COMM, body)
        else:
            each(0, COMM, body)

    level_row = lax.broadcasted_iota(jnp.int32, (levels, cells), 0)

    def mix(w):
        above = jnp.where(level_row == 0, w, pltpu.roll(w, 1, 0))
        below = jnp.where(level_row == levels - 1, w, pltpu.roll(w, levels - 1, 0))
        return level_mix * (above - 2.0 * w + below)

    def ocean(step, drift):
        before = currents if step == 0 else state
        target = state if step == 0 else cur_out
        received(zonal_pair(step))
        u, v = before[0], before[1]
        rot = coriolis[...]
        turn = 0.5 * (pltpu.roll(v, cells - 1, 1) - pltpu.roll(v, 1, 1)) - 0.5 * (zhalo[step, 1] - zhalo[step, 0])
        mix_u, mix_v = mix(u), mix(v)
        drift_x, drift_y = drift()
        target[0] = u + OCEAN_STEP * (rot * (v + drift_y) + turn * drift_y + mix_u)
        target[1] = v + OCEAN_STEP * (-rot * (u + drift_x) - turn * drift_x + mix_v)

    oslots = lax.broadcasted_iota(jnp.int32, (points, cells), 0).astype(F32)
    origin = (pos * points).astype(F32)

    def last_table(q):
        value = jnp.zeros((points, cells), F32)
        for j in range(4):
            value = value + jnp.where(
                orx[b + q, j : j + 1, :] - origin == oslots, orx[b + q, 4 + j : 5 + j, :], 0.0
            )
        otab[q, 0], otab[q, 1] = split(value)
        owner = (wrap(pos - 1 + q) * cells).astype(F32)
        value = jnp.zeros((cells, points), F32)
        for j in range(4):
            value = value + jnp.where(pidx[j : j + 1, :].astype(F32) - owner == slots, pwt[j : j + 1, :], 0.0)
        rtab[0, q * cells : (q + 1) * cells, :], rtab[1, q * cells : (q + 1) * cells, :] = split(value)

    for c in range(3, COMM):
        forward(c)
        advect(0, c - 3, keep)
        if (c - 3) % 2:
            multiply((c - 3) // 2)
    advect(0, COMM - 3, keep)
    multiply(2)
    advect(0, COMM - 2, keep)
    advect(0, COMM - 1, keep)
    multiply(KPARTS - 1)
    source(0, bmeta[8:9, :])

    stokes = dot(table[...], midb[...])
    parts = dot_split(stokes, btab[0], btab[1])
    for t in range((TEAM + 2) // 2):
        zonal = parts[0:levels, t * lanes : (t + 1) * lanes]
        merid = parts[levels : 2 * levels, t * lanes : (t + 1) * lanes]
        dm[2 * t], dm[2 * t + 1] = even(zonal, merid), odd(zonal, merid)
    start(drift_out())
    drx[b] = dm[b + 1]
    def own_out(c):
        for t in range(2):
            tile = mid[rows(c), t * lanes : (t + 1) * lanes]
            first, second = tile[0:half], tile[half:size]
            pk2[2 * t, halves(c), :] = even(first, second)
            pk2[2 * t + 1, halves(c), :] = odd(first, second)
        start(piece_out(1, c))
        rx[1, b, halves(c), :] = pk2[b, halves(c), :]

    each(1, 3, halo_out)
    each(0, EARLY - 1, own_out)
    each(EARLY, COMM, rim_out)
    start(sides_out())
    for q in range(3):
        last_table(q)

    def team_drift():
        inner, outer = drift_in()
        received(inner)

        @pl.when((b == 0) | (b == TEAM - 1))
        def _():
            received(outer)

        drift_x = jnp.zeros((levels, cells), F32)
        drift_y = jnp.zeros((levels, cells), F32)
        for s in range(TEAM):
            part = drx[s] + drx[TEAM + s]
            to = (window * s - window // 2) % cells
            drift_x += pltpu.roll(jnp.where(low, part, 0.0), to, 1)
            drift_y += pltpu.roll(jnp.where(low, pltpu.roll(part, width, 1), 0.0), to, 1)
        return drift_x, drift_y

    ocean(0, team_drift)
    surface(state, sbuf, 0)
    row_start_outer(1)
    row_start(1)
    each(3, 5, halo_out)
    each(EARLY - 1, EARLY, own_out)
    each(5, COMM, halo_out)
    srx[b + 1] = sbuf[...]

    def beside(c):
        received(halo_in(1, c))
        sides_y = []
        for sub in range(2):
            at = pl.ds(pl.multiple_of(c * size + sub * half, half), half)
            turned = [pltpu.roll(mid[at, t * lanes : (t + 1) * lanes], width, 1) for t in range(2)]
            below, above = zin[1, 0, halves(c), :], zin[1, 1, halves(c), :]
            if sub:
                below = pltpu.roll(below, width, 1)
            else:
                above = pltpu.roll(above, width, 1)
            middle = jnp.where(low, turned[0], turned[1])
            north = (jnp.where(low, below, turned[0]), middle)
            south = (middle, jnp.where(low, turned[1], above))
            sense_y = cols[at, 3:4]
            sides_y.append([jnp.where(sense_y > 0, north[t], south[t]) for t in range(2)])
        for t in range(2):
            pkb[2 * t, halves(c), :] = even(sides_y[0][t], sides_y[1][t])
            pkb[2 * t + 1, halves(c), :] = odd(sides_y[0][t], sides_y[1][t])
        start(beside_out(c))
        rxb[b, halves(c), :] = pkb[b, halves(c), :]

    each(0, EARLY, beside)
    received(sides())
    edge[1, later, :] = jnp.where(lax.rem(lane_rim[8 * EARLY :], 2) == 1, exin[0, later, :], exin[1, later, :])
    received(row_in(1))
    flow(1)

    def stack(c, r, values):
        packed = pl.ds(pl.multiple_of(c * half + r * unit, unit), unit)
        for t in range(2):
            first, second = values[0][t], values[1][t]
            pk2[2 * t, packed, :] = jnp.where(low_unit, first, pltpu.roll(second, width, 1))
            pk2[2 * t + 1, packed, :] = jnp.where(low_unit, pltpu.roll(first, width, 1), second)

    def give(c):
        advect(1, c, stack)
        start(piece_out(1, c))
        rx[1, b, halves(c), :] = pk2[b, halves(c), :]

    def take(c):
        received(piece_in(1, c))
        for sub, join in enumerate((even, odd)):
            at = pl.ds(pl.multiple_of(c * size + sub * half, half), half)
            for t in range(2):
                value = join(rx[1, 2 * t, halves(c), :], rx[1, 2 * t + 1, halves(c), :])
                adv[at, t * lanes : (t + 1) * lanes] = value
                advb[at, t * lanes : (t + 1) * lanes] = value.astype(BF16)

    def flow_row():
        own_part = sall[:, pl.ds(pl.multiple_of(b * cells, cells), 3 * cells)]
        tanr[...] = jnp.tanh(dot_split(own_part, rtab[0], rtab[1]))

    def advance(c):
        received(piece_in(1, c))
        received(beside_in(c))
        for sub, join in enumerate((even, odd)):
            at = pl.ds(pl.multiple_of(c * size + sub * half, half), half)
            col = cols[at, :]
            sense_x, sense_y = col[:, 2:3], col[:, 3:4]
            own = [join(rx[1, 2 * t, halves(c), :], rx[1, 2 * t + 1, halves(c), :]) for t in range(2)]
            behind_y = [join(rxb[2 * t, halves(c), :], rxb[2 * t + 1, halves(c), :]) for t in range(2)]
            forth = [pltpu.roll(x, 1, 1) for x in own]
            back = [pltpu.roll(x, lanes - 1, 1) for x in own]
            for t in range(2):
                x = own[t]
                west = jnp.where(lane == 0, forth[1 - t], forth[t])
                east = jnp.where(lane == lanes - 1, back[1 - t], back[t])
                behind_x = jnp.where(sense_x > 0, west, east)
                lane_at = slice(t * lanes, (t + 1) * lanes)
                speed_x = col[:, 0:1] * (1.0 + 0.5 * (sense_x * tanr[0:1, lane_at]))
                speed_y = col[:, 1:2] * (1.0 + 0.5 * (sense_y * tanr[1:2, lane_at]))
                value = x - speed_x * (x - behind_x) - speed_y * (x - behind_y[t])
                adv[at, lane_at] = value
                advb[at, lane_at] = value.astype(BF16)

    each(EARLY, COMM, give)
    start(zonal_out(1))
    flow_row()
    for c in range(COMM):
        advance(c) if c < EARLY else take(c)
        if c % 2:
            multiply(c // 2)
    source(1, wet[...].astype(F32))

    stokes = dot(table[...], midb[...])
    copies = last_out()
    dbuf[0] = dot_split(stokes, otab[2, 0], otab[2, 1])
    copies[0].start()
    dbuf[1] = dot_split(stokes, otab[0, 0], otab[0, 1])
    copies[1].start()
    dself[...] = dot_split(stokes, otab[1, 0], otab[1, 1])

    def last_drift():
        received(last_pair())
        drift = dself[...] + dhalo[0] + dhalo[1]
        return drift[0:levels], drift[levels : 2 * levels]

    ocean(1, last_drift)

    sent(beside_all())
    sent(meta_in())
    sent(edges_in())
    sent(sides())
    sent(drift_all())
    sent(last_pair())
    for step in range(STEPS):
        row_sent(step)
        sent(zonal_pair(step))
        sent(piece_all(step))
        sent(halo_all(step))


def local(
    spectrum, water_mask, courant, stencil_sign, quad_index, quad_weight, nonlinear, stokes_table,
    point_index, point_weight, ocean_index, ocean_weight, currents, coriolis, mixing, surface_weights,
):
    comps, points = spectrum.shape
    levels, cells = currents.shape[1:]
    lanes = points // 2
    packed = comps // 2
    rim = comps // 16
    vm = pl.BlockSpec(memory_space=pltpu.VMEM)
    dma = pltpu.SemaphoreType.DMA

    def f32(*shape):
        return pltpu.VMEM(shape, F32)

    def bf16(*shape):
        return pltpu.VMEM(shape, BF16)

    scratch = [
        f32(128, comps),
        f32(comps, 128),
        f32(128, 128),
        bf16(4 * comps, comps),
        f32(TEAM, packed, lanes),
        f32(TEAM, packed, lanes),
        f32(TEAM, packed * EARLY // COMM, lanes),
        f32(STEPS, TEAM, packed, lanes),
        f32(TEAM, packed * EARLY // COMM, lanes),
        f32(2, packed, lanes),
        f32(STEPS, 2, packed, lanes),
        f32(STEPS, rim, lanes),
        f32(2, rim, lanes),
        f32(TEAM, rim // 4, lanes),
        f32(TEAM, rim // 4, lanes),
        f32(STEPS, rim, lanes),
        f32(comps, points),
        bf16(comps, points),
        f32(4 * comps, points),
        f32(comps, points),
        bf16(comps, points),
        f32(2, levels, cells),
        f32(8, points),
        f32(TEAM, 8, points),
        f32(16, points),
        f32(16, cells),
        f32(TEAM + 2, 16, cells),
        f32(8, cells),
        f32(TEAM + 2, 8, cells),
        f32(8, (TEAM + 2) * cells),
        f32(STEPS, 2, levels, cells),
        bf16(2, (TEAM + 2) * cells, points),
        bf16(2, 3 * cells, points),
        bf16(2, points, (TEAM + 2) // 2 * lanes),
        bf16(3, 2, points, cells),
        f32(TEAM + 2, levels, lanes),
        f32(2 * TEAM, levels, lanes),
        f32(2, 2 * levels, cells),
        f32(2, 2 * levels, cells),
        f32(2 * levels, cells),
        f32(8, points),
        f32(8, points),
        dma((STEPS,)),
        dma((STEPS, COMM)),
        dma((1,)),
        dma((EARLY,)),
        dma((STEPS,)),
        dma((STEPS, COMM)),
        dma((1,)),
        dma((1,)),
        dma((1,)),
        dma((1,)),
        dma((1,)),
        dma((1,)),
        dma((2,)),
        dma((1,)),
        dma((2,)),
        dma((1,)),
        dma((1,)),
        dma((2,)),
        dma((STEPS,)),
        dma((STEPS,)),
        dma((1,)),
        dma((1,)),
        pltpu.SemaphoreType.REGULAR,
    ]
    operands = (
        spectrum,
        water_mask.reshape(1, points),
        courant,
        stencil_sign,
        quad_index.transpose(0, 2, 1),
        quad_weight.transpose(0, 2, 1),
        nonlinear.reshape(1, comps),
        stokes_table,
        point_index,
        point_weight,
        ocean_index,
        ocean_weight,
        currents,
        coriolis.reshape(1, cells),
        mixing.reshape(1, levels),
        surface_weights.reshape(1, levels),
    )
    scratch = [pltpu.VMEM(x.shape, x.dtype) for x in operands] + [dma((INPUTS,))] + scratch
    return pl.pallas_call(
        wave_kernel,
        out_shape=(
            pltpu.VMEM((comps, points), F32),
            pltpu.VMEM(currents.shape, F32),
        ),
        in_specs=[pl.BlockSpec(memory_space=pltpu.HBM)] * INPUTS,
        out_specs=(vm, vm),
        scratch_shapes=scratch,
        compiler_params=pltpu.CompilerParams(
            collective_id=0, has_side_effects=True, vmem_limit_bytes=56 * 1024 * 1024
        ),
    )(*operands)


def solution(mesh):
    ring = P(("mp", "dev"))
    split_last = P(None, ("mp", "dev"))
    deep = P(None, None, ("mp", "dev"))
    return jax.shard_map(
        local,
        mesh=mesh,
        in_specs=(
            split_last, ring, P(), P(), P(), P(), P(), P(), split_last, split_last, split_last, split_last, deep,
            ring, P(), P(),
        ),
        out_specs=(split_last, deep),
        check_vma=False,
    )
```

```python
import jax
import jax.numpy as jnp
from jax import lax
from jax.experimental import pallas as pl
from jax.experimental.pallas import tpu as pltpu
from jax.sharding import PartitionSpec as P

STEPS = 2
OCEAN_STEP = 0.5
TEAM = 4
COMM = 8
EARLY = 2
INPUTS = 16
KPARTS = 4
MESH = pl.DeviceIdType.MESH
F32, BF16 = jnp.float32, jnp.bfloat16


def split(x):
    high = x.astype(BF16)
    return high, (x - high.astype(F32)).astype(BF16)


def dot(a, b):
    return jnp.dot(a, b, preferred_element_type=F32)


def dot_split(x, table_high, table_low):
    rows = x.shape[0]
    high, low = split(x)
    main = dot(jnp.concatenate([high, low], axis=0), table_high)
    return main[0:rows] + (main[rows:] + dot(high, table_low))


def wave_kernel(*refs):
    given, (spec_out, cur_out), scratch = refs[:INPUTS], refs[INPUTS : INPUTS + 2], refs[INPUTS + 2 :]
    copied, load_sems, rest = scratch[:INPUTS], scratch[INPUTS], scratch[INPUTS + 1 :]
    head = given[0].shape[0] // COMM
    pairs = [(given[0].at[0:head], copied[0].at[0:head])] + list(zip(given[1:], copied[1:]))
    pairs.append((given[0].at[head:], copied[0].at[head:]))
    loads = [pltpu.make_async_copy(a, c, load_sems.at[i]) for i, (a, c) in enumerate(pairs)]
    wave_body(loads, *copied, spec_out, cur_out, *rest)


def wave_body(
    loads,
    spec, wet, courant, sign, qidx, qwt, nonlinear, table, pidx, pwt, oidx, owt,
    currents, coriolis, mixing, sweight,
    spec_out, cur_out,
    araw, cols, lraw, quad, pk, pk2, pkb, rx, rxb, zpk, zin, ex, exin, ce, cein, edge, adv, advb, acc, mid, midb, state,
    mbuf, meta, bmeta, osm, orx, sbuf, srx, sall, zhalo, ptab, rtab, btab, otab, dm, drx, dbuf, dhalo, dself, tan, tanr,
    rxs, rxr, bs, br, zs, zr, es, er, fs, fr, ms, mr, os_, or_, ss, sr, ds_, dr, us, ur, hs, hr, hello,
):
    comps, points = spec.shape
    cells = coriolis.shape[1]
    levels = mixing.shape[1]
    dev_count = lax.axis_size("dev")
    total = lax.axis_size("mp") * dev_count
    pos = lax.axis_index("mp") * dev_count + lax.axis_index("dev")
    b = lax.rem(pos, TEAM)
    base = pos - b
    width = points // TEAM
    window = cells // TEAM
    size = comps // COMM
    half = size // 2
    lanes = 2 * width

    none = lax.div(pos, total)

    def wrap(p):
        return lax.rem(p + total, total)

    up, down = wrap(pos + 1), wrap(pos - 1)
    ahead, behind = wrap(pos + TEAM), wrap(pos - TEAM)
    mates = [lax.rem(b + i, TEAM) for i in range(1, TEAM)]

    def remote(src, dst, ssem, rsem, p):
        return pltpu.make_async_remote_copy(
            src_ref=src, dst_ref=dst, send_sem=ssem, recv_sem=rsem,
            device_id=(lax.div(p, dev_count), lax.rem(p, dev_count)), device_id_type=MESH,
        )

    def span(c, n):
        return pl.ds(pl.multiple_of(c * n, n), n)

    def rows(c):
        return span(c, size)

    def halves(c):
        return span(c, half)

    def each(low, high, body):
        def run(c, carry):
            body(c)
            return carry

        lax.fori_loop(low, high, run, 0)

    def start(copies):
        for copy in copies:
            copy.start()

    def received(copies):
        for copy in copies:
            copy.wait_recv()

    def sent(copies):
        for copy in copies:
            copy.wait_send()

    def spread(src, dst, ssem, rsem):
        return [remote(src.at[d], dst, ssem, rsem, base + d) for d in mates]

    def gather(src, dst, ssem, rsem, count):
        return [remote(src.at[0:count], dst.at[0:count], ssem, rsem, base + mates[0])]

    def piece(step, c):
        return (pk if step == 0 else pk2).at[:, halves(c)], rx.at[step, :, halves(c)]

    def piece_out(step, c):
        src, dst = piece(step, c)
        return spread(src, dst.at[b], rxs.at[step], rxr.at[step, c])

    def piece_in(step, c):
        src, dst = piece(step, c)
        return gather(src, dst, rxs.at[step], rxr.at[step, c], TEAM - 1)

    def piece_all(step):
        return gather(pk if step == 0 else pk2, rx.at[step], rxs.at[step], rxr.at[step, 0], TEAM - 1)

    def halo(step, c):
        from_low = rx.at[0, TEAM - 1, halves(c)] if step == 0 else zpk.at[0, halves(c)]
        from_high = rx.at[0, 0, halves(c)] if step == 0 else zpk.at[1, halves(c)]
        return [
            remote(from_low, zin.at[step, 0, halves(c)], zs.at[step], zr.at[step, c], ahead),
            remote(from_high, zin.at[step, 1, halves(c)], zs.at[step], zr.at[step, c], behind),
        ]

    def halo_in(step, c):
        return [remote(zpk.at[:, halves(c)], zin.at[step, :, halves(c)], zs.at[step], zr.at[step, c], ahead)]

    def halo_all(step):
        return [remote(zpk, zin.at[step], zs.at[step], zr.at[step, 0], ahead)]

    def beside_out(c):
        return spread(pkb.at[:, halves(c)], rxb.at[b, halves(c)], bs.at[0], br.at[c])

    def beside_in(c):
        return gather(pkb.at[:, halves(c)], rxb.at[:, halves(c)], bs.at[0], br.at[c], TEAM - 1)

    def beside_all():
        return gather(pkb, rxb, bs.at[0], br.at[0], TEAM - 1)

    def edges_out():
        return spread(ce, cein.at[b], es.at[0], er.at[0])

    def edges_in():
        return gather(ce, cein, es.at[0], er.at[0], TEAM - 1)

    right, left = base + mates[0], base + mates[2]

    later = pl.ds(8 * EARLY, 8 * (COMM - EARLY))

    def sides_out():
        return [
            remote(ex.at[1, later], exin.at[0, later], fs.at[0], fr.at[0], right),
            remote(ex.at[1, later], exin.at[1, later], fs.at[0], fr.at[0], left),
        ]

    def sides():
        return [remote(ex.at[:, later], exin.at[:, later], fs.at[0], fr.at[0], right)]

    def meta_out():
        return [remote(mbuf, meta.at[b], ms.at[0], mr.at[0], base + d) for d in mates]

    def meta_in():
        return gather(meta, meta, ms.at[0], mr.at[0], TEAM - 1)

    def row_refs(step):
        return (osm, orx, os_, or_) if step == 0 else (sbuf, srx, ss, sr)

    def row_out(step):
        src, dst, ssem, rsem = row_refs(step)
        inner = [remote(src, dst.at[b + 1], ssem.at[0], rsem.at[0], base + d) for d in mates]
        before = [
            remote(src, dst.at[TEAM + 1], ssem.at[1], rsem.at[0], wrap(base - TEAM + k)) for k in range(TEAM)
        ]
        after = [remote(src, dst.at[0], ssem.at[1], rsem.at[0], wrap(base + TEAM + k)) for k in range(TEAM)]
        return inner, before, after

    def row_start(step):
        start(row_out(step)[0])

    def row_start_outer(step):
        inner, before, after = row_out(step)

        @pl.when(b == 0)
        def _():
            start(before)

        @pl.when(b == TEAM - 1)
        def _():
            start(after)

    def row_sent(step):
        src, dst, ssem, rsem = row_refs(step)
        sent(gather(dst, dst, ssem.at[0], rsem.at[0], TEAM - 1))

        @pl.when((b == 0) | (b == TEAM - 1))
        def _():
            sent(gather(dst, dst, ssem.at[1], rsem.at[0], TEAM))

    def row_in(step):
        src, dst, ssem, rsem = row_refs(step)
        return gather(dst, dst, ssem.at[0], rsem.at[0], TEAM + 1)

    def drift_out():
        copies = [
            remote(dm.at[0], drx.at[TEAM + b], ds_.at[0], dr.at[1], wrap(base - 1)),
            remote(dm.at[TEAM + 1], drx.at[TEAM + b], ds_.at[0], dr.at[1], wrap(base + TEAM)),
        ]
        return copies + [remote(dm.at[d + 1], drx.at[b], ds_.at[0], dr.at[0], base + d) for d in mates]

    def drift_all():
        return gather(dm, drx, ds_.at[0], dr.at[0], TEAM + 1)

    def drift_in():
        return gather(dm, drx, ds_.at[0], dr.at[0], TEAM - 1), gather(dm, drx, ds_.at[0], dr.at[1], TEAM)

    def zonal_out(step):
        src = currents.at[0] if step == 0 else state.at[0]
        return [
            remote(src, zhalo.at[step, 0], us.at[step], ur.at[step], up),
            remote(src, zhalo.at[step, 1], us.at[step], ur.at[step], down),
        ]

    def zonal_pair(step):
        return [remote(currents, zhalo.at[step], us.at[step], ur.at[step], up)]

    def last_out():
        return [
            remote(dbuf.at[0], dhalo.at[0], hs.at[0], hr.at[0], up),
            remote(dbuf.at[1], dhalo.at[1], hs.at[0], hr.at[0], down),
        ]

    def last_pair():
        return [remote(dbuf, dhalo, hs.at[0], hr.at[0], up)]

    start(loads)
    drx[TEAM : 2 * TEAM] = jnp.zeros((TEAM, levels, lanes), F32)
    barrier = pltpu.get_barrier_semaphore()

    def greet(sem, p):
        pl.semaphore_signal(
            sem, inc=1, device_id=(lax.div(p, dev_count), lax.rem(p, dev_count)), device_id_type=MESH
        )

    partners = [base + d for d in mates] + [ahead, behind]
    for p in partners:
        greet(barrier, p)

    lane = lax.broadcasted_iota(jnp.int32, (half, lanes), 1)
    low = lane < width

    def even(a, c):
        return jnp.where(low, a, pltpu.roll(c, width, 1))

    def odd(a, c):
        return jnp.where(low, pltpu.roll(a, width, 1), c)

    lane_row = lax.broadcasted_iota(jnp.int32, (8, lanes), 1)
    wide_lane = lax.broadcasted_iota(jnp.int32, (size, lanes), 1)
    rim = lax.rem(wide_lane + 1, width) < 2

    def pack_rim(first, second):
        mixed = jnp.where(rim, first, pltpu.roll(second, 2, 1))
        out = jnp.zeros((8, lanes), F32)
        for g in range(size // 8):
            here = lax.rem(lane_row + 1 - 4 * g + lanes, width) < 4
            part = mixed[8 * g : 8 * g + 8]
            out = jnp.where(here, pltpu.roll(part, 4 * g, 1) if g else part, out)
        return out

    loads[0].wait()
    pl.semaphore_wait(barrier, len(partners))
    greet(hello, ahead)
    greet(hello, behind)

    def pack_in(c):
        for t in range(2):
            tile = spec[rows(c), t * lanes : (t + 1) * lanes]
            first, second = tile[0:half], tile[half:size]
            pk[2 * t, halves(c), :] = even(first, second)
            pk[2 * t + 1, halves(c), :] = odd(first, second)
        rx[0, b, halves(c), :] = pk[b, halves(c), :]
        start(piece_out(0, c))

    each(0, 1, pack_in)
    for load in loads[1:]:
        load.wait()
    lraw[...] = jnp.zeros_like(lraw)
    lraw[0:1, 0:levels] = mixing[...]
    lraw[1:2, 0:levels] = sweight[...]
    lcols = jnp.transpose(lraw[...])
    level_mix = lcols[0:levels, 0:1]
    level_weight = lcols[0:levels, 1:2]

    def surface(source, dst, at):
        dst[at : at + 8, :] = jnp.zeros((8, cells), F32)
        for a in range(2):
            dst[at + a : at + a + 1, :] = jnp.sum(level_weight * source[a], axis=0, keepdims=True)

    osm[0:4, :] = oidx[...].astype(F32)
    osm[4:8, :] = owt[...]
    surface(currents, osm, 8)
    orx[b + 1] = osm[...]
    row_start(0)
    mbuf[0:4, :] = pidx[...].astype(F32)
    mbuf[0:1, :] = (2 * pidx[0:1, :] + wet[...]).astype(F32)
    mbuf[4:8, :] = pwt[...]
    meta[b] = mbuf[...]
    start(meta_out())
    each(1, 2, pack_in)

    def rim_in(c):
        ex[0, span(c, 8), :] = pack_rim(spec[rows(c), 0:lanes], spec[rows(c), lanes : 2 * lanes])

    each(0, COMM, rim_in)
    last = width - 1
    from_left = (1, last, lanes - 1, last + 2)
    from_right = (width, 2, width + 2, 0)
    quarter = lax.rem(lane_row, 4)
    ahead_half = lane_row < width
    for d in range(TEAM):
        for v in range(COMM // 4):
            out = jnp.zeros((8, lanes), F32)
            for k in range(4):
                part = ex[0, 8 * (4 * v + k) : 8 * (4 * v + k) + 8, :]
                west = pltpu.roll(part, (k - from_left[d]) % lanes, 1)
                east = pltpu.roll(part, (width + k - from_right[d]) % lanes, 1)
                out = jnp.where(quarter == k, jnp.where(ahead_half, west, east), out)
            ce[d, 8 * v : 8 * v + 8, :] = out
    cein[b] = ce[b]
    start(edges_out())
    each(2, COMM, pack_in)
    pl.semaphore_wait(hello, 2)
    row_start_outer(0)
    start(zonal_out(0))
    araw[...] = jnp.zeros_like(araw)
    araw[0:2, :] = courant[...]
    araw[2:4, :] = (2 * sign[...] - 1).astype(F32)
    araw[4:5, :] = nonlinear[...]
    for j in range(4):
        index, weight = qidx[j], qwt[j]
        twice = index[0:1] == index[1:2]
        araw[8 + 2 * j : 10 + 2 * j, :] = index.astype(F32)
        araw[16 + 2 * j : 17 + 2 * j, :] = jnp.where(twice, weight[0:1] + weight[1:2], weight[0:1])
        araw[17 + 2 * j : 18 + 2 * j, :] = weight[1:2]
    cols[...] = jnp.transpose(araw[...])
    long_lane = lax.broadcasted_iota(jnp.int32, (32, comps), 1).astype(F32)

    def build_quad(c):
        for sub in range(size // 32):
            begin = pl.multiple_of(c * size + sub * 32, 32)
            col = cols[pl.ds(begin, 32), :]
            for j in range(4):
                two = jnp.where(col[:, 9 + 2 * j : 10 + 2 * j] == long_lane, col[:, 17 + 2 * j : 18 + 2 * j], 0.0)
                one = jnp.where(col[:, 8 + 2 * j : 9 + 2 * j] == long_lane, col[:, 16 + 2 * j : 17 + 2 * j], two)
                quad[pl.ds(begin + j * comps, 32), :] = one.astype(BF16)

    def forward(c):
        received(piece_in(0, c))
        start(halo(0, c))

    each(0, COMM // 2, build_quad)
    forward(0)
    each(COMM // 2, COMM - 1, build_quad)
    forward(1)
    each(COMM - 1, COMM, build_quad)
    received(meta_in())
    aside = lax.rem(b, 2)
    for t in range(2):
        pieces = []
        for r in (2 * t, 2 * t + 1):
            tile = meta[r, :, pl.ds(pl.multiple_of(lax.div(b, 2) * lanes, lanes), lanes)]
            pieces.append(jnp.where(aside == r % 2, tile, pltpu.roll(tile, width, 1)))
        bmeta[0:8, t * lanes : (t + 1) * lanes] = jnp.where(low[0:8], pieces[0], pieces[1])

    joined = bmeta[0:1, :]
    halved = jnp.floor(0.5 * joined)
    bmeta[8:9, :] = joined - 2.0 * halved
    bmeta[0:1, :] = halved
    received(row_in(0))
    slots = lax.broadcasted_iota(jnp.int32, (cells, points), 0).astype(F32)
    for q in range(TEAM + 2):
        owner = (wrap(base - 1 + q) * cells).astype(F32)
        value = jnp.zeros((cells, points), F32)
        for j in range(4):
            value = value + jnp.where(bmeta[j : j + 1, :] - owner == slots, bmeta[4 + j : 5 + j, :], 0.0)
        ptab[0, q * cells : (q + 1) * cells, :], ptab[1, q * cells : (q + 1) * cells, :] = split(value)

    shift = lax.rem(cells + window // 2 - window * b, cells)
    pointer = lax.broadcasted_iota(jnp.int32, (width, cells), 0).astype(F32)
    for t in range((TEAM + 2) // 2):
        near = pltpu.roll(orx[2 * t, 0:8], shift, 1)
        far = pltpu.roll(orx[2 * t + 1, 0:8], shift, 1)
        both = jnp.where(low[0:8], near, pltpu.roll(far, width, 1))
        for r in range(TEAM):
            origin = ((base + r) * points + width * b).astype(F32)
            value = jnp.zeros((width, cells), F32)
            for j in range(4):
                value = value + jnp.where(both[j : j + 1, :] - origin == pointer, both[4 + j : 5 + j, :], 0.0)
            high_part, low_part = split(value)
            btab[0, r * width : (r + 1) * width, t * lanes : (t + 1) * lanes] = high_part
            btab[1, r * width : (r + 1) * width, t * lanes : (t + 1) * lanes] = low_part

    forward(2)
    received(edges_in())
    lane_rim = lax.broadcasted_iota(jnp.int32, (8 * COMM, lanes), 1)
    upper = lane_row >= last
    to_left = (last, lanes - 1, last + 2, 1)
    to_right = (0, width, 2, width + 2)
    on_left = (
        (quarter == 3) & upper & (lane_row < lanes - 1),
        (quarter == 3) & ((lane_row < last) | (lane_row == lanes - 1)),
        (quarter == 1) & upper,
        (quarter == 1) & ~upper,
    )
    on_right = ((quarter == 0) & ~upper, (quarter == 0) & upper, (quarter == 2) & ~upper, (quarter == 2) & upper)
    for c in range(COMM):
        v, k = c // 4, c % 4
        out = jnp.zeros((8, lanes), F32)
        for r in range(TEAM):
            part = cein[r, 8 * v : 8 * v + 8, :]
            out = jnp.where(on_left[r], pltpu.roll(part, (to_left[r] - k) % lanes, 1), out)
            out = jnp.where(on_right[r], pltpu.roll(part, (to_right[r] - width - k) % lanes, 1), out)
        edge[0, 8 * c : 8 * c + 8, :] = out

    def flow(step):
        for q in range(TEAM + 2):
            sall[:, q * cells : (q + 1) * cells] = orx[q, 8:16] if step == 0 else srx[q]
        tan[...] = jnp.tanh(dot_split(sall[...], ptab[0], ptab[1]))

    flow(0)

    lane_half = lax.rem(lane, width)
    at_first, at_last = lane_half == 0, lane_half == width - 1

    unit = half
    low_unit = low[0:unit]
    at_first, at_last = at_first[0:unit], at_last[0:unit]

    def advect(step, c, emit):
        received(halo_in(step, c))

        def body(r):
            packed = pl.ds(pl.multiple_of(c * half + r * unit, unit), unit)
            turn = lax.rem(lanes - 4 * (unit // 8) * r, lanes)
            rim_row = pltpu.roll(edge[step, span(c, 8), :], turn, 1)
            out = []
            for sub in range(2):
                at = pl.ds(pl.multiple_of(c * size + sub * half + r * unit, unit), unit)
                col = cols[at, :]
                if step == 0:
                    own = []
                    for t in range(2):
                        a, d = rx[0, 2 * t, packed, :], rx[0, 2 * t + 1, packed, :]
                        if sub:
                            own.append(jnp.where(low_unit, pltpu.roll(a, width, 1), d))
                        else:
                            own.append(jnp.where(low_unit, a, pltpu.roll(d, width, 1)))
                else:
                    own = [mid[at, t * lanes : (t + 1) * lanes] for t in range(2)]
                turned = [pltpu.roll(x, width, 1) for x in own]
                below, above = zin[step, 0, packed, :], zin[step, 1, packed, :]
                if sub:
                    below = pltpu.roll(below, width, 1)
                else:
                    above = pltpu.roll(above, width, 1)
                middle = jnp.where(low_unit, turned[0], turned[1])
                north = (jnp.where(low_unit, below, turned[0]), middle)
                south = (middle, jnp.where(low_unit, turned[1], above))
                groups = range(sub * half // 8, sub * half // 8 + unit // 8)
                spin = [
                    jnp.concatenate([pltpu.roll(rim_row, (k - 4 * g) % lanes, 1) for g in groups], axis=0)
                    for k in (width + 1, width - 1, width - 3)
                ]
                sense_x, sense_y = col[:, 2:3], col[:, 3:4]
                values = []
                for t in range(2):
                    x = own[t]
                    west = jnp.where(at_first, spin[t], pltpu.roll(x, 1, 1))
                    east = jnp.where(at_last, spin[t + 1], pltpu.roll(x, lanes - 1, 1))
                    behind_x = jnp.where(sense_x > 0, west, east)
                    behind_y = jnp.where(sense_y > 0, north[t], south[t])
                    lane_at = slice(t * lanes, (t + 1) * lanes)
                    speed_x = col[:, 0:1] * (1.0 + 0.5 * (sense_x * tan[0:1, lane_at]))
                    speed_y = col[:, 1:2] * (1.0 + 0.5 * (sense_y * tan[1:2, lane_at]))
                    values.append(x - speed_x * (x - behind_x) - speed_y * (x - behind_y))
                out.append(values)
            emit(c, r, out)

        each(0, half // unit, body)

    def keep(c, r, values):
        for sub in range(2):
            at = pl.ds(pl.multiple_of(c * size + sub * half + r * unit, unit), unit)
            for t in range(2):
                adv[at, t * lanes : (t + 1) * lanes] = values[sub][t]
                advb[at, t * lanes : (t + 1) * lanes] = values[sub][t].astype(BF16)

    deep = comps // KPARTS

    def multiply(part):
        k_at = slice(part * deep, (part + 1) * deep)

        def body(i):
            if part:
                acc[...] = acc[...] + dot(quad[:, k_at], advb[k_at, :])
            else:
                acc[...] = dot(quad[:, k_at], advb[k_at, :])

        each(none, none + 1, body)

    def halo_out(c):
        tiles = [mid[rows(c), t * lanes : (t + 1) * lanes] for t in range(2)]
        zpk[0, halves(c), :] = odd(tiles[1][0:half], tiles[1][half:size])
        zpk[1, halves(c), :] = even(tiles[0][0:half], tiles[0][half:size])
        start(halo(1, c))

    def rim_out(c):
        ex[1, span(c, 8), :] = pack_rim(mid[rows(c), 0:lanes], mid[rows(c), lanes : 2 * lanes])

    def source(step, wet_row):
        target = mid if step == 0 else spec_out

        def body(c):
            at = rows(c)
            terms = [acc[pl.ds(pl.multiple_of(j * comps + c * size, size), size), :] for j in range(4)]
            value = adv[at, :]
            total_sum = terms[0] + terms[1] + terms[2] + terms[3]
            pair_sum = terms[0] * terms[1] + terms[2] * terms[3]
            new = wet_row * (value + cols[at, 4:5] * (value * value * total_sum - value * pair_sum))
            target[at, :] = new
            midb[at, :] = new.astype(BF16)

        if step == 0:
            each(0, 1, body)
            each(0, 1, halo_out)
            each(1, COMM, body)
        else:
            each(0, COMM, body)

    level_row = lax.broadcasted_iota(jnp.int32, (levels, cells), 0)

    def mix(w):
        above = jnp.where(level_row == 0, w, pltpu.roll(w, 1, 0))
        below = jnp.where(level_row == levels - 1, w, pltpu.roll(w, levels - 1, 0))
        return level_mix * (above - 2.0 * w + below)

    def ocean(step, drift):
        before = currents if step == 0 else state
        target = state if step == 0 else cur_out
        received(zonal_pair(step))
        u, v = before[0], before[1]
        rot = coriolis[...]
        turn = 0.5 * (pltpu.roll(v, cells - 1, 1) - pltpu.roll(v, 1, 1)) - 0.5 * (zhalo[step, 1] - zhalo[step, 0])
        mix_u, mix_v = mix(u), mix(v)
        drift_x, drift_y = drift()
        target[0] = u + OCEAN_STEP * (rot * (v + drift_y) + turn * drift_y + mix_u)
        target[1] = v + OCEAN_STEP * (-rot * (u + drift_x) - turn * drift_x + mix_v)

    oslots = lax.broadcasted_iota(jnp.int32, (points, cells), 0).astype(F32)
    origin = (pos * points).astype(F32)

    def last_table(q):
        value = jnp.zeros((points, cells), F32)
        for j in range(4):
            value = value + jnp.where(
                orx[b + q, j : j + 1, :] - origin == oslots, orx[b + q, 4 + j : 5 + j, :], 0.0
            )
        otab[q, 0], otab[q, 1] = split(value)
        owner = (wrap(pos - 1 + q) * cells).astype(F32)
        value = jnp.zeros((cells, points), F32)
        for j in range(4):
            value = value + jnp.where(pidx[j : j + 1, :].astype(F32) - owner == slots, pwt[j : j + 1, :], 0.0)
        rtab[0, q * cells : (q + 1) * cells, :], rtab[1, q * cells : (q + 1) * cells, :] = split(value)

    for c in range(3, COMM):
        forward(c)
        advect(0, c - 3, keep)
        if (c - 3) % 2:
            multiply((c - 3) // 2)
    advect(0, COMM - 3, keep)
    multiply(2)
    advect(0, COMM - 2, keep)
    advect(0, COMM - 1, keep)
    multiply(KPARTS - 1)
    source(0, bmeta[8:9, :])

    stokes = dot(table[...], midb[...])
    parts = dot_split(stokes, btab[0], btab[1])
    for t in range((TEAM + 2) // 2):
        zonal = parts[0:levels, t * lanes : (t + 1) * lanes]
        merid = parts[levels : 2 * levels, t * lanes : (t + 1) * lanes]
        dm[2 * t], dm[2 * t + 1] = even(zonal, merid), odd(zonal, merid)
    start(drift_out())
    drx[b] = dm[b + 1]
    def own_out(c):
        for t in range(2):
            tile = mid[rows(c), t * lanes : (t + 1) * lanes]
            first, second = tile[0:half], tile[half:size]
            pk2[2 * t, halves(c), :] = even(first, second)
            pk2[2 * t + 1, halves(c), :] = odd(first, second)
        start(piece_out(1, c))
        rx[1, b, halves(c), :] = pk2[b, halves(c), :]

    each(1, 3, halo_out)
    each(0, EARLY, own_out)
    each(EARLY, COMM, rim_out)
    start(sides_out())
    for q in range(3):
        last_table(q)

    def team_drift():
        inner, outer = drift_in()
        received(inner)

        @pl.when((b == 0) | (b == TEAM - 1))
        def _():
            received(outer)

        drift_x = jnp.zeros((levels, cells), F32)
        drift_y = jnp.zeros((levels, cells), F32)
        for s in range(TEAM):
            part = drx[s] + drx[TEAM + s]
            to = (window * s - window // 2) % cells
            drift_x += pltpu.roll(jnp.where(low, part, 0.0), to, 1)
            drift_y += pltpu.roll(jnp.where(low, pltpu.roll(part, width, 1), 0.0), to, 1)
        return drift_x, drift_y

    ocean(0, team_drift)
    surface(state, sbuf, 0)
    row_start_outer(1)
    row_start(1)
    each(3, 5, halo_out)
    each(5, COMM, halo_out)
    srx[b + 1] = sbuf[...]

    def beside(c):
        received(halo_in(1, c))
        sides_y = []
        for sub in range(2):
            at = pl.ds(pl.multiple_of(c * size + sub * half, half), half)
            turned = [pltpu.roll(mid[at, t * lanes : (t + 1) * lanes], width, 1) for t in range(2)]
            below, above = zin[1, 0, halves(c), :], zin[1, 1, halves(c), :]
            if sub:
                below = pltpu.roll(below, width, 1)
            else:
                above = pltpu.roll(above, width, 1)
            middle = jnp.where(low, turned[0], turned[1])
            north = (jnp.where(low, below, turned[0]), middle)
            south = (middle, jnp.where(low, turned[1], above))
            sense_y = cols[at, 3:4]
            sides_y.append([jnp.where(sense_y > 0, north[t], south[t]) for t in range(2)])
        for t in range(2):
            pkb[2 * t, halves(c), :] = even(sides_y[0][t], sides_y[1][t])
            pkb[2 * t + 1, halves(c), :] = odd(sides_y[0][t], sides_y[1][t])
        start(beside_out(c))
        rxb[b, halves(c), :] = pkb[b, halves(c), :]

    each(0, EARLY, beside)
    received(sides())
    edge[1, later, :] = jnp.where(lax.rem(lane_rim[8 * EARLY :], 2) == 1, exin[0, later, :], exin[1, later, :])
    received(row_in(1))
    flow(1)

    def stack(c, r, values):
        packed = pl.ds(pl.multiple_of(c * half + r * unit, unit), unit)
        for t in range(2):
            first, second = values[0][t], values[1][t]
            pk2[2 * t, packed, :] = jnp.where(low_unit, first, pltpu.roll(second, width, 1))
            pk2[2 * t + 1, packed, :] = jnp.where(low_unit, pltpu.roll(first, width, 1), second)

    def give(c):
        advect(1, c, stack)
        start(piece_out(1, c))
        rx[1, b, halves(c), :] = pk2[b, halves(c), :]

    def take(c):
        received(piece_in(1, c))
        for sub, join in enumerate((even, odd)):
            at = pl.ds(pl.multiple_of(c * size + sub * half, half), half)
            for t in range(2):
                value = join(rx[1, 2 * t, halves(c), :], rx[1, 2 * t + 1, halves(c), :])
                adv[at, t * lanes : (t + 1) * lanes] = value
                advb[at, t * lanes : (t + 1) * lanes] = value.astype(BF16)

    def flow_row():
        own_part = sall[:, pl.ds(pl.multiple_of(b * cells, cells), 3 * cells)]
        tanr[...] = jnp.tanh(dot_split(own_part, rtab[0], rtab[1]))

    def advance(c):
        received(piece_in(1, c))
        received(beside_in(c))
        for sub, join in enumerate((even, odd)):
            at = pl.ds(pl.multiple_of(c * size + sub * half, half), half)
            col = cols[at, :]
            sense_x, sense_y = col[:, 2:3], col[:, 3:4]
            own = [join(rx[1, 2 * t, halves(c), :], rx[1, 2 * t + 1, halves(c), :]) for t in range(2)]
            behind_y = [join(rxb[2 * t, halves(c), :], rxb[2 * t + 1, halves(c), :]) for t in range(2)]
            forth = [pltpu.roll(x, 1, 1) for x in own]
            back = [pltpu.roll(x, lanes - 1, 1) for x in own]
            for t in range(2):
                x = own[t]
                west = jnp.where(lane == 0, forth[1 - t], forth[t])
                east = jnp.where(lane == lanes - 1, back[1 - t], back[t])
                behind_x = jnp.where(sense_x > 0, west, east)
                lane_at = slice(t * lanes, (t + 1) * lanes)
                speed_x = col[:, 0:1] * (1.0 + 0.5 * (sense_x * tanr[0:1, lane_at]))
                speed_y = col[:, 1:2] * (1.0 + 0.5 * (sense_y * tanr[1:2, lane_at]))
                value = x - speed_x * (x - behind_x) - speed_y * (x - behind_y[t])
                adv[at, lane_at] = value
                advb[at, lane_at] = value.astype(BF16)

    each(EARLY, COMM, give)
    flow_row()
    for c in range(COMM):
        if c == COMM - 2:
            start(zonal_out(1))
        advance(c) if c < EARLY else take(c)
        if c % 2:
            multiply(c // 2)
    source(1, wet[...].astype(F32))

    stokes = dot(table[...], midb[...])
    copies = last_out()
    dbuf[0] = dot_split(stokes, otab[2, 0], otab[2, 1])
    copies[0].start()
    dbuf[1] = dot_split(stokes, otab[0, 0], otab[0, 1])
    copies[1].start()
    dself[...] = dot_split(stokes, otab[1, 0], otab[1, 1])

    def last_drift():
        received(last_pair())
        drift = dself[...] + dhalo[0] + dhalo[1]
        return drift[0:levels], drift[levels : 2 * levels]

    ocean(1, last_drift)

    sent(beside_all())
    sent(meta_in())
    sent(edges_in())
    sent(sides())
    sent(drift_all())
    sent(last_pair())
    for step in range(STEPS):
        row_sent(step)
        sent(zonal_pair(step))
        sent(piece_all(step))
        sent(halo_all(step))


def local(
    spectrum, water_mask, courant, stencil_sign, quad_index, quad_weight, nonlinear, stokes_table,
    point_index, point_weight, ocean_index, ocean_weight, currents, coriolis, mixing, surface_weights,
):
    comps, points = spectrum.shape
    levels, cells = currents.shape[1:]
    lanes = points // 2
    packed = comps // 2
    rim = comps // 16
    vm = pl.BlockSpec(memory_space=pltpu.VMEM)
    dma = pltpu.SemaphoreType.DMA

    def f32(*shape):
        return pltpu.VMEM(shape, F32)

    def bf16(*shape):
        return pltpu.VMEM(shape, BF16)

    scratch = [
        f32(128, comps),
        f32(comps, 128),
        f32(128, 128),
        bf16(4 * comps, comps),
        f32(TEAM, packed, lanes),
        f32(TEAM, packed, lanes),
        f32(TEAM, packed * EARLY // COMM, lanes),
        f32(STEPS, TEAM, packed, lanes),
        f32(TEAM, packed * EARLY // COMM, lanes),
        f32(2, packed, lanes),
        f32(STEPS, 2, packed, lanes),
        f32(STEPS, rim, lanes),
        f32(2, rim, lanes),
        f32(TEAM, rim // 4, lanes),
        f32(TEAM, rim // 4, lanes),
        f32(STEPS, rim, lanes),
        f32(comps, points),
        bf16(comps, points),
        f32(4 * comps, points),
        f32(comps, points),
        bf16(comps, points),
        f32(2, levels, cells),
        f32(8, points),
        f32(TEAM, 8, points),
        f32(16, points),
        f32(16, cells),
        f32(TEAM + 2, 16, cells),
        f32(8, cells),
        f32(TEAM + 2, 8, cells),
        f32(8, (TEAM + 2) * cells),
        f32(STEPS, 2, levels, cells),
        bf16(2, (TEAM + 2) * cells, points),
        bf16(2, 3 * cells, points),
        bf16(2, points, (TEAM + 2) // 2 * lanes),
        bf16(3, 2, points, cells),
        f32(TEAM + 2, levels, lanes),
        f32(2 * TEAM, levels, lanes),
        f32(2, 2 * levels, cells),
        f32(2, 2 * levels, cells),
        f32(2 * levels, cells),
        f32(8, points),
        f32(8, points),
        dma((STEPS,)),
        dma((STEPS, COMM)),
        dma((1,)),
        dma((EARLY,)),
        dma((STEPS,)),
        dma((STEPS, COMM)),
        dma((1,)),
        dma((1,)),
        dma((1,)),
        dma((1,)),
        dma((1,)),
        dma((1,)),
        dma((2,)),
        dma((1,)),
        dma((2,)),
        dma((1,)),
        dma((1,)),
        dma((2,)),
        dma((STEPS,)),
        dma((STEPS,)),
        dma((1,)),
        dma((1,)),
        pltpu.SemaphoreType.REGULAR,
    ]
    operands = (
        spectrum,
        water_mask.reshape(1, points),
        courant,
        stencil_sign,
        quad_index.transpose(0, 2, 1),
        quad_weight.transpose(0, 2, 1),
        nonlinear.reshape(1, comps),
        stokes_table,
        point_index,
        point_weight,
        ocean_index,
        ocean_weight,
        currents,
        coriolis.reshape(1, cells),
        mixing.reshape(1, levels),
        surface_weights.reshape(1, levels),
    )
    scratch = [pltpu.VMEM(x.shape, x.dtype) for x in operands] + [dma((INPUTS + 1,))] + scratch
    return pl.pallas_call(
        wave_kernel,
        out_shape=(
            pltpu.VMEM((comps, points), F32),
            pltpu.VMEM(currents.shape, F32),
        ),
        in_specs=[pl.BlockSpec(memory_space=pltpu.HBM)] * INPUTS,
        out_specs=(vm, vm),
        scratch_shapes=scratch,
        compiler_params=pltpu.CompilerParams(
            collective_id=0, has_side_effects=True, vmem_limit_bytes=56 * 1024 * 1024
        ),
    )(*operands)


def solution(mesh):
    ring = P(("mp", "dev"))
    split_last = P(None, ("mp", "dev"))
    deep = P(None, None, ("mp", "dev"))
    return jax.shard_map(
        local,
        mesh=mesh,
        in_specs=(
            split_last, ring, P(), P(), P(), P(), P(), P(), split_last, split_last, split_last, split_last, deep,
            ring, P(), P(),
        ),
        out_specs=(split_last, deep),
        check_vma=False,
    )
```

```python
import jax
import jax.numpy as jnp
from jax import lax
from jax.experimental import pallas as pl
from jax.experimental.pallas import tpu as pltpu
from jax.sharding import PartitionSpec as P

STEPS = 2
OCEAN_STEP = 0.5
TEAM = 4
COMM = 8
EARLY = 2
INPUTS = 16
KPARTS = 4
MESH = pl.DeviceIdType.MESH
F32, BF16 = jnp.float32, jnp.bfloat16


def split(x):
    high = x.astype(BF16)
    return high, (x - high.astype(F32)).astype(BF16)


def dot(a, b):
    return jnp.dot(a, b, preferred_element_type=F32)


def dot_split(x, table_high, table_low):
    rows = x.shape[0]
    high, low = split(x)
    main = dot(jnp.concatenate([high, low], axis=0), table_high)
    return main[0:rows] + (main[rows:] + dot(high, table_low))


def wave_kernel(*refs):
    given, (spec_out, cur_out), scratch = refs[:INPUTS], refs[INPUTS : INPUTS + 2], refs[INPUTS + 2 :]
    copied, load_sems, rest = scratch[:INPUTS], scratch[INPUTS], scratch[INPUTS + 1 :]
    head = given[0].shape[0] // COMM
    pairs = [(given[0].at[0:head], copied[0].at[0:head])] + list(zip(given[1:], copied[1:]))
    pairs.append((given[0].at[head:], copied[0].at[head:]))
    loads = [pltpu.make_async_copy(a, c, load_sems.at[i]) for i, (a, c) in enumerate(pairs)]
    wave_body(loads, *copied, spec_out, cur_out, *rest)


def wave_body(
    loads,
    spec, wet, courant, sign, qidx, qwt, nonlinear, table, pidx, pwt, oidx, owt,
    currents, coriolis, mixing, sweight,
    spec_out, cur_out,
    araw, cols, lraw, quad, pk, pk2, pkb, rx, rxb, zpk, zin, ex, exin, ce, cein, edge, adv, advb, acc, mid, midb, state,
    mbuf, meta, bmeta, osm, orx, sbuf, srx, sall, zhalo, ptab, rtab, btab, otab, dm, drx, dbuf, dhalo, dself, tan, tanr,
    rxs, rxr, bs, br, zs, zr, es, er, fs, fr, ms, mr, os_, or_, ss, sr, ds_, dr, us, ur, hs, hr, hello,
):
    comps, points = spec.shape
    cells = coriolis.shape[1]
    levels = mixing.shape[1]
    dev_count = lax.axis_size("dev")
    total = lax.axis_size("mp") * dev_count
    pos = lax.axis_index("mp") * dev_count + lax.axis_index("dev")
    b = lax.rem(pos, TEAM)
    base = pos - b
    width = points // TEAM
    window = cells // TEAM
    size = comps // COMM
    half = size // 2
    lanes = 2 * width

    none = lax.div(pos, total)

    def wrap(p):
        return lax.rem(p + total, total)

    up, down = wrap(pos + 1), wrap(pos - 1)
    ahead, behind = wrap(pos + TEAM), wrap(pos - TEAM)
    mates = [lax.rem(b + i, TEAM) for i in range(1, TEAM)]

    def remote(src, dst, ssem, rsem, p):
        return pltpu.make_async_remote_copy(
            src_ref=src, dst_ref=dst, send_sem=ssem, recv_sem=rsem,
            device_id=(lax.div(p, dev_count), lax.rem(p, dev_count)), device_id_type=MESH,
        )

    def span(c, n):
        return pl.ds(pl.multiple_of(c * n, n), n)

    def rows(c):
        return span(c, size)

    def halves(c):
        return span(c, half)

    def each(low, high, body):
        def run(c, carry):
            body(c)
            return carry

        lax.fori_loop(low, high, run, 0)

    def start(copies):
        for copy in copies:
            copy.start()

    def received(copies):
        for copy in copies:
            copy.wait_recv()

    def sent(copies):
        for copy in copies:
            copy.wait_send()

    def spread(src, dst, ssem, rsem):
        return [remote(src.at[d], dst, ssem, rsem, base + d) for d in mates]

    def gather(src, dst, ssem, rsem, count):
        return [remote(src.at[0:count], dst.at[0:count], ssem, rsem, base + mates[0])]

    def piece(step, c):
        return (pk if step == 0 else pk2).at[:, halves(c)], rx.at[step, :, halves(c)]

    def piece_out(step, c):
        src, dst = piece(step, c)
        return spread(src, dst.at[b], rxs.at[step], rxr.at[step, c])

    def piece_in(step, c):
        src, dst = piece(step, c)
        return gather(src, dst, rxs.at[step], rxr.at[step, c], TEAM - 1)

    def piece_all(step):
        return gather(pk if step == 0 else pk2, rx.at[step], rxs.at[step], rxr.at[step, 0], TEAM - 1)

    def halo(step, c):
        from_low = rx.at[0, TEAM - 1, halves(c)] if step == 0 else zpk.at[0, halves(c)]
        from_high = rx.at[0, 0, halves(c)] if step == 0 else zpk.at[1, halves(c)]
        return [
            remote(from_low, zin.at[step, 0, halves(c)], zs.at[step], zr.at[step, c], ahead),
            remote(from_high, zin.at[step, 1, halves(c)], zs.at[step], zr.at[step, c], behind),
        ]

    def halo_in(step, c):
        return [remote(zpk.at[:, halves(c)], zin.at[step, :, halves(c)], zs.at[step], zr.at[step, c], ahead)]

    def halo_all(step):
        return [remote(zpk, zin.at[step], zs.at[step], zr.at[step, 0], ahead)]

    def beside_out(c):
        return spread(pkb.at[:, halves(c)], rxb.at[b, halves(c)], bs.at[0], br.at[c])

    def beside_in(c):
        return gather(pkb.at[:, halves(c)], rxb.at[:, halves(c)], bs.at[0], br.at[c], TEAM - 1)

    def beside_all():
        return gather(pkb, rxb, bs.at[0], br.at[0], TEAM - 1)

    def edges_out():
        return spread(ce, cein.at[b], es.at[0], er.at[0])

    def edges_in():
        return gather(ce, cein, es.at[0], er.at[0], TEAM - 1)

    right, left = base + mates[0], base + mates[2]

    later = pl.ds(8 * EARLY, 8 * (COMM - EARLY))

    def sides_out():
        return [
            remote(ex.at[1, later], exin.at[0, later], fs.at[0], fr.at[0], right),
            remote(ex.at[1, later], exin.at[1, later], fs.at[0], fr.at[0], left),
        ]

    def sides():
        return [remote(ex.at[:, later], exin.at[:, later], fs.at[0], fr.at[0], right)]

    def meta_out():
        return [remote(mbuf, meta.at[b], ms.at[0], mr.at[0], base + d) for d in mates]

    def meta_in():
        return gather(meta, meta, ms.at[0], mr.at[0], TEAM - 1)

    def row_refs(step):
        return (osm, orx, os_, or_) if step == 0 else (sbuf, srx, ss, sr)

    def row_out(step):
        src, dst, ssem, rsem = row_refs(step)
        inner = [remote(src, dst.at[b + 1], ssem.at[0], rsem.at[0], base + d) for d in mates]
        before = [
            remote(src, dst.at[TEAM + 1], ssem.at[1], rsem.at[0], wrap(base - TEAM + k)) for k in range(TEAM)
        ]
        after = [remote(src, dst.at[0], ssem.at[1], rsem.at[0], wrap(base + TEAM + k)) for k in range(TEAM)]
        return inner, before, after

    def row_start(step):
        start(row_out(step)[0])

    def row_start_outer(step):
        inner, before, after = row_out(step)

        @pl.when(b == 0)
        def _():
            start(before)

        @pl.when(b == TEAM - 1)
        def _():
            start(after)

    def row_sent(step):
        src, dst, ssem, rsem = row_refs(step)
        sent(gather(dst, dst, ssem.at[0], rsem.at[0], TEAM - 1))

        @pl.when((b == 0) | (b == TEAM - 1))
        def _():
            sent(gather(dst, dst, ssem.at[1], rsem.at[0], TEAM))

    def row_in(step):
        src, dst, ssem, rsem = row_refs(step)
        return gather(dst, dst, ssem.at[0], rsem.at[0], TEAM + 1)

    def drift_out():
        copies = [
            remote(dm.at[0], drx.at[TEAM + b], ds_.at[0], dr.at[1], wrap(base - 1)),
            remote(dm.at[TEAM + 1], drx.at[TEAM + b], ds_.at[0], dr.at[1], wrap(base + TEAM)),
        ]
        return [remote(dm.at[d + 1], drx.at[b], ds_.at[0], dr.at[0], base + d) for d in mates] + copies

    def drift_all():
        return gather(dm, drx, ds_.at[0], dr.at[0], TEAM + 1)

    def drift_in():
        return gather(dm, drx, ds_.at[0], dr.at[0], TEAM - 1), gather(dm, drx, ds_.at[0], dr.at[1], TEAM)

    def zonal_out(step):
        src = currents.at[0] if step == 0 else state.at[0]
        return [
            remote(src, zhalo.at[step, 0], us.at[step], ur.at[step], up),
            remote(src, zhalo.at[step, 1], us.at[step], ur.at[step], down),
        ]

    def zonal_pair(step):
        return [remote(currents, zhalo.at[step], us.at[step], ur.at[step], up)]

    def last_out():
        return [
            remote(dbuf.at[0], dhalo.at[0], hs.at[0], hr.at[0], up),
            remote(dbuf.at[1], dhalo.at[1], hs.at[0], hr.at[0], down),
        ]

    def last_pair():
        return [remote(dbuf, dhalo, hs.at[0], hr.at[0], up)]

    start(loads)
    drx[TEAM : 2 * TEAM] = jnp.zeros((TEAM,) + drx.shape[1:], F32)
    barrier = pltpu.get_barrier_semaphore()

    def greet(sem, p):
        pl.semaphore_signal(
            sem, inc=1, device_id=(lax.div(p, dev_count), lax.rem(p, dev_count)), device_id_type=MESH
        )

    partners = [base + d for d in mates] + [ahead, behind]
    for p in partners:
        greet(barrier, p)

    lane = lax.broadcasted_iota(jnp.int32, (half, lanes), 1)
    low = lane < width

    def even(a, c):
        return jnp.where(low, a, pltpu.roll(c, width, 1))

    def odd(a, c):
        return jnp.where(low, pltpu.roll(a, width, 1), c)

    lane_row = lax.broadcasted_iota(jnp.int32, (8, lanes), 1)
    fold = drx.shape[1]
    third = lanes // 3
    margin = (third - window - 2) // 2
    lane_fold = lane[0:fold]
    in_first, in_second, in_third = lane_fold < third, lane_fold < 2 * third, lane_fold < 3 * third
    wide_lane = lax.broadcasted_iota(jnp.int32, (size, lanes), 1)
    rim = lax.rem(wide_lane + 1, width) < 2

    def pack_rim(first, second):
        mixed = jnp.where(rim, first, pltpu.roll(second, 2, 1))
        out = jnp.zeros((8, lanes), F32)
        for g in range(size // 8):
            here = lax.rem(lane_row + 1 - 4 * g + lanes, width) < 4
            part = mixed[8 * g : 8 * g + 8]
            out = jnp.where(here, pltpu.roll(part, 4 * g, 1) if g else part, out)
        return out

    loads[0].wait()
    pl.semaphore_wait(barrier, len(partners))
    greet(hello, ahead)
    greet(hello, behind)

    def pack_in(c):
        for t in range(2):
            tile = spec[rows(c), t * lanes : (t + 1) * lanes]
            first, second = tile[0:half], tile[half:size]
            pk[2 * t, halves(c), :] = even(first, second)
            pk[2 * t + 1, halves(c), :] = odd(first, second)
        rx[0, b, halves(c), :] = pk[b, halves(c), :]
        start(piece_out(0, c))

    each(0, 1, pack_in)
    for load in loads[1:]:
        load.wait()
    lraw[...] = jnp.zeros_like(lraw)
    lraw[0:1, 0:levels] = mixing[...]
    lraw[1:2, 0:levels] = sweight[...]
    lcols = jnp.transpose(lraw[...])
    level_mix = lcols[0:levels, 0:1]
    level_weight = lcols[0:levels, 1:2]

    def surface(source, dst, at):
        dst[at : at + 8, :] = jnp.zeros((8, cells), F32)
        for a in range(2):
            dst[at + a : at + a + 1, :] = jnp.sum(level_weight * source[a], axis=0, keepdims=True)

    osm[0:4, :] = oidx[...].astype(F32)
    osm[4:8, :] = owt[...]
    surface(currents, osm, 8)
    orx[b + 1] = osm[...]
    row_start(0)
    mbuf[0:4, :] = pidx[...].astype(F32)
    mbuf[0:1, :] = (2 * pidx[0:1, :] + wet[...]).astype(F32)
    mbuf[4:8, :] = pwt[...]
    meta[b] = mbuf[...]
    start(meta_out())
    each(1, 2, pack_in)

    def rim_in(c):
        ex[0, span(c, 8), :] = pack_rim(spec[rows(c), 0:lanes], spec[rows(c), lanes : 2 * lanes])

    each(0, COMM, rim_in)
    last = width - 1
    from_left = (1, last, lanes - 1, last + 2)
    from_right = (width, 2, width + 2, 0)
    quarter = lax.rem(lane_row, 4)
    ahead_half = lane_row < width
    for d in range(TEAM):
        for v in range(COMM // 4):
            out = jnp.zeros((8, lanes), F32)
            for k in range(4):
                part = ex[0, 8 * (4 * v + k) : 8 * (4 * v + k) + 8, :]
                west = pltpu.roll(part, (k - from_left[d]) % lanes, 1)
                east = pltpu.roll(part, (width + k - from_right[d]) % lanes, 1)
                out = jnp.where(quarter == k, jnp.where(ahead_half, west, east), out)
            ce[d, 8 * v : 8 * v + 8, :] = out
    cein[b] = ce[b]
    start(edges_out())
    each(2, COMM, pack_in)
    pl.semaphore_wait(hello, 2)
    row_start_outer(0)
    start(zonal_out(0))
    araw[...] = jnp.zeros_like(araw)
    araw[0:2, :] = courant[...]
    araw[2:4, :] = (2 * sign[...] - 1).astype(F32)
    araw[4:5, :] = nonlinear[...]
    for j in range(4):
        index, weight = qidx[j], qwt[j]
        twice = index[0:1] == index[1:2]
        araw[8 + 2 * j : 10 + 2 * j, :] = index.astype(F32)
        araw[16 + 2 * j : 17 + 2 * j, :] = jnp.where(twice, weight[0:1] + weight[1:2], weight[0:1])
        araw[17 + 2 * j : 18 + 2 * j, :] = weight[1:2]
    cols[...] = jnp.transpose(araw[...])
    long_lane = lax.broadcasted_iota(jnp.int32, (32, comps), 1).astype(F32)

    def build_quad(c):
        for sub in range(size // 32):
            begin = pl.multiple_of(c * size + sub * 32, 32)
            col = cols[pl.ds(begin, 32), :]
            for j in range(4):
                two = jnp.where(col[:, 9 + 2 * j : 10 + 2 * j] == long_lane, col[:, 17 + 2 * j : 18 + 2 * j], 0.0)
                one = jnp.where(col[:, 8 + 2 * j : 9 + 2 * j] == long_lane, col[:, 16 + 2 * j : 17 + 2 * j], two)
                quad[pl.ds(begin + j * comps, 32), :] = one.astype(BF16)

    def forward(c):
        received(piece_in(0, c))
        start(halo(0, c))

    each(0, COMM // 2, build_quad)
    forward(0)
    each(COMM // 2, COMM - 1, build_quad)
    forward(1)
    each(COMM - 1, COMM, build_quad)
    received(meta_in())
    aside = lax.rem(b, 2)
    for t in range(2):
        pieces = []
        for r in (2 * t, 2 * t + 1):
            tile = meta[r, :, pl.ds(pl.multiple_of(lax.div(b, 2) * lanes, lanes), lanes)]
            pieces.append(jnp.where(aside == r % 2, tile, pltpu.roll(tile, width, 1)))
        bmeta[0:8, t * lanes : (t + 1) * lanes] = jnp.where(low[0:8], pieces[0], pieces[1])

    joined = bmeta[0:1, :]
    halved = jnp.floor(0.5 * joined)
    bmeta[8:9, :] = joined - 2.0 * halved
    bmeta[0:1, :] = halved
    received(row_in(0))
    slots = lax.broadcasted_iota(jnp.int32, (cells, points), 0).astype(F32)
    for q in range(TEAM + 2):
        owner = (wrap(base - 1 + q) * cells).astype(F32)
        value = jnp.zeros((cells, points), F32)
        for j in range(4):
            value = value + jnp.where(bmeta[j : j + 1, :] - owner == slots, bmeta[4 + j : 5 + j, :], 0.0)
        ptab[0, q * cells : (q + 1) * cells, :], ptab[1, q * cells : (q + 1) * cells, :] = split(value)

    shift = lax.rem(cells + margin - window * b, cells)
    pointer = lax.broadcasted_iota(jnp.int32, (width, cells), 0).astype(F32)
    for t in range((TEAM + 2) // 2):
        near = pltpu.roll(orx[2 * t, 0:8], shift, 1)
        far = pltpu.roll(orx[2 * t + 1, 0:8], shift, 1)
        both = jnp.where(low[0:8], near, pltpu.roll(far, width, 1))
        for r in range(TEAM):
            origin = ((base + r) * points + width * b).astype(F32)
            value = jnp.zeros((width, cells), F32)
            for j in range(4):
                value = value + jnp.where(both[j : j + 1, :] - origin == pointer, both[4 + j : 5 + j, :], 0.0)
            high_part, low_part = split(value)
            btab[0, r * width : (r + 1) * width, t * lanes : (t + 1) * lanes] = high_part
            btab[1, r * width : (r + 1) * width, t * lanes : (t + 1) * lanes] = low_part

    forward(2)
    received(edges_in())
    lane_rim = lax.broadcasted_iota(jnp.int32, (8 * COMM, lanes), 1)
    upper = lane_row >= last
    to_left = (last, lanes - 1, last + 2, 1)
    to_right = (0, width, 2, width + 2)
    on_left = (
        (quarter == 3) & upper & (lane_row < lanes - 1),
        (quarter == 3) & ((lane_row < last) | (lane_row == lanes - 1)),
        (quarter == 1) & upper,
        (quarter == 1) & ~upper,
    )
    on_right = ((quarter == 0) & ~upper, (quarter == 0) & upper, (quarter == 2) & ~upper, (quarter == 2) & upper)
    for c in range(COMM):
        v, k = c // 4, c % 4
        out = jnp.zeros((8, lanes), F32)
        for r in range(TEAM):
            part = cein[r, 8 * v : 8 * v + 8, :]
            out = jnp.where(on_left[r], pltpu.roll(part, (to_left[r] - k) % lanes, 1), out)
            out = jnp.where(on_right[r], pltpu.roll(part, (to_right[r] - width - k) % lanes, 1), out)
        edge[0, 8 * c : 8 * c + 8, :] = out

    def flow(step):
        for q in range(TEAM + 2):
            sall[:, q * cells : (q + 1) * cells] = orx[q, 8:16] if step == 0 else srx[q]
        tan[...] = jnp.tanh(dot_split(sall[...], ptab[0], ptab[1]))

    flow(0)

    lane_half = lax.rem(lane, width)
    at_first, at_last = lane_half == 0, lane_half == width - 1

    unit = half
    low_unit = low[0:unit]
    at_first, at_last = at_first[0:unit], at_last[0:unit]

    def advect(step, c, emit):
        received(halo_in(step, c))

        def body(r):
            packed = pl.ds(pl.multiple_of(c * half + r * unit, unit), unit)
            turn = lax.rem(lanes - 4 * (unit // 8) * r, lanes)
            rim_row = pltpu.roll(edge[step, span(c, 8), :], turn, 1)
            out = []
            for sub in range(2):
                at = pl.ds(pl.multiple_of(c * size + sub * half + r * unit, unit), unit)
                col = cols[at, :]
                if step == 0:
                    own = []
                    for t in range(2):
                        a, d = rx[0, 2 * t, packed, :], rx[0, 2 * t + 1, packed, :]
                        if sub:
                            own.append(jnp.where(low_unit, pltpu.roll(a, width, 1), d))
                        else:
                            own.append(jnp.where(low_unit, a, pltpu.roll(d, width, 1)))
                else:
                    own = [mid[at, t * lanes : (t + 1) * lanes] for t in range(2)]
                turned = [pltpu.roll(x, width, 1) for x in own]
                below, above = zin[step, 0, packed, :], zin[step, 1, packed, :]
                if sub:
                    below = pltpu.roll(below, width, 1)
                else:
                    above = pltpu.roll(above, width, 1)
                middle = jnp.where(low_unit, turned[0], turned[1])
                north = (jnp.where(low_unit, below, turned[0]), middle)
                south = (middle, jnp.where(low_unit, turned[1], above))
                groups = range(sub * half // 8, sub * half // 8 + unit // 8)
                spin = [
                    jnp.concatenate([pltpu.roll(rim_row, (k - 4 * g) % lanes, 1) for g in groups], axis=0)
                    for k in (width + 1, width - 1, width - 3)
                ]
                sense_x, sense_y = col[:, 2:3], col[:, 3:4]
                values = []
                for t in range(2):
                    x = own[t]
                    west = jnp.where(at_first, spin[t], pltpu.roll(x, 1, 1))
                    east = jnp.where(at_last, spin[t + 1], pltpu.roll(x, lanes - 1, 1))
                    behind_x = jnp.where(sense_x > 0, west, east)
                    behind_y = jnp.where(sense_y > 0, north[t], south[t])
                    lane_at = slice(t * lanes, (t + 1) * lanes)
                    speed_x = col[:, 0:1] * (1.0 + 0.5 * (sense_x * tan[0:1, lane_at]))
                    speed_y = col[:, 1:2] * (1.0 + 0.5 * (sense_y * tan[1:2, lane_at]))
                    values.append(x - speed_x * (x - behind_x) - speed_y * (x - behind_y))
                out.append(values)
            emit(c, r, out)

        each(0, half // unit, body)

    def keep(c, r, values):
        for sub in range(2):
            at = pl.ds(pl.multiple_of(c * size + sub * half + r * unit, unit), unit)
            for t in range(2):
                adv[at, t * lanes : (t + 1) * lanes] = values[sub][t]
                advb[at, t * lanes : (t + 1) * lanes] = values[sub][t].astype(BF16)

    deep = comps // KPARTS

    def multiply(part):
        k_at = slice(part * deep, (part + 1) * deep)

        def body(i):
            if part:
                acc[...] = acc[...] + dot(quad[:, k_at], advb[k_at, :])
            else:
                acc[...] = dot(quad[:, k_at], advb[k_at, :])

        each(none, none + 1, body)

    def halo_out(c):
        tiles = [mid[rows(c), t * lanes : (t + 1) * lanes] for t in range(2)]
        zpk[0, halves(c), :] = odd(tiles[1][0:half], tiles[1][half:size])
        zpk[1, halves(c), :] = even(tiles[0][0:half], tiles[0][half:size])
        start(halo(1, c))

    def rim_out(c):
        ex[1, span(c, 8), :] = pack_rim(mid[rows(c), 0:lanes], mid[rows(c), lanes : 2 * lanes])

    def source(step, wet_row):
        target = mid if step == 0 else spec_out

        def body(c):
            at = rows(c)
            terms = [acc[pl.ds(pl.multiple_of(j * comps + c * size, size), size), :] for j in range(4)]
            value = adv[at, :]
            total_sum = terms[0] + terms[1] + terms[2] + terms[3]
            pair_sum = terms[0] * terms[1] + terms[2] * terms[3]
            new = wet_row * (value + cols[at, 4:5] * (value * value * total_sum - value * pair_sum))
            target[at, :] = new
            midb[at, :] = new.astype(BF16)

        if step == 0:
            each(0, 1, body)
            each(0, 1, halo_out)
            each(1, COMM, body)
        else:
            each(0, COMM, body)

    level_row = lax.broadcasted_iota(jnp.int32, (levels, cells), 0)

    def mix(w):
        above = jnp.where(level_row == 0, w, pltpu.roll(w, 1, 0))
        below = jnp.where(level_row == levels - 1, w, pltpu.roll(w, levels - 1, 0))
        return level_mix * (above - 2.0 * w + below)

    def ocean(step, drift):
        before = currents if step == 0 else state
        target = state if step == 0 else cur_out
        received(zonal_pair(step))
        u, v = before[0], before[1]
        rot = coriolis[...]
        turn = 0.5 * (pltpu.roll(v, cells - 1, 1) - pltpu.roll(v, 1, 1)) - 0.5 * (zhalo[step, 1] - zhalo[step, 0])
        mix_u, mix_v = mix(u), mix(v)
        drift_x, drift_y = drift()
        target[0] = u + OCEAN_STEP * (rot * (v + drift_y) + turn * drift_y + mix_u)
        target[1] = v + OCEAN_STEP * (-rot * (u + drift_x) - turn * drift_x + mix_v)

    oslots = lax.broadcasted_iota(jnp.int32, (points, cells), 0).astype(F32)
    origin = (pos * points).astype(F32)

    def last_table(q):
        value = jnp.zeros((points, cells), F32)
        for j in range(4):
            value = value + jnp.where(
                orx[b + q, j : j + 1, :] - origin == oslots, orx[b + q, 4 + j : 5 + j, :], 0.0
            )
        otab[q, 0], otab[q, 1] = split(value)
        owner = (wrap(pos - 1 + q) * cells).astype(F32)
        value = jnp.zeros((cells, points), F32)
        for j in range(4):
            value = value + jnp.where(pidx[j : j + 1, :].astype(F32) - owner == slots, pwt[j : j + 1, :], 0.0)
        rtab[0, q * cells : (q + 1) * cells, :], rtab[1, q * cells : (q + 1) * cells, :] = split(value)

    for c in range(3, COMM):
        forward(c)
        advect(0, c - 3, keep)
        if (c - 3) % 2:
            multiply((c - 3) // 2)
    advect(0, COMM - 3, keep)
    multiply(2)
    advect(0, COMM - 2, keep)
    advect(0, COMM - 1, keep)
    multiply(KPARTS - 1)
    source(0, bmeta[8:9, :])

    stokes = dot(table[...], midb[...])
    parts = dot_split(stokes, btab[0], btab[1])
    for t in range((TEAM + 2) // 2):
        tile = parts[:, t * lanes : (t + 1) * lanes]
        rest = jnp.concatenate([tile[2 * fold :], jnp.zeros((3 * fold - 2 * levels, lanes), F32)], axis=0)
        for k in range(2):
            first, second, last_rows = (
                pltpu.roll(x, (i * third - k * width) % lanes, 1) if i or k else x
                for i, x in enumerate((tile[0:fold], tile[fold : 2 * fold], rest))
            )
            dm[2 * t + k] = jnp.where(in_first, first, jnp.where(in_second, second, last_rows))
    start(drift_out())
    drx[b] = dm[b + 1]
    def own_out(c):
        for t in range(2):
            tile = mid[rows(c), t * lanes : (t + 1) * lanes]
            first, second = tile[0:half], tile[half:size]
            pk2[2 * t, halves(c), :] = even(first, second)
            pk2[2 * t + 1, halves(c), :] = odd(first, second)
        start(piece_out(1, c))
        rx[1, b, halves(c), :] = pk2[b, halves(c), :]

    each(1, 3, halo_out)
    each(0, EARLY, own_out)
    each(EARLY, COMM, rim_out)
    start(sides_out())
    for q in range(3):
        last_table(q)

    def team_drift():
        inner, outer = drift_in()
        received(inner)

        @pl.when((b == 0) | (b == TEAM - 1))
        def _():
            received(outer)

        sums = [jnp.zeros((fold, cells), F32)] * 3
        for s in range(TEAM):
            part = drx[s] + drx[TEAM + s]
            picks = (
                jnp.where(in_first, part, 0.0),
                jnp.where(in_second & ~in_first, part, 0.0),
                jnp.where(in_third & ~in_second, part, 0.0),
            )
            sums = [
                total_part + pltpu.roll(x, (window * s - margin - i * third) % cells, 1)
                for i, (total_part, x) in enumerate(zip(sums, picks))
            ]
        drift = jnp.concatenate([sums[0], sums[1], sums[2][0 : 2 * levels - 2 * fold]], axis=0)
        return drift[0:levels], drift[levels : 2 * levels]

    ocean(0, team_drift)
    surface(state, sbuf, 0)
    row_start_outer(1)
    row_start(1)
    each(3, 5, halo_out)
    each(5, COMM, halo_out)
    srx[b + 1] = sbuf[...]

    def beside(c):
        received(halo_in(1, c))
        sides_y = []
        for sub in range(2):
            at = pl.ds(pl.multiple_of(c * size + sub * half, half), half)
            turned = [pltpu.roll(mid[at, t * lanes : (t + 1) * lanes], width, 1) for t in range(2)]
            below, above = zin[1, 0, halves(c), :], zin[1, 1, halves(c), :]
            if sub:
                below = pltpu.roll(below, width, 1)
            else:
                above = pltpu.roll(above, width, 1)
            middle = jnp.where(low, turned[0], turned[1])
            north = (jnp.where(low, below, turned[0]), middle)
            south = (middle, jnp.where(low, turned[1], above))
            sense_y = cols[at, 3:4]
            sides_y.append([jnp.where(sense_y > 0, north[t], south[t]) for t in range(2)])
        for t in range(2):
            pkb[2 * t, halves(c), :] = even(sides_y[0][t], sides_y[1][t])
            pkb[2 * t + 1, halves(c), :] = odd(sides_y[0][t], sides_y[1][t])
        start(beside_out(c))
        rxb[b, halves(c), :] = pkb[b, halves(c), :]

    each(0, EARLY, beside)
    received(sides())
    edge[1, later, :] = jnp.where(lax.rem(lane_rim[8 * EARLY :], 2) == 1, exin[0, later, :], exin[1, later, :])
    received(row_in(1))
    flow(1)

    def stack(c, r, values):
        packed = pl.ds(pl.multiple_of(c * half + r * unit, unit), unit)
        for t in range(2):
            first, second = values[0][t], values[1][t]
            pk2[2 * t, packed, :] = jnp.where(low_unit, first, pltpu.roll(second, width, 1))
            pk2[2 * t + 1, packed, :] = jnp.where(low_unit, pltpu.roll(first, width, 1), second)

    def give(c):
        advect(1, c, stack)
        start(piece_out(1, c))
        rx[1, b, halves(c), :] = pk2[b, halves(c), :]

    def take(c):
        received(piece_in(1, c))
        for sub, join in enumerate((even, odd)):
            at = pl.ds(pl.multiple_of(c * size + sub * half, half), half)
            for t in range(2):
                value = join(rx[1, 2 * t, halves(c), :], rx[1, 2 * t + 1, halves(c), :])
                adv[at, t * lanes : (t + 1) * lanes] = value
                advb[at, t * lanes : (t + 1) * lanes] = value.astype(BF16)

    def flow_row():
        own_part = sall[:, pl.ds(pl.multiple_of(b * cells, cells), 3 * cells)]
        tanr[...] = jnp.tanh(dot_split(own_part, rtab[0], rtab[1]))

    def advance(c):
        received(piece_in(1, c))
        received(beside_in(c))
        for sub, join in enumerate((even, odd)):
            at = pl.ds(pl.multiple_of(c * size + sub * half, half), half)
            col = cols[at, :]
            sense_x, sense_y = col[:, 2:3], col[:, 3:4]
            own = [join(rx[1, 2 * t, halves(c), :], rx[1, 2 * t + 1, halves(c), :]) for t in range(2)]
            behind_y = [join(rxb[2 * t, halves(c), :], rxb[2 * t + 1, halves(c), :]) for t in range(2)]
            forth = [pltpu.roll(x, 1, 1) for x in own]
            back = [pltpu.roll(x, lanes - 1, 1) for x in own]
            for t in range(2):
                x = own[t]
                west = jnp.where(lane == 0, forth[1 - t], forth[t])
                east = jnp.where(lane == lanes - 1, back[1 - t], back[t])
                behind_x = jnp.where(sense_x > 0, west, east)
                lane_at = slice(t * lanes, (t + 1) * lanes)
                speed_x = col[:, 0:1] * (1.0 + 0.5 * (sense_x * tanr[0:1, lane_at]))
                speed_y = col[:, 1:2] * (1.0 + 0.5 * (sense_y * tanr[1:2, lane_at]))
                value = x - speed_x * (x - behind_x) - speed_y * (x - behind_y[t])
                adv[at, lane_at] = value
                advb[at, lane_at] = value.astype(BF16)

    each(EARLY, COMM, give)
    flow_row()
    for c in range(COMM):
        if c == COMM - 2:
            start(zonal_out(1))
        advance(c) if c < EARLY else take(c)
        if c % 2:
            multiply(c // 2)
    source(1, wet[...].astype(F32))

    stokes = dot(table[...], midb[...])
    copies = last_out()
    dbuf[0] = dot_split(stokes, otab[2, 0], otab[2, 1])
    copies[0].start()
    dbuf[1] = dot_split(stokes, otab[0, 0], otab[0, 1])
    copies[1].start()
    dself[...] = dot_split(stokes, otab[1, 0], otab[1, 1])

    def last_drift():
        received(last_pair())
        drift = dself[...] + dhalo[0] + dhalo[1]
        return drift[0:levels], drift[levels : 2 * levels]

    ocean(1, last_drift)

    sent(beside_all())
    sent(meta_in())
    sent(edges_in())
    sent(sides())
    sent(drift_all())
    sent(last_pair())
    for step in range(STEPS):
        row_sent(step)
        sent(zonal_pair(step))
        sent(piece_all(step))
        sent(halo_all(step))


def local(
    spectrum, water_mask, courant, stencil_sign, quad_index, quad_weight, nonlinear, stokes_table,
    point_index, point_weight, ocean_index, ocean_weight, currents, coriolis, mixing, surface_weights,
):
    comps, points = spectrum.shape
    levels, cells = currents.shape[1:]
    lanes = points // 2
    packed = comps // 2
    rim = comps // 16
    fold = -(-2 * levels // 24) * 8
    vm = pl.BlockSpec(memory_space=pltpu.VMEM)
    dma = pltpu.SemaphoreType.DMA

    def f32(*shape):
        return pltpu.VMEM(shape, F32)

    def bf16(*shape):
        return pltpu.VMEM(shape, BF16)

    scratch = [
        f32(128, comps),
        f32(comps, 128),
        f32(128, 128),
        bf16(4 * comps, comps),
        f32(TEAM, packed, lanes),
        f32(TEAM, packed, lanes),
        f32(TEAM, packed * EARLY // COMM, lanes),
        f32(STEPS, TEAM, packed, lanes),
        f32(TEAM, packed * EARLY // COMM, lanes),
        f32(2, packed, lanes),
        f32(STEPS, 2, packed, lanes),
        f32(STEPS, rim, lanes),
        f32(2, rim, lanes),
        f32(TEAM, rim // 4, lanes),
        f32(TEAM, rim // 4, lanes),
        f32(STEPS, rim, lanes),
        f32(comps, points),
        bf16(comps, points),
        f32(4 * comps, points),
        f32(comps, points),
        bf16(comps, points),
        f32(2, levels, cells),
        f32(8, points),
        f32(TEAM, 8, points),
        f32(16, points),
        f32(16, cells),
        f32(TEAM + 2, 16, cells),
        f32(8, cells),
        f32(TEAM + 2, 8, cells),
        f32(8, (TEAM + 2) * cells),
        f32(STEPS, 2, levels, cells),
        bf16(2, (TEAM + 2) * cells, points),
        bf16(2, 3 * cells, points),
        bf16(2, points, (TEAM + 2) // 2 * lanes),
        bf16(3, 2, points, cells),
        f32(TEAM + 2, fold, lanes),
        f32(2 * TEAM, fold, lanes),
        f32(2, 2 * levels, cells),
        f32(2, 2 * levels, cells),
        f32(2 * levels, cells),
        f32(8, points),
        f32(8, points),
        dma((STEPS,)),
        dma((STEPS, COMM)),
        dma((1,)),
        dma((EARLY,)),
        dma((STEPS,)),
        dma((STEPS, COMM)),
        dma((1,)),
        dma((1,)),
        dma((1,)),
        dma((1,)),
        dma((1,)),
        dma((1,)),
        dma((2,)),
        dma((1,)),
        dma((2,)),
        dma((1,)),
        dma((1,)),
        dma((2,)),
        dma((STEPS,)),
        dma((STEPS,)),
        dma((1,)),
        dma((1,)),
        pltpu.SemaphoreType.REGULAR,
    ]
    operands = (
        spectrum,
        water_mask.reshape(1, points),
        courant,
        stencil_sign,
        quad_index.transpose(0, 2, 1),
        quad_weight.transpose(0, 2, 1),
        nonlinear.reshape(1, comps),
        stokes_table,
        point_index,
        point_weight,
        ocean_index,
        ocean_weight,
        currents,
        coriolis.reshape(1, cells),
        mixing.reshape(1, levels),
        surface_weights.reshape(1, levels),
    )
    scratch = [pltpu.VMEM(x.shape, x.dtype) for x in operands] + [dma((INPUTS + 1,))] + scratch
    return pl.pallas_call(
        wave_kernel,
        out_shape=(
            pltpu.VMEM((comps, points), F32),
            pltpu.VMEM(currents.shape, F32),
        ),
        in_specs=[pl.BlockSpec(memory_space=pltpu.HBM)] * INPUTS,
        out_specs=(vm, vm),
        scratch_shapes=scratch,
        compiler_params=pltpu.CompilerParams(
            collective_id=0, has_side_effects=True, vmem_limit_bytes=56 * 1024 * 1024
        ),
    )(*operands)


def solution(mesh):
    ring = P(("mp", "dev"))
    split_last = P(None, ("mp", "dev"))
    deep = P(None, None, ("mp", "dev"))
    return jax.shard_map(
        local,
        mesh=mesh,
        in_specs=(
            split_last, ring, P(), P(), P(), P(), P(), P(), split_last, split_last, split_last, split_last, deep,
            ring, P(), P(),
        ),
        out_specs=(split_last, deep),
        check_vma=False,
    )
```
